16 devices in a mesh: dp: 16 (over z, y, x, core).
Axes of the slice: x: 2, y: 2, z: 2, core: 2. Of those that a mesh axis runs over, the one named last changes fastest.
Arguments:
- grad_embed: bfloat16 [16, 8192, 1152], P('dp')
- grad_q: bfloat16 [16, 6, 1152, 32], P('dp')
- grad_k: bfloat16 [16, 6, 1152, 8], P('dp')
- grad_v: bfloat16 [16, 6, 1152, 8], P('dp')
- grad_out: bfloat16 [16, 6, 32, 1152], P('dp')
- grad_gate: bfloat16 [16, 6, 1152, 216], P('dp')
- grad_up: bfloat16 [16, 6, 1152, 216], P('dp')
- grad_down: bfloat16 [16, 6, 216, 1152], P('dp')
- grad_norms: bfloat16 [16, 6, 4, 1152], P('dp')
- grad_qk_norms: bfloat16 [16, 6, 2, 256], P('dp')
- first_moment: float32 [14499840], P('dp')
- second_moment: float32 [14499840], P('dp')
- master_param: float32 [14499840], P('dp')
- hyper_params: float32 [5], replicated
Outputs:
- output 1: bfloat16 [8192, 1152], replicated
- output 2: bfloat16 [6, 1152, 32], replicated
- output 3: bfloat16 [6, 1152, 8], replicated
- output 4: bfloat16 [6, 1152, 8], replicated
- output 5: bfloat16 [6, 32, 1152], replicated
- output 6: bfloat16 [6, 1152, 216], replicated
- output 7: bfloat16 [6, 1152, 216], replicated
- output 8: bfloat16 [6, 216, 1152], replicated
- output 9: bfloat16 [6, 4, 1152], replicated
- output 10: bfloat16 [6, 2, 256], replicated
- output 11: float32 [14499840], P('dp')
- output 12: float32 [14499840], P('dp')
- output 13: float32 [14499840], P('dp')
All inputs are finite; a program needn't handle non-finite values.
Results may differ from the reference program's by a relative error of at most 0.001.
Values are sent between devices in bfloat16 or wider.
A program may use at most 1 GiB of HBM per device.

```python
import math
import jax
import jax.numpy as jnp

D_MODEL = 1152
FF_WIDTH = 6912
Q_HEADS = 4
KV_HEADS = 1
HEAD_DIM = 256
VOCAB_SIZE = 262144
TP_RANKS = 32
NUM_LAYERS = 6
DATA_PAR = 16
ADAM_STEP = 7

ADAM_EPS = 1e-8
CLIP_EPS = 1e-6
Q_COLS = Q_HEADS * HEAD_DIM // TP_RANKS
KV_COLS = KV_HEADS * HEAD_DIM // TP_RANKS
FF_COLS = FF_WIDTH // TP_RANKS
VOCAB_ROWS = VOCAB_SIZE // TP_RANKS
PARAM_SHAPES = ((VOCAB_ROWS, D_MODEL), (NUM_LAYERS, D_MODEL, Q_COLS), (NUM_LAYERS, D_MODEL, KV_COLS), (NUM_LAYERS, D_MODEL, KV_COLS), (NUM_LAYERS, Q_COLS, D_MODEL), (NUM_LAYERS, D_MODEL, FF_COLS), (NUM_LAYERS, D_MODEL, FF_COLS), (NUM_LAYERS, FF_COLS, D_MODEL), (NUM_LAYERS, 4, D_MODEL), (NUM_LAYERS, 2, HEAD_DIM))
PARAM_SIZES = tuple(math.prod(tensor_dims) for tensor_dims in PARAM_SHAPES)
PARAMS_TOTAL = sum(PARAM_SIZES)
DECAY_LEN = PARAMS_TOTAL - PARAM_SIZES[8] - PARAM_SIZES[9]
GRAD_NAMES = ("grad_embed", "grad_q", "grad_k", "grad_v", "grad_out", "grad_gate", "grad_up", "grad_down", "grad_norms", "grad_qk_norms")


def setup_inputs(seed: int = 0) -> dict:
    key_list = jax.random.split(jax.random.key(seed), 16)
    grad_scale = math.sqrt(DATA_PAR)
    inputs = {}
    square_sum = jnp.float32(0.0)
    for tensor_index, tensor_dims in enumerate(PARAM_SHAPES):
        noise_draw = jax.random.normal(key_list[tensor_index], (DATA_PAR,) + tensor_dims, jnp.float32)
        grad_arr = (grad_scale * noise_draw).astype(jnp.bfloat16)
        mean_grad = jnp.sum(grad_arr, axis=0, dtype=jnp.float32) / DATA_PAR
        square_sum = square_sum + jnp.sum(mean_grad * mean_grad)
        inputs[GRAD_NAMES[tensor_index]] = grad_arr
    inputs["first_moment"] = 0.1 * jax.random.normal(key_list[10], (PARAMS_TOTAL,), jnp.float32)
    inputs["second_moment"] = 0.015 * jnp.exp(0.5 * jax.random.normal(key_list[11], (PARAMS_TOTAL,), jnp.float32))
    inputs["master_param"] = 0.5 * jax.random.normal(key_list[12], (PARAMS_TOTAL,), jnp.float32)
    hyper_draw = jax.random.uniform(key_list[13], (5,), jnp.float32)
    inputs["hyper_params"] = jnp.stack([0.05 + 0.1 * hyper_draw[0], 0.8 + 0.15 * hyper_draw[1], 0.9 + 0.09 * hyper_draw[2], 0.3 + 1.2 * hyper_draw[3], (0.3 + 0.4 * hyper_draw[4]) * jnp.sqrt(square_sum)])
    return inputs


def reference(grad_embed, grad_q, grad_k, grad_v, grad_out, grad_gate, grad_up, grad_down, grad_norms, grad_qk_norms, first_moment, second_moment, master_param, hyper_params):
    grads = (grad_embed, grad_q, grad_k, grad_v, grad_out, grad_gate, grad_up, grad_down, grad_norms, grad_qk_norms)
    mean_grad = jnp.concatenate([jnp.sum(grad_arr, axis=0, dtype=jnp.float32).reshape(-1) for grad_arr in grads]) / DATA_PAR
    learn_rate = hyper_params[0]
    beta_one = hyper_params[1]
    beta_two = hyper_params[2]
    weight_decay = hyper_params[3]
    grad_norm = jnp.sqrt(jnp.sum(mean_grad * mean_grad))
    clip_scale = jnp.minimum(1.0, hyper_params[4] / (grad_norm + CLIP_EPS))
    clipped = mean_grad * clip_scale
    moment_one = beta_one * first_moment + (1.0 - beta_one) * clipped
    moment_two = beta_two * second_moment + (1.0 - beta_two) * (clipped * clipped)
    m_hat = moment_one / (1.0 - beta_one ** ADAM_STEP)
    v_hat = moment_two / (1.0 - beta_two ** ADAM_STEP)
    keep_decay = jnp.arange(PARAMS_TOTAL) < DECAY_LEN
    direction = m_hat / (jnp.sqrt(v_hat) + ADAM_EPS) + jnp.where(keep_decay, weight_decay * master_param, 0.0)
    new_master = master_param - learn_rate * direction
    new_params = new_master.astype(jnp.bfloat16)
    out_list = []
    start_pos = 0
    for tensor_dims, tensor_size in zip(PARAM_SHAPES, PARAM_SIZES):
        out_list.append(new_params[start_pos:start_pos + tensor_size].reshape(tensor_dims))
        start_pos = start_pos + tensor_size
    return (out_list[0], out_list[1], out_list[2], out_list[3], out_list[4], out_list[5], out_list[6], out_list[7], out_list[8], out_list[9], moment_one, moment_two, new_master)
```

```python
import functools
import jax
import jax.numpy as jnp
from jax import lax
from jax.experimental import pallas as pl
from jax.experimental.pallas import tpu as pltpu
from jax.sharding import PartitionSpec as P

ADAM_EPS = 1e-8
CLIP_EPS = 1e-6
GRAD_COUNT = 10
MESH = pl.DeviceIdType.MESH

ROWS, LANES = 8, 128
TILE = (ROWS, LANES)
SHARE = 885
WIN = 918
NC = 6
WC = WIN // 3
T = WC // NC
STEP = 17
SMALL = 16 * 1024 * 1024
EMB = 9216
TAIL = 8847
LAY = 5313
LAYP = LAY + 33
HEAD = 21
PUB = 900
PC = PUB // 3
EXT = HEAD + SHARE
OFF_Q, OFF_K, OFF_V, OFF_O = 369, 585, 639, 693
OFF_G, OFF_U, OFF_D, OFF_N = 909, 2367, 3825, 5283
DIM = (2, 4, 8)
SHIFT = 88


def start_of(s):
    return 9 * ((SHARE * s) // 9) - jnp.where(s == 13, 18, 0) - jnp.where(s == 14, 9, 0)


def axes(colour):
    return [(colour + n) % 3 for n in range(3)]


def bit(d, dim):
    return (d // DIM[dim]) % 2


def flip(d, dim):
    return d + DIM[dim] * (1 - 2 * bit(d, dim))


def copies_wait(ref, sem):
    pltpu.make_async_copy(ref, ref, sem).wait()


def lanes():
    return lax.broadcasted_iota(jnp.int32, TILE, 1)


def gate_segments():
    rows = []
    for kap in range(27):
        pieces, f = [], LANES * kap
        while f < LANES * (kap + 1):
            i, c = f // 216, f % 216
            pieces.append((f - LANES * kap, i, c // LANES))
            f = min(LANES * (kap + 1), 216 * i + (128 if c < 128 else 216))
        rows.append(pieces)
    return rows


def gate_inverse():
    table = {}
    for kap, pieces in enumerate(gate_segments()):
        for n, (lo, i, half) in enumerate(pieces):
            hi = pieces[n + 1][0] if n + 1 < len(pieces) else 128
            table.setdefault((i, half), []).append((lo, hi, kap))
    return table


def merge(pieces, ids):
    out = pieces[0][1]
    for lo, val in pieces[1:]:
        out = jnp.where(ids >= lo, val, out)
    return out


def rows9_to_flat(win, flat, tmp, o, f):
    for ct in range(9):
        flat[pl.ds(f * ROWS + ct, ROWS, 9), :] = win[o + ct]


def gate_to_flat(win, flat, tmp, o, f):
    for half in range(2):
        tmp[half] = win[pl.ds(o + 16 * half, 16)].reshape(LANES, LANES).T
    ids = lanes()
    rolled = {}
    for i in range(16):
        for half in range(2):
            x = tmp[half, pl.ds(i, ROWS, 16), :]
            rolled[i, half] = pltpu.roll(x, (SHIFT * i) % LANES, 1)
    for kap, pieces in enumerate(gate_segments()):
        val = merge([(lo, rolled[i, half]) for lo, i, half in pieces], ids)
        flat[pl.ds(f * ROWS + kap, ROWS, 27), :] = val


def swap_groups(xs, width):
    ids = lanes() // width
    xs, step = list(xs), 1
    while step < len(xs):
        high = (ids // step) % 2 == 1
        for n in range(len(xs)):
            if not n & step:
                lo, hi = xs[n], xs[n + step]
                xs[n] = jnp.where(high, pltpu.roll(hi, width * step, 1), lo)
                xs[n + step] = jnp.where(high, hi, pltpu.roll(lo, LANES - width * step, 1))
        step = 2 * step
    return xs


def q_to_flat(win, flat, tmp, o, f):
    tmp[0] = win[pl.ds(o, 16)].reshape(LANES, LANES).T
    for kb in range(4):
        xs = swap_groups([tmp[0, pl.ds(32 * kb + i, ROWS, 4), :] for i in range(4)], 32)
        for u in range(4):
            flat[pl.ds((f + 4 * u + kb) * ROWS, ROWS), :] = xs[u]


def kv_to_flat(win, flat, tmp, o, f):
    tmp[0] = win[pl.ds(o, 16)].reshape(LANES, LANES).T
    xs = swap_groups([tmp[0, pl.ds(i, ROWS, 16), :] for i in range(16)], 8)
    for u in range(16):
        flat[pl.ds((f + u) * ROWS, ROWS), :] = xs[u]


def copy_to_flat(win, flat, tmp, o, f):
    flat[pl.ds(f * ROWS, ROWS), :] = win[o]


def rows9_to_tiles(stage, flat, tmp, o, f):
    for ct in range(9):
        stage[o + ct] = flat[pl.ds(f * ROWS + ct, ROWS, 9), :].astype(jnp.bfloat16)


def gate_to_tiles(stage, flat, tmp, o, f):
    ids = lanes()
    rows = [flat[pl.ds(f * ROWS + kap, ROWS, 27), :] for kap in range(27)]
    for (i, half), pieces in gate_inverse().items():
        val = rows[pieces[0][2]]
        for lo, hi, kap in pieces[1:]:
            val = jnp.where((ids >= lo) & (ids < hi), rows[kap], val)
        tmp[half, pl.ds(i, ROWS, 16), :] = pltpu.roll(val, (LANES - SHIFT * i) % LANES, 1)
    stage[pl.ds(o, 16)] = tmp[0].T.reshape(16, ROWS, LANES).astype(jnp.bfloat16)
    stage[pl.ds(o + 16, 11)] = tmp[1].T[:88].reshape(11, ROWS, LANES).astype(jnp.bfloat16)


def q_to_tiles(stage, flat, tmp, o, f):
    for kb in range(4):
        xs = swap_groups([flat[pl.ds((f + 4 * u + kb) * ROWS, ROWS), :] for u in range(4)], 32)
        for i in range(4):
            tmp[0, pl.ds(32 * kb + i, ROWS, 4), :] = xs[i]
    stage[pl.ds(o, 16)] = tmp[0].T.reshape(16, ROWS, LANES).astype(jnp.bfloat16)


def kv_to_tiles(stage, flat, tmp, o, f):
    xs = swap_groups([flat[pl.ds((f + u) * ROWS, ROWS), :] for u in range(16)], 8)
    for i in range(16):
        tmp[0, pl.ds(i, ROWS, 16), :] = xs[i]
    stage[pl.ds(o, 16)] = tmp[0].T.reshape(16, ROWS, LANES).astype(jnp.bfloat16)


def copy_to_tiles(stage, flat, tmp, o, f):
    stage[o] = flat[pl.ds(f * ROWS, ROWS), :].astype(jnp.bfloat16)


def walk_units(me, base, wide, rows9, gate, q, kv, one):
    def pick(table):
        return sum(jnp.where(me == d, n, 0) for d, n in table.items())
    ends = (SHARE * (me + 1) + (8 if wide else 0)) // 9 - (SHARE * me) // 9
    first = jnp.where(me < 10, ends, pick({10: 41, 11: 3, 15: 95}))
    n_q = pick({10: 14})
    n_kv = pick({10: 7})
    n_gate = pick({11: 32, 12: 33 if wide else 32, 13: 34 if wide else 33, 14: 11})
    second = pick({10: 22 if wide else 21, 14: 67})
    n_one = pick({15: 30})
    pos = 0
    for count, size, fn, over in ((first, 9, rows9, 0), (n_q, 16, q, pick({10: 8})), (n_kv, 16, kv, pick({10: 4})),
                                  (n_gate, 27, gate, 0), (second, 9, rows9, 0), (n_one, 1, one, 0)):
        def step(u, carry, pos=pos, size=size, fn=fn):
            fn(pos + u * size, base + pos + u * size)
            return carry
        lax.fori_loop(0, count, step, 0)
        pos = pos + count * size - over


def reduce_kernel(emb, q, k, v, out, gate, up, down, norm, mom, var, mas,
                  flat_out, norm_out, head_out,
                  lay, raw, own, acc, recv2, recv3, flat, tmp, part,
                  lay_sem, head_sems, own_sem, raw_send, raw_recv, s2_send, s2_recv, s3_send, s3_recv, n_send, n_recv, o_sem):
    me = lax.axis_index("dp")
    core = me % 2
    nxt = lax.rem(me + 1, 16)

    for src, off, n in ((emb.at[pl.ds(TAIL, OFF_Q)], 0, OFF_Q), (out, OFF_O, 216), (down, OFF_D, 1458), (norm, OFF_N, 30)):
        pltpu.make_async_copy(src, lay.at[pl.ds(off, n)], lay_sem).start()

    def load(i, carry):
        l, rb = i // 9, lax.rem(i, 9)
        for src, off, n in ((q, OFF_Q, 4), (k, OFF_K, 1), (v, OFF_V, 1), (gate, OFF_G, 27), (up, OFF_U, 27)):
            pltpu.make_async_copy(src.at[l, :, rb], lay.at[pl.ds(off + i * n, n)], lay_sem).start()
        return carry

    lax.fori_loop(0, 54, load, 0)
    lay[pl.ds(LAY, LAYP - LAY)] = jnp.zeros((LAYP - LAY, ROWS, LANES), jnp.bfloat16)

    heads = []
    for n, src in enumerate((mom, var, mas)):
        copy = pltpu.make_async_remote_copy(
            src_ref=src.at[pl.ds(SHARE - HEAD, HEAD)], dst_ref=head_out.at[n], send_sem=head_sems.at[0, n], recv_sem=head_sems.at[1, n],
            device_id=(nxt,), device_id_type=MESH)
        copy.start()
        heads.append(copy)

    def send_raw(s, pos, dst, target, recv_sem, turn):
        first = start_of(s) + pos

        def send(src):
            pltpu.make_async_remote_copy(
                src_ref=src, dst_ref=dst, send_sem=raw_send, recv_sem=recv_sem, device_id=(target,), device_id_type=MESH).start()

        @pl.when((s < 10) & (turn != 1))
        def _():
            send(emb.at[pl.ds(first, T)])

        @pl.when((s >= 10) & (turn != 0))
        def _():
            send(lay.at[pl.ds(first - TAIL, T)])

    def scatter(turn, carry):
        ch = jnp.maximum(turn - 1, 0)

        @pl.when(turn == 1)
        def _():
            copies_wait(lay.at[pl.ds(0, LAY)], lay_sem)

        for kc in range(3):
            a, b, e = axes(kc)
            pos = kc * (WC) + ch * T
            far = flip(me, a)

            def share_step(j, carry):
                near = (j // 2) * DIM[b] + (j % 2) * DIM[e]
                for to in range(2):
                    s = (1 - bit(me, a)) * DIM[a] + near + to
                    send_raw(s, pos, raw.at[kc, ch, core, j], far - core + to, raw_recv.at[kc, ch], turn)
                s = bit(me, a) * DIM[a] + near + 1 - core
                send_raw(s, pos, raw.at[kc, ch, 2, j], me + 1 - 2 * core, raw_recv.at[kc, ch], turn)
                return carry

            lax.fori_loop(0, 4, share_step, 0)
        return carry

    lax.fori_loop(0, NC + 1, scatter, 0)

    def first_sum(ch, carry):
        for kc in range(3):
            a, b, e = axes(kc)
            pos = kc * (WC) + ch * T
            mine = [bit(me, a) * DIM[a] + (j // 2) * DIM[b] + (j % 2) * DIM[e] + core for j in range(4)]
            for j in range(4):
                first = start_of(mine[j]) + pos

                @pl.when(mine[j] < 10)
                def _():
                    pltpu.make_async_copy(emb.at[pl.ds(first, T)], own.at[j], own_sem.at[j]).start()

                @pl.when(mine[j] >= 10)
                def _():
                    own[j] = lay[pl.ds(first - TAIL, T)]

            copies_wait(raw.at[kc, ch], raw_recv.at[kc, ch])
            for j in range(4):
                @pl.when(mine[j] < 10)
                def _():
                    copies_wait(own.at[j], own_sem.at[j])

            def sum_step(n, carry):
                j = (n // 2 + 1 - bit(me, b)) % 2 * 2 + n % 2

                def tile_step(t, carry):
                    i = pl.ds(t * STEP, STEP)
                    acc[kc, ch, pl.ds(j * T + t * STEP, STEP)] = (
                        (own[j, i].astype(jnp.float32) + raw[kc, ch, 2, j, i].astype(jnp.float32))
                        + (raw[kc, ch, 0, j, i].astype(jnp.float32) + raw[kc, ch, 1, j, i].astype(jnp.float32)))
                    return carry

                lax.fori_loop(0, T // STEP, tile_step, 0)
                return carry

            lax.fori_loop(0, 4, sum_step, 0)
            pltpu.make_async_remote_copy(
                src_ref=acc.at[kc, ch, pl.ds(2 * (1 - bit(me, b)) * T, 2 * T)], dst_ref=recv2.at[pl.ds((kc * NC + ch) * 2 * T, 2 * T)],
                send_sem=s2_send, recv_sem=s2_recv.at[kc, ch], device_id=(flip(me, b),), device_id_type=MESH).start()
        return carry

    lax.fori_loop(0, NC, first_sum, 0)

    def second_sum(ch, carry):
        for kc in range(3):
            a, b, e = axes(kc)
            slot = (kc * NC + ch) * 2 * T
            copies_wait(recv2.at[pl.ds(slot, 2 * T)], s2_recv.at[kc, ch])
            for n in range(2):
                je = (1 - bit(me, e)) if n == 0 else bit(me, e)
                j = 2 * bit(me, b) + je

                def tile_step(t, carry):
                    i = pl.ds(t * STEP, STEP)
                    at = pl.ds(j * T + t * STEP, STEP)
                    acc[kc, ch, at] = acc[kc, ch, at] + recv2[pl.ds(slot + je * T + t * STEP, STEP)]
                    return carry

                lax.fori_loop(0, T // STEP, tile_step, 0)
            pltpu.make_async_remote_copy(
                src_ref=acc.at[kc, ch, pl.ds((2 * bit(me, b) + 1 - bit(me, e)) * T, T)], dst_ref=recv3.at[kc, ch],
                send_sem=s3_send, recv_sem=s3_recv.at[kc, ch], device_id=(flip(me, e),), device_id_type=MESH).start()
        return carry

    lax.fori_loop(0, NC, second_sum, 0)

    def third_sum(ch, carry):
        for kc in range(3):
            a, b, e = axes(kc)
            copies_wait(recv3.at[kc, ch], s3_recv.at[kc, ch])
            j = 2 * bit(me, b) + bit(me, e)

            def tile_step(t, carry):
                i = pl.ds(t * STEP, STEP)
                recv2[pl.ds((kc * NC + ch) * T + t * STEP, STEP)] = (acc[kc, ch, pl.ds(j * T + t * STEP, STEP)] + recv3[kc, ch, i]) * 0.0625
                return carry

            lax.fori_loop(0, T // STEP, tile_step, 0)
        return carry

    lax.fori_loop(0, NC, third_sum, 0)

    base = HEAD - (SHARE * me - start_of(me))
    walk_units(me, base, True, *[functools.partial(fn, recv2, flat, tmp) for fn in (rows9_to_flat, gate_to_flat, q_to_flat, kv_to_flat, copy_to_flat)])

    store = pltpu.make_async_copy(flat.at[pl.ds(0, EXT * ROWS)], flat_out, o_sem)
    store.start()

    def square_step(t, total):
        for n in range(15):
            x = flat[pl.ds((HEAD + t * 15 + n) * ROWS, ROWS), :]
            total = total + x * x
        return total

    part[me] = lax.fori_loop(0, SHARE // 15, square_step, jnp.zeros(TILE, jnp.float32))
    for step in range(1, 16):
        pltpu.make_async_remote_copy(
            src_ref=part.at[me], dst_ref=part.at[me], send_sem=n_send, recv_sem=n_recv,
            device_id=(lax.rem(me + step, 16),), device_id_type=MESH).start()
    copies_wait(part.at[pl.ds(0, 15)], n_recv)
    norm_out[...] = jnp.sum(part[...], axis=0)
    copies_wait(part.at[pl.ds(0, 15)], n_send)
    copies_wait(raw, raw_send)
    copies_wait(recv2, s2_send)
    copies_wait(recv3, s3_send)
    for copy in heads:
        copy.wait()
    store.wait()


def update_kernel(flat_in, norm_in, head, mom, var, mas, hyper,
                  gathered, m, v, p,
                  g, tmp, in_sems, send_sem, recv_sems, pair_recv):
    me = lax.axis_index("dp")
    core = me % 2
    loads = []
    for n, (src, dst) in enumerate(((mom, m), (var, v), (mas, p))):
        loads.append(pltpu.make_async_copy(src, dst.at[pl.ds(HEAD * ROWS, SHARE * ROWS)], in_sems.at[n]))
        loads.append(pltpu.make_async_copy(head.at[n], dst.at[pl.ds(0, HEAD * ROWS)], in_sems.at[n + 3]))
    loads.append(pltpu.make_async_copy(flat_in, g, in_sems.at[6]))
    for copy in loads:
        copy.start()

    def full(x):
        return jnp.full(TILE, x, jnp.float32)

    def power7(x):
        x2 = x * x
        return x2 * x2 * x2 * x

    total = full(jnp.sum(norm_in[...]))
    rate, b1, b2, decay, limit = (full(hyper[n]) for n in range(5))
    clip = jnp.minimum(1.0, limit / (jnp.sqrt(total) + CLIP_EPS))
    a1 = (1.0 - b1) * clip
    a2 = (1.0 - b2) * (clip * clip)
    fix1 = 1.0 / (1.0 - power7(b1))
    fix2 = 1.0 / (1.0 - power7(b2))
    for copy in loads:
        copy.wait()

    def update(t, carry):
        for n in range(6):
            tile = t * 6 + n
            i = pl.ds(tile * ROWS, ROWS)
            gt, pt = g[i, :], p[i, :]
            mt = b1 * m[i, :] + (1.0 - b1) * (gt * clip)
            h = gt * clip
            vt = b2 * v[i, :] + (1.0 - b2) * (h * h)
            has_decay = SHARE * me - HEAD + tile < 14130
            u = (mt * fix1) / (jnp.sqrt(vt * fix2) + ADAM_EPS) + jnp.where(has_decay, decay, 0.0) * pt
            m[i, :] = mt
            v[i, :] = vt
            p[i, :] = pt - rate * u
        return carry

    lax.fori_loop(0, EXT // 6, update, 0)
    base = HEAD - (SHARE * me - start_of(me))
    stage = gathered.at[pl.ds(me * PUB, PUB)]
    walk_units(me, base, False, *[functools.partial(fn, stage, p, tmp) for fn in (rows9_to_tiles, gate_to_tiles, q_to_tiles, kv_to_tiles, copy_to_tiles)])

    pair = me + 1 - 2 * core

    def send(src, owner, kc, target, recv):
        pltpu.make_async_remote_copy(
            src_ref=src, dst_ref=gathered.at[pl.ds(owner * PUB + kc * PC, PC)], send_sem=send_sem, recv_sem=recv,
            device_id=(target,), device_id_type=MESH).start()

    for hop in range(3):
        for kc in range(3):
            dim = (kc + hop) % 3
            send(stage.at[pl.ds(kc * PC, PC)], me, kc, flip(me, dim), recv_sems.at[kc, (0, 1, 3)[hop]])
    for kc in range(3):
        send(stage.at[pl.ds(kc * PC, PC)], me, kc, pair, pair_recv)
    for piece in range(7):
        for kc in range(3):
            a, b, e = axes(kc)
            n = piece + 1
            owner = me
            for pos, dim in enumerate((a, b, e)):
                if (n >> pos) & 1:
                    owner = flip(owner, dim)
            block = gathered.at[pl.ds(owner * PUB + kc * PC, PC)]
            copies_wait(block, recv_sems.at[kc, piece])
            if n == 1:
                send(block, owner, kc, flip(me, b), recv_sems.at[kc, 2])
            if n < 4:
                send(block, owner, kc, flip(me, e), recv_sems.at[kc, n + 3])
            send(block, owner, kc, pair, pair_recv)
    copies_wait(gathered.at[pl.ds(0, 8 * PUB)], pair_recv)
    copies_wait(gathered.at[pl.ds(0, 15 * PUB)], send_sem)


def finish_kernel(gathered, m, v, p, emb, q, k, v_out, out, gate, up, down, norm, mom_out, var_out, mas_out, sem, state_sem):
    starts = [9 * (SHARE * s // 9) - {13: 18, 14: 9}.get(s, 0) for s in range(16)] + [TAIL + LAY]
    state = [pltpu.make_async_copy(src.at[pl.ds(HEAD * ROWS, SHARE * ROWS)], dst, state_sem.at[n])
             for n, (src, dst) in enumerate(((m, mom_out), (v, var_out), (p, mas_out)))]
    for copy in state:
        copy.start()
    for dst, first, n, size in ((emb, 0, EMB, 1), (q, TAIL + OFF_Q, 54, 4), (k, TAIL + OFF_K, 54, 1), (v_out, TAIL + OFF_V, 54, 1),
                                (out, TAIL + OFF_O, 216, 1), (gate, TAIL + OFF_G, 54, 27), (up, TAIL + OFF_U, 54, 27),
                                (down, TAIL + OFF_D, 1458, 1), (norm, TAIL + OFF_N, 30, 1)):
        for s in range(16):
            lo, hi = max(starts[s], first), min(starts[s + 1], first + n * size)
            if lo >= hi:
                continue
            src = s * PUB + lo - starts[s]
            if len(dst.shape) == 3:
                pltpu.make_async_copy(gathered.at[pl.ds(src, hi - lo)], dst.at[pl.ds(lo - first, hi - lo)], sem).start()
                continue
            unit = (lo - first) // size

            def step(i, carry, dst=dst, src=src, unit=unit, size=size):
                l, rb = (unit + i) // 9, lax.rem(unit + i, 9)
                pltpu.make_async_copy(gathered.at[pl.ds(src + i * size, size)], dst.at[l, :, rb], sem).start()
                return carry

            lax.fori_loop(0, (hi - lo) // size, step, 0)
    copies_wait(gathered.at[pl.ds(0, TAIL + LAY)], sem)
    for copy in state:
        copy.wait()


ANY = pl.BlockSpec(memory_space=pl.ANY)
VM = pl.BlockSpec(memory_space=pltpu.VMEM)
DMA = pltpu.SemaphoreType.DMA


def tiled(x):
    rows, cols = x.shape[-2:]
    x = x.reshape(x.shape[:-2] + (rows // ROWS, ROWS, cols // LANES, LANES))
    return jnp.swapaxes(x, -3, -2)


def solution(mesh):
    def local_update(*arrays):
        emb, q, k, v, out, gate, up, down, norms, qk = [a[0] for a in arrays[:GRAD_COUNT]]
        mom, var, mas, hyper = arrays[GRAD_COUNT:]
        emb_t = tiled(emb).reshape(EMB, ROWS, LANES)
        q, k, v, gate, up = [tiled(jnp.swapaxes(x, 1, 2)) for x in (q, k, v, gate, up)]
        out_t, down_t = tiled(out).reshape(216, ROWS, LANES), tiled(down).reshape(1458, ROWS, LANES)
        norm = jnp.concatenate([norms.reshape(-1), qk.reshape(-1)]).reshape(30, ROWS, LANES)
        state = [x.reshape(SHARE, ROWS, LANES) for x in (mom, var, mas)]

        flat, total, head = pl.pallas_call(
            reduce_kernel,
            out_shape=(jax.ShapeDtypeStruct((EXT * ROWS, 128), jnp.float32), jax.ShapeDtypeStruct(TILE, jnp.float32),
                       jax.ShapeDtypeStruct((3, HEAD, ROWS, LANES), jnp.float32)),
            in_specs=[ANY] * 12,
            out_specs=(ANY, VM, ANY),
            scratch_shapes=[
                pltpu.VMEM((LAYP, ROWS, LANES), jnp.bfloat16),
                pltpu.VMEM((3, NC, 3, 4, T, ROWS, LANES), jnp.bfloat16),
                pltpu.VMEM((4, T, ROWS, LANES), jnp.bfloat16),
                pltpu.VMEM((3, NC, 4 * T, ROWS, LANES), jnp.float32),
                pltpu.VMEM((2 * WIN, ROWS, LANES), jnp.float32),
                pltpu.VMEM((3, NC, T, ROWS, LANES), jnp.float32),
                pltpu.VMEM(((HEAD + WIN) * ROWS, 128), jnp.float32),
                pltpu.VMEM((2, LANES, LANES), jnp.float32),
                pltpu.VMEM((16, ROWS, LANES), jnp.float32),
                DMA, DMA((2, 3)), DMA((4,)), DMA, DMA((3, NC)), DMA, DMA((3, NC)), DMA, DMA((3, NC)), DMA, DMA, DMA,
            ],
            compiler_params=pltpu.CompilerParams(has_side_effects=True, vmem_limit_bytes=67043328),
            name="reduce",
        )(emb_t, q, k, v, out_t, gate, up, down_t, norm, *state)

        rows = [x.reshape(SHARE * ROWS, 128) for x in (mom, var, mas)]
        held = [pltpu.VMEM((16 * PUB, ROWS, LANES), jnp.bfloat16)] + [pltpu.VMEM((EXT * ROWS, 128), jnp.float32)] * 3
        kept = pl.pallas_call(
            update_kernel,
            out_shape=tuple(held),
            in_specs=[ANY, VM] + [ANY] * 4 + [pl.BlockSpec(memory_space=pltpu.SMEM)],
            out_specs=(VM,) * 4,
            scratch_shapes=[
                pltpu.VMEM((EXT * ROWS, 128), jnp.float32), pltpu.VMEM((2, LANES, LANES), jnp.float32),
                DMA((7,)), DMA, DMA((3, 7)), DMA,
            ],
            compiler_params=pltpu.CompilerParams(has_side_effects=True, vmem_limit_bytes=SMALL),
            name="update",
        )(flat, total, head.reshape(3, HEAD * ROWS, 128), *rows, hyper)

        like = [emb_t, q, k, v, out_t, gate, up, down_t, norm] + rows
        emb2, q2, k2, v2, out2, gate2, up2, down2, norm2, *state2 = pl.pallas_call(
            finish_kernel,
            out_shape=tuple(jax.ShapeDtypeStruct(x.shape, x.dtype) for x in like),
            in_specs=[VM] * 4,
            out_specs=(ANY,) * 12,
            scratch_shapes=[DMA, DMA((3,))],
            compiler_params=pltpu.CompilerParams(vmem_limit_bytes=SMALL),
            name="finish",
        )(*[pltpu.with_memory_space_constraint(x, pltpu.VMEM) for x in kept])

        def matrices(x):
            return jnp.swapaxes(x, 2, 3).reshape(6, -1, 1152)

        def columns(x):
            return jnp.swapaxes(matrices(x), 1, 2)

        flat_norm = norm2.reshape(-1)
        cut = norms.size
        params = (jnp.swapaxes(emb2.reshape(1024, 9, ROWS, LANES), 1, 2).reshape(emb.shape),
                  columns(q2), columns(k2), columns(v2), matrices(out2.reshape(6, 4, 9, ROWS, LANES)), columns(gate2), columns(up2),
                  matrices(down2.reshape(6, 27, 9, ROWS, LANES)), flat_norm[:cut].reshape(norms.shape), flat_norm[cut:].reshape(qk.shape))
        return params + tuple(x.reshape(-1) for x in state2)

    in_specs = tuple([P("dp")] * GRAD_COUNT + [P("dp"), P("dp"), P("dp"), P()])
    out_specs = tuple([P()] * GRAD_COUNT + [P("dp"), P("dp"), P("dp")])
    return jax.shard_map(local_update, mesh=mesh, in_specs=in_specs, out_specs=out_specs, check_vma=False)
```

```python
import functools
import jax
import jax.numpy as jnp
from jax import lax
from jax.experimental import pallas as pl
from jax.experimental.pallas import tpu as pltpu
from jax.sharding import PartitionSpec as P

ADAM_EPS = 1e-8
CLIP_EPS = 1e-6
GRAD_COUNT = 10
MESH = pl.DeviceIdType.MESH
F32, BF16 = jnp.float32, jnp.bfloat16

ROWS, LANES = 8, 128
TILE = (ROWS, LANES)
DEVICES = 16
SHARE = 885
WIN = 891
WIDE = 918
CUT = (14, 13)
NC = 9
T = 33
STEP = 11
MINI = 9
EMB = 9216
TAIL = 8847
LAY = 5313
LAYP = LAY + MINI
HALF = 2367
HEAD = 21
PUB = 900
NA = 3
PC = 100
EXT = HEAD + SHARE
OFF_Q, OFF_K, OFF_V, OFF_O = 369, 585, 639, 693
OFF_G, OFF_U, OFF_D, OFF_N = 909, 2367, 3825, 5283
DIM = (2, 4, 8)
SHIFT = 88
GRANT = 26300000
RAW_END = 12 * WIN
OWN_AT = RAW_END
RAW_M = OWN_AT + 12 * T
OWN_M = RAW_M + 9 * MINI
STAGE_AT = OWN_M + 3 * MINI


def start_of(s):
    return 9 * ((SHARE * s) // 9) - jnp.where(s == 13, 18, 0) - jnp.where(s == 14, 9, 0)


def axes(colour):
    return [(colour + n) % 3 for n in range(3)]


def bit(d, dim):
    return (d // DIM[dim]) % 2


def flip(d, dim):
    return d + DIM[dim] * (1 - 2 * bit(d, dim))


def copies_wait(ref, sem):
    pltpu.make_async_copy(ref, ref, sem).wait()


def put(src, dst, send_sem, recv_sem, target):
    copy = pltpu.make_async_remote_copy(
        src_ref=src, dst_ref=dst, send_sem=send_sem, recv_sem=recv_sem, device_id=(target,), device_id_type=MESH)
    copy.start()
    return copy


def loop(lo, hi, fn):
    def step(i, carry):
        fn(i)
        return carry
    lax.fori_loop(lo, hi, step, 0)


def lanes():
    return lax.broadcasted_iota(jnp.int32, TILE, 1)


def gate_segments():
    rows = []
    for kap in range(27):
        pieces, f = [], LANES * kap
        while f < LANES * (kap + 1):
            i, c = f // 216, f % 216
            pieces.append((f - LANES * kap, i, c // LANES))
            f = min(LANES * (kap + 1), 216 * i + (LANES if c < LANES else 216))
        rows.append(pieces)
    return rows


def gate_inverse():
    table = {}
    for kap, pieces in enumerate(gate_segments()):
        ends = [lo for lo, _, _ in pieces[1:]] + [LANES]
        for (lo, i, half), hi in zip(pieces, ends):
            table.setdefault((i, half), []).append((lo, hi, kap))
    return table


def swap_groups(xs, width):
    ids = lanes() // width
    xs, step = list(xs), 1
    while step < len(xs):
        high = (ids // step) % 2 == 1
        for n in range(len(xs)):
            if not n & step:
                lo, hi = xs[n], xs[n + step]
                xs[n] = jnp.where(high, pltpu.roll(hi, width * step, 1), lo)
                xs[n + step] = jnp.where(high, hi, pltpu.roll(lo, LANES - width * step, 1))
        step = 2 * step
    return xs


def turned(win, o):
    return win[pl.ds(o, 16)].reshape(LANES, LANES).T


def rows9_to_flat(win, flat, tmp, o, f):
    for ct in range(9):
        flat[pl.ds(f * ROWS + ct, ROWS, 9), :] = win[o + ct]


def gate_to_flat(win, flat, tmp, o, f):
    for half in range(2):
        tmp[half] = turned(win, o + 16 * half)
    ids = lanes()
    rolled = {}
    for i in range(16):
        for half in range(2):
            rolled[i, half] = pltpu.roll(tmp[half, pl.ds(i, ROWS, 16), :], (SHIFT * i) % LANES, 1)
    for kap, pieces in enumerate(gate_segments()):
        val = None
        for lo, i, half in pieces:
            val = rolled[i, half] if val is None else jnp.where(ids >= lo, rolled[i, half], val)
        flat[pl.ds(f * ROWS + kap, ROWS, 27), :] = val


def q_to_flat(win, flat, tmp, o, f):
    tmp[0] = turned(win, o)
    for kb in range(4):
        xs = swap_groups([tmp[0, pl.ds(32 * kb + i, ROWS, 4), :] for i in range(4)], 32)
        for u in range(4):
            flat[pl.ds((f + 4 * u + kb) * ROWS, ROWS), :] = xs[u]


def kv_to_flat(win, flat, tmp, o, f):
    tmp[0] = turned(win, o)
    xs = swap_groups([tmp[0, pl.ds(i, ROWS, 16), :] for i in range(16)], ROWS)
    for u in range(16):
        flat[pl.ds((f + u) * ROWS, ROWS), :] = xs[u]


def copy_to_flat(win, flat, tmp, o, f):
    flat[pl.ds(f * ROWS, ROWS), :] = win[o]


def rows9_to_tiles(stage, flat, tmp, o, f):
    for ct in range(9):
        stage[o + ct] = flat[pl.ds(f * ROWS + ct, ROWS, 9), :].astype(BF16)


def gate_to_tiles(stage, flat, tmp, o, f):
    ids = lanes()
    rows = [flat[pl.ds(f * ROWS + kap, ROWS, 27), :] for kap in range(27)]
    for (i, half), pieces in gate_inverse().items():
        val = rows[pieces[0][2]]
        for lo, hi, kap in pieces[1:]:
            val = jnp.where((ids >= lo) & (ids < hi), rows[kap], val)
        tmp[half, pl.ds(i, ROWS, 16), :] = pltpu.roll(val, (LANES - SHIFT * i) % LANES, 1)
    stage[pl.ds(o, 16)] = tmp[0].T.reshape(16, ROWS, LANES).astype(BF16)
    stage[pl.ds(o + 16, 11)] = tmp[1].T[:SHIFT].reshape(11, ROWS, LANES).astype(BF16)


def q_to_tiles(stage, flat, tmp, o, f):
    for kb in range(4):
        xs = swap_groups([flat[pl.ds((f + 4 * u + kb) * ROWS, ROWS), :] for u in range(4)], 32)
        for i in range(4):
            tmp[0, pl.ds(32 * kb + i, ROWS, 4), :] = xs[i]
    stage[pl.ds(o, 16)] = tmp[0].T.reshape(16, ROWS, LANES).astype(BF16)


def kv_to_tiles(stage, flat, tmp, o, f):
    xs = swap_groups([flat[pl.ds((f + u) * ROWS, ROWS), :] for u in range(16)], ROWS)
    for i in range(16):
        tmp[0, pl.ds(i, ROWS, 16), :] = xs[i]
    stage[pl.ds(o, 16)] = tmp[0].T.reshape(16, ROWS, LANES).astype(BF16)


def copy_to_tiles(stage, flat, tmp, o, f):
    stage[o] = flat[pl.ds(f * ROWS, ROWS), :].astype(BF16)


TO_FLAT = (rows9_to_flat, gate_to_flat, q_to_flat, kv_to_flat, copy_to_flat)
TO_TILES = (rows9_to_tiles, gate_to_tiles, q_to_tiles, kv_to_tiles, copy_to_tiles)


def walk_units(me, wide, lo, hi, fns, run):
    def pick(table):
        return sum(jnp.where(me == d, n, 0) for d, n in table.items())
    rows9, gate, q, kv, one = fns
    ends = (SHARE * (me + 1) + (8 if wide else 0)) // 9 - (SHARE * me) // 9
    first = jnp.where(me < 10, ends, pick({10: 41, 11: 3, 15: 95}))
    n_gate = pick({11: 32, 12: 33 if wide else 32, 13: 34 if wide else 33, 14: 11})
    second = pick({10: 22 if wide else 21, 14: 67})
    pos = 0
    for count, size, fn, over in ((first, 9, rows9, 0), (pick({10: 14}), 16, q, pick({10: 8})), (pick({10: 7}), 16, kv, pick({10: 4})),
                                  (n_gate, 27, gate, 0), (second, 9, rows9, 0), (pick({15: 30}), 1, one, 0)):
        def done(x):
            return jnp.minimum(jnp.maximum(x - pos + (0 if wide else size - 1), 0) // size, count)

        loop(done(lo), done(hi), lambda u, pos=pos, size=size, fn=fn: run(fn, pos + u * size))
        pos = pos + count * size - over


def step_kernel(emb, q, k, v, out, gate, up, down, norm, mom, var, mas, hyper,
                full, m_buf, v_buf, p_buf, lay,
                acc, buf, recv3, tmp, part, acc_m, recv2_m, recv3_m,
                lay_sem, state_sem, head_sems, own_sem, raw_send, raw_recv, s2_send, s2_recv, s3_send, s3_recv, n_send, n_recv,
                m_raw_send, m_raw_recv, m_own, m_send, m_recv, a_send, a_recv, pair_recv):
    me = lax.axis_index("dp")
    core = me % 2
    pair = me + 1 - 2 * core
    flat = buf.reshape(2 * WIDE * ROWS, LANES)

    state = ((mom, m_buf), (var, v_buf), (mas, p_buf))
    loads = [pltpu.make_async_copy(src, dst.at[pl.ds(HEAD * ROWS, SHARE * ROWS)], state_sem.at[n]) for n, (src, dst) in enumerate(state)]
    for copy in loads:
        copy.start()
    heads = [put(src.at[pl.ds((SHARE - HEAD) * ROWS, HEAD * ROWS)], dst.at[pl.ds(0, HEAD * ROWS)], head_sems.at[0, n], head_sems.at[1, n],
                 lax.rem(me + 1, DEVICES)) for n, (src, dst) in enumerate(state)]

    def raw_at(kc, ch, src, j):
        return full.at[pl.ds(((kc * NC + ch) * 12 + src * 4 + j) * T, T)]

    def share_tiles(s, pos, n, fn):
        first = start_of(s) + pos

        @pl.when(s < 10)
        def _():
            fn(emb.at[pl.ds(first, n)])

        @pl.when(s >= 10)
        def _():
            fn(lay.at[pl.ds(first - TAIL, n)])

    def scatter(ch, with_emb, with_lay):
        def one(s, kc, src, j, target):
            @pl.when(jnp.where(s < 10, with_emb, with_lay) == 1)
            def _():
                share_tiles(s, (ch * 3 + kc) * T, T, lambda ref: put(ref, raw_at(kc, ch, src, j), raw_send, raw_recv.at[kc, ch], target))

        for kc in range(3):
            a, b, e = axes(kc)
            far = flip(me, a)

            def share_step(j):
                near = (j // 2) * DIM[b] + (j % 2) * DIM[e]
                for to in range(2):
                    one((1 - bit(me, a)) * DIM[a] + near + to, kc, core, j, far - core + to)
                one(bit(me, a) * DIM[a] + near + 1 - core, kc, 2, j, pair)

            loop(0, 4, share_step)

    loop(0, 3, lambda ch: scatter(ch, 1, 0))
    for lo, whole, split in ((0, ((emb.at[pl.ds(TAIL, OFF_Q)], 0), (out, OFF_O)), ((q, OFF_Q, 4), (k, OFF_K, 1), (v, OFF_V, 1), (gate, OFF_G, 27))),
                             (HALF, ((down, OFF_D), (norm, OFF_N)), ((up, OFF_U, 27),))):
        n = HALF if lo == 0 else LAY - HALF
        stage = full.at[pl.ds(STAGE_AT, n)]
        for src, off in whole:
            pltpu.make_async_copy(src, full.at[pl.ds(STAGE_AT + off - lo, src.shape[0])], lay_sem.at[0]).start()

        def load(i):
            for src, off, size in split:
                pltpu.make_async_copy(src.at[i // 9, :, lax.rem(i, 9)], full.at[pl.ds(STAGE_AT + off - lo + i * size, size)], lay_sem.at[0]).start()

        loop(0, 54, load)
        copies_wait(stage, lay_sem.at[0])
        save = pltpu.make_async_copy(stage, lay.at[pl.ds(lo, n)], lay_sem.at[1])
        save.start()
        save.wait()
    loop(0, NC, lambda ch: scatter(ch, jnp.where(ch < 3, 0, 1), 1))

    cut = jnp.where(core == 0, *CUT)

    def extra_at(kc):
        return WIN + kc * MINI

    def extra_sends(fn):
        for kc in range(3):
            for to, s in enumerate(CUT):
                far = bit(me, kc) != bit(s, kc)

                @pl.when(far | (core != to))
                def _():
                    fn(kc, to, s, far)

    def extra_send(kc, to, s, far):
        put(lay.at[pl.ds(start_of(s) - TAIL + extra_at(kc), MINI)],
            full.at[pl.ds(RAW_M + (kc * 3 + jnp.where(far, core, 2)) * MINI, MINI)], m_raw_send.at[kc, to], m_raw_recv.at[kc],
            jnp.where(far, flip(me, kc), me) - core + to)

    extra_sends(extra_send)

    def fetch(ch, kc):
        a, b, e = axes(kc)
        for j in range(4):
            s = bit(me, a) * DIM[a] + (j // 2) * DIM[b] + (j % 2) * DIM[e] + core
            share_tiles(s, (ch * 3 + kc) * T, T,
                        lambda ref: pltpu.make_async_copy(ref, full.at[pl.ds(OWN_AT + (kc * 4 + j) * T, T)], own_sem.at[kc]).start())

    for kc in range(3):
        fetch(0, kc)

    def first_sum(ch):
        for kc in range(3):
            a, b, e = axes(kc)
            copies_wait(full.at[pl.ds((kc * NC + ch) * 12 * T, 12 * T)], raw_recv.at[kc, ch])
            copies_wait(full.at[pl.ds(OWN_AT + kc * 4 * T, 4 * T)], own_sem.at[kc])

            def sum_step(n):
                j = (n // 2 + 1 - bit(me, b)) % 2 * 2 + n % 2

                def tile_step(t):
                    def one(at):
                        return full[pl.ds(at + t * STEP, STEP)].astype(F32)
                    raw = [one(((kc * NC + ch) * 12 + src * 4 + j) * T) for src in range(3)]
                    acc[kc, ch, pl.ds(j * T + t * STEP, STEP)] = (one(OWN_AT + (kc * 4 + j) * T) + raw[2]) + (raw[0] + raw[1])

                loop(0, T // STEP, tile_step)

            loop(0, 4, sum_step)
            put(acc.at[kc, ch, pl.ds(2 * (1 - bit(me, b)) * T, 2 * T)], buf.at[pl.ds((kc * NC + ch) * 2 * T, 2 * T)],
                s2_send, s2_recv.at[kc, ch], flip(me, b))

            @pl.when(ch + 1 < NC)
            def _():
                fetch(ch + 1, kc)

    loop(0, NC, first_sum)

    def near(*dims):
        same = bit(me, dims[0]) == bit(cut, dims[0])
        for dim in dims[1:]:
            same = same & (bit(me, dim) == bit(cut, dim))
        return same

    for kc in range(3):
        a, b, e = axes(kc)

        @pl.when(near(a))
        def _():
            own = full.at[pl.ds(OWN_M + kc * MINI, MINI)]
            copy = pltpu.make_async_copy(lay.at[pl.ds(start_of(cut) - TAIL + extra_at(kc), MINI)], own, m_own)
            copy.start()
            raw = [full.at[pl.ds(RAW_M + (kc * 3 + src) * MINI, MINI)] for src in range(3)]
            copies_wait(full.at[pl.ds(RAW_M + kc * 3 * MINI, 3 * MINI)], m_raw_recv.at[kc])
            copy.wait()
            acc_m[kc] = (own[...].astype(F32) + raw[2][...].astype(F32)) + (raw[0][...].astype(F32) + raw[1][...].astype(F32))

            @pl.when(bit(me, b) != bit(cut, b))
            def _():
                put(acc_m.at[kc], recv2_m.at[kc], m_send.at[kc], m_recv.at[0, kc], flip(me, b))

    def second_sum(ch):
        for kc in range(3):
            a, b, e = axes(kc)
            slot = (kc * NC + ch) * 2 * T
            copies_wait(buf.at[pl.ds(slot, 2 * T)], s2_recv.at[kc, ch])
            for je in ((1 - bit(me, e)), bit(me, e)):
                def tile_step(t):
                    at = pl.ds((2 * bit(me, b) + je) * T + t * STEP, STEP)
                    acc[kc, ch, at] = acc[kc, ch, at] + buf[pl.ds(slot + je * T + t * STEP, STEP)]

                loop(0, T // STEP, tile_step)
            put(acc.at[kc, ch, pl.ds((2 * bit(me, b) + 1 - bit(me, e)) * T, T)], recv3.at[pl.ds((ch * 3 + kc) * T, T)],
                s3_send, s3_recv.at[kc, ch], flip(me, e))

    loop(0, NC, second_sum)
    for kc in range(3):
        a, b, e = axes(kc)

        @pl.when(near(a, b))
        def _():
            copies_wait(recv2_m.at[kc], m_recv.at[0, kc])
            acc_m[kc] = acc_m[kc] + recv2_m[kc]

            @pl.when(bit(me, e) != bit(cut, e))
            def _():
                put(acc_m.at[kc], recv3_m.at[kc], m_send.at[kc], m_recv.at[1, kc], flip(me, e))

    base = HEAD - (SHARE * me - start_of(me))

    def to_flat(lo, hi):
        walk_units(me, True, lo, hi, TO_FLAT, lambda fn, o: fn(buf, flat, tmp, o, WIDE + base + o))

    def flat_rows(t):
        return pl.ds((WIDE + t) * ROWS, ROWS)

    def squares(lo, hi, total):
        def step(t, total):
            for n in range(15):
                x = flat[flat_rows(HEAD + t * 15 + n), :]
                total = total + x * x
            return total
        return lax.fori_loop(lo, hi, step, total)

    def ready(ch):
        return jnp.maximum((ch * 3 * T - 48) // 15, 0)

    def third_sum(ch, total):
        for kc in range(3):
            a, b, e = axes(kc)
            copies_wait(recv3.at[pl.ds((ch * 3 + kc) * T, T)], s3_recv.at[kc, ch])

            def tile_step(t):
                i = pl.ds((ch * 3 + kc) * T + t * STEP, STEP)
                buf[i] = (acc[kc, ch, pl.ds((2 * bit(me, b) + bit(me, e)) * T + t * STEP, STEP)] + recv3[i]) * 0.0625

            loop(0, T // STEP, tile_step)
        to_flat(ch * 3 * T, (ch + 1) * 3 * T)
        return squares(ready(ch), ready(ch + 1), total)

    total = lax.fori_loop(0, NC, third_sum, jnp.zeros(TILE, F32))

    @pl.when(me == cut)
    def _():
        for kc in range(3):
            copies_wait(recv3_m.at[kc], m_recv.at[1, kc])
            buf[pl.ds(extra_at(kc), MINI)] = (acc_m[kc] + recv3_m[kc]) * 0.0625

    to_flat(NC * 3 * T, 2 * WIDE)
    part[me] = squares(ready(NC), SHARE // 15, total)
    loop(1, DEVICES, lambda n: put(part.at[me], part.at[me], n_send, n_recv, lax.rem(me + n, DEVICES)))

    for copy in loads + heads:
        copy.wait()

    def fill(x):
        return jnp.full(TILE, x, F32)

    def power7(x):
        x2 = x * x
        return x2 * x2 * x2 * x

    rate, b1, b2, decay, limit = (fill(hyper[n]) for n in range(5))
    fix1 = 1.0 / (1.0 - power7(b1))
    fix2 = 1.0 / (1.0 - power7(b2))
    others = pl.ds(0, DEVICES - 1)
    copies_wait(part.at[others], n_recv)
    norm_sum = fill(jnp.sum(jnp.sum(part[...], axis=0)))
    clip = jnp.minimum(1.0, limit / (jnp.sqrt(norm_sum) + CLIP_EPS))

    def update(t):
        for n in range(6):
            tile = t * 6 + n
            i = pl.ds(tile * ROWS, ROWS)
            h = flat[flat_rows(tile), :] * clip
            pt = p_buf[i, :]
            mt = b1 * m_buf[i, :] + (1.0 - b1) * h
            vt = b2 * v_buf[i, :] + (1.0 - b2) * (h * h)
            has_decay = SHARE * me - HEAD + tile < TAIL + OFF_N
            u = (mt * fix1) / (jnp.sqrt(vt * fix2) + ADAM_EPS) + jnp.where(has_decay, decay, 0.0) * pt
            m_buf[i, :] = mt
            v_buf[i, :] = vt
            p_buf[i, :] = pt - rate * u

    def send(owner, c, kc, target, recv):
        block = full.at[pl.ds(owner * PUB + (c * 3 + kc) * PC, PC)]
        put(block, block, a_send, recv, target)

    mine = full.at[pl.ds(me * PUB, PUB)]

    def publish(c):
        loop(jnp.where(c == 0, 0, 9 + 50 * c), jnp.minimum(59 + 50 * c, EXT // 6), update)
        walk_units(me, False, c * 3 * PC, (c + 1) * 3 * PC, TO_TILES, lambda fn, o: fn(mine, p_buf, tmp, o, base + o))
        for hop in range(3):
            for kc in range(3):
                dim = axes(kc)[hop]
                send(me, c, kc, flip(me, dim), a_recv.at[c, kc, (0, 1, 3)[hop]])
        for kc in range(3):
            send(me, c, kc, pair, pair_recv)

    loop(0, NA, publish)

    def pass_on(level, c):
        for kc in range(3):
            a, b, e = axes(kc)
            for n in ((1,), (2, 3), (4, 5, 6, 7))[level]:
                owner = me
                for pos, dim in enumerate((a, b, e)):
                    if (n >> pos) & 1:
                        owner = flip(owner, dim)
                copies_wait(full.at[pl.ds(owner * PUB + (c * 3 + kc) * PC, PC)], a_recv.at[c, kc, n - 1])
                if level == 0:
                    send(owner, c, kc, flip(me, b), a_recv.at[c, kc, 2])
                if level < 2:
                    send(owner, c, kc, flip(me, e), a_recv.at[c, kc, n + 3])
                send(owner, c, kc, pair, pair_recv)

    for level in range(3):
        loop(0, NA, functools.partial(pass_on, level))

    copies_wait(full.at[pl.ds(0, DEVICES // 2 * PUB)], pair_recv)
    copies_wait(full.at[pl.ds(0, (DEVICES - 1) * PUB)], a_send)
    copies_wait(full.at[pl.ds(0, RAW_END)], raw_send)
    copies_wait(buf.at[pl.ds(0, 2 * WIN)], s2_send)
    copies_wait(recv3, s3_send)
    copies_wait(part.at[others], n_send)
    extra_sends(lambda kc, to, s, far: copies_wait(lay.at[pl.ds(0, MINI)], m_raw_send.at[kc, to]))
    for kc in range(3):
        a, b, e = axes(kc)

        @pl.when(near(a) & jnp.logical_not(near(a, b, e)))
        def _():
            copies_wait(acc_m.at[kc], m_send.at[kc])


def finish_kernel(gathered, m, v, p, emb, q, k, v_out, out, gate, up, down, norm, mom_out, var_out, mas_out, sem, state_sem):
    starts = [9 * (SHARE * s // 9) - {13: 18, 14: 9}.get(s, 0) for s in range(16)] + [TAIL + LAY]
    state = [pltpu.make_async_copy(src.at[pl.ds(HEAD * ROWS, SHARE * ROWS)], dst, state_sem.at[n])
             for n, (src, dst) in enumerate(((m, mom_out), (v, var_out), (p, mas_out)))]
    for copy in state:
        copy.start()
    for dst, first, n, size in ((emb, 0, EMB, 1), (q, TAIL + OFF_Q, 54, 4), (k, TAIL + OFF_K, 54, 1), (v_out, TAIL + OFF_V, 54, 1),
                                (out, TAIL + OFF_O, 216, 1), (gate, TAIL + OFF_G, 54, 27), (up, TAIL + OFF_U, 54, 27),
                                (down, TAIL + OFF_D, 1458, 1), (norm, TAIL + OFF_N, 30, 1)):
        for s in range(16):
            lo, hi = max(starts[s], first), min(starts[s + 1], first + n * size)
            if lo >= hi:
                continue
            src = s * PUB + lo - starts[s]
            if len(dst.shape) == 3:
                pltpu.make_async_copy(gathered.at[pl.ds(src, hi - lo)], dst.at[pl.ds(lo - first, hi - lo)], sem).start()
                continue
            unit = (lo - first) // size

            def step(i, carry, dst=dst, src=src, unit=unit, size=size):
                l, rb = (unit + i) // 9, lax.rem(unit + i, 9)
                pltpu.make_async_copy(gathered.at[pl.ds(src + i * size, size)], dst.at[l, :, rb], sem).start()
                return carry

            lax.fori_loop(0, (hi - lo) // size, step, 0)
    copies_wait(gathered.at[pl.ds(0, TAIL + LAY)], sem)
    for copy in state:
        copy.wait()


ANY = pl.BlockSpec(memory_space=pl.ANY)
VM = pl.BlockSpec(memory_space=pltpu.VMEM)
DMA = pltpu.SemaphoreType.DMA


def tiled(x):
    rows, cols = x.shape[-2:]
    x = x.reshape(x.shape[:-2] + (rows // ROWS, ROWS, cols // LANES, LANES))
    return jnp.swapaxes(x, -3, -2)


def flat_tiles(x):
    return tiled(x).reshape((-1,) + TILE)


def solution(mesh):
    def local_update(*arrays):
        emb, q, k, v, out, gate, up, down, norms, qk = [a[0] for a in arrays[:GRAD_COUNT]]
        *state, hyper = arrays[GRAD_COUNT:]
        q_t, k_t, v_t, gate_t, up_t = [tiled(jnp.swapaxes(x, 1, 2)) for x in (q, k, v, gate, up)]
        norm = jnp.concatenate([norms.reshape(-1), qk.reshape(-1)]).reshape((-1,) + TILE)
        rows = [x.reshape(SHARE * ROWS, LANES) for x in state]
        args = [flat_tiles(emb), q_t, k_t, v_t, flat_tiles(out), gate_t, up_t, flat_tiles(down), norm] + rows

        *kept, _ = pl.pallas_call(
            step_kernel,
            out_shape=(pltpu.VMEM((DEVICES * PUB,) + TILE, BF16),) + (pltpu.VMEM((EXT * ROWS, LANES), F32),) * 3
            + (jax.ShapeDtypeStruct((LAYP,) + TILE, BF16),),
            in_specs=[ANY] * 12 + [pl.BlockSpec(memory_space=pltpu.SMEM)],
            out_specs=(VM,) * 4 + (ANY,),
            scratch_shapes=[
                pltpu.VMEM((3, NC, 4 * T) + TILE, F32), pltpu.VMEM((2 * WIDE,) + TILE, F32), pltpu.VMEM((WIN,) + TILE, F32),
                pltpu.VMEM((2, LANES, LANES), F32), pltpu.VMEM((DEVICES,) + TILE, F32)]
            + [pltpu.VMEM((3, MINI) + TILE, F32)] * 3
            + [DMA((2,)), DMA((3,)), DMA((2, 3)), DMA((3,)), DMA, DMA((3, NC)), DMA, DMA((3, NC)), DMA, DMA((3, NC)), DMA, DMA,
               DMA((3, 2)), DMA((3,)), DMA, DMA((3,)), DMA((2, 3)), DMA, DMA((NA, 3, 7)), DMA],
            compiler_params=pltpu.CompilerParams(has_side_effects=True, vmem_limit_bytes=GRANT),
            name="step",
        )(*args, hyper)

        emb2, q2, k2, v2, out2, gate2, up2, down2, norm2, *state2 = pl.pallas_call(
            finish_kernel,
            out_shape=tuple(jax.ShapeDtypeStruct(x.shape, x.dtype) for x in args),
            in_specs=[VM] * 4,
            out_specs=(ANY,) * 12,
            scratch_shapes=[DMA, DMA((3,))],
            compiler_params=pltpu.CompilerParams(vmem_limit_bytes=GRANT),
            name="finish",
        )(*[pltpu.with_memory_space_constraint(x, pltpu.VMEM) for x in kept])

        def matrices(x, like):
            x = x.reshape(like.shape[:-2] + (-1, like.shape[-1] // LANES) + TILE)
            return jnp.swapaxes(x, -3, -2).reshape(like.shape)

        def columns(x, like):
            return jnp.swapaxes(matrices(x, jnp.swapaxes(like, 1, 2)), 1, 2)

        flat_norm = norm2.reshape(-1)
        cut = norms.size
        params = (matrices(emb2, emb), columns(q2, q), columns(k2, k), columns(v2, v), matrices(out2, out), columns(gate2, gate), columns(up2, up),
                  matrices(down2, down), flat_norm[:cut].reshape(norms.shape), flat_norm[cut:].reshape(qk.shape))
        return params + tuple(x.reshape(-1) for x in state2)

    in_specs = tuple([P("dp")] * GRAD_COUNT + [P("dp"), P("dp"), P("dp"), P()])
    out_specs = tuple([P()] * GRAD_COUNT + [P("dp"), P("dp"), P("dp")])
    return jax.shard_map(local_update, mesh=mesh, in_specs=in_specs, out_specs=out_specs, check_vma=False)
```

```python
import functools
import jax
import jax.numpy as jnp
from jax import lax
from jax.experimental import pallas as pl
from jax.experimental.pallas import tpu as pltpu
from jax.sharding import PartitionSpec as P

ADAM_EPS = 1e-8
CLIP_EPS = 1e-6
GRAD_COUNT = 10
MESH = pl.DeviceIdType.MESH
F32, BF16 = jnp.float32, jnp.bfloat16

ROWS, LANES = 8, 128
TILE = (ROWS, LANES)
DEVICES = 16
SHARE = 885
WIN = 891
WIDE = 918
CUT = (14, 13)
NC = 9
T = 33
EARLY = 5
STEP = 11
MINI = 9
EMB = 9216
TAIL = 8847
LAY = 5313
LAYP = LAY + MINI
HALF = 2367
HEAD = 21
PUB = 900
NA = 6
PC = 50
EXT = HEAD + SHARE
OFF_Q, OFF_K, OFF_V, OFF_O = 369, 585, 639, 693
OFF_G, OFF_U, OFF_D, OFF_N = 909, 2367, 3825, 5283
DIM = (2, 4, 8)
SHIFT = 88
GRANT = 26400000
RAW_END = 12 * WIN
RAW_M = RAW_END
OWN_M = RAW_M + 9 * MINI
STAGE_AT = OWN_M + 3 * MINI
OWN_AT = STAGE_AT


def start_of(s):
    return 9 * ((SHARE * s) // 9) - jnp.where(s == 13, 18, 0) - jnp.where(s == 14, 9, 0)


def axes(colour):
    return [(colour + n) % 3 for n in range(3)]


def bit(d, dim):
    return (d // DIM[dim]) % 2


def flip(d, dim):
    return d + DIM[dim] * (1 - 2 * bit(d, dim))


def copies_wait(ref, sem):
    pltpu.make_async_copy(ref, ref, sem).wait()


def put(src, dst, send_sem, recv_sem, target):
    copy = pltpu.make_async_remote_copy(
        src_ref=src, dst_ref=dst, send_sem=send_sem, recv_sem=recv_sem, device_id=(target,), device_id_type=MESH)
    copy.start()
    return copy


def loop(lo, hi, fn):
    def step(i, carry):
        fn(i)
        return carry
    lax.fori_loop(lo, hi, step, 0)


def lanes():
    return lax.broadcasted_iota(jnp.int32, TILE, 1)


def gate_segments():
    rows = []
    for kap in range(27):
        pieces, f = [], LANES * kap
        while f < LANES * (kap + 1):
            i, c = f // 216, f % 216
            pieces.append((f - LANES * kap, i, c // LANES))
            f = min(LANES * (kap + 1), 216 * i + (LANES if c < LANES else 216))
        rows.append(pieces)
    return rows


def gate_inverse():
    table = {}
    for kap, pieces in enumerate(gate_segments()):
        ends = [lo for lo, _, _ in pieces[1:]] + [LANES]
        for (lo, i, half), hi in zip(pieces, ends):
            table.setdefault((i, half), []).append((lo, hi, kap))
    return table


def swap_groups(xs, width):
    ids = lanes() // width
    xs, step = list(xs), 1
    while step < len(xs):
        high = (ids // step) % 2 == 1
        for n in range(len(xs)):
            if not n & step:
                lo, hi = xs[n], xs[n + step]
                xs[n] = jnp.where(high, pltpu.roll(hi, width * step, 1), lo)
                xs[n + step] = jnp.where(high, hi, pltpu.roll(lo, LANES - width * step, 1))
        step = 2 * step
    return xs


def turned(win, o):
    return win[pl.ds(o, 16)].reshape(LANES, LANES).T


def rows9_to_flat(win, flat, tmp, o, f):
    for ct in range(9):
        flat[pl.ds(f * ROWS + ct, ROWS, 9), :] = win[o + ct]


def gate_to_flat(win, flat, tmp, o, f):
    for half in range(2):
        tmp[half] = turned(win, o + 16 * half)
    ids = lanes()
    rolled = {}
    for i in range(16):
        for half in range(2):
            rolled[i, half] = pltpu.roll(tmp[half, pl.ds(i, ROWS, 16), :], (SHIFT * i) % LANES, 1)
    for kap, pieces in enumerate(gate_segments()):
        val = None
        for lo, i, half in pieces:
            val = rolled[i, half] if val is None else jnp.where(ids >= lo, rolled[i, half], val)
        flat[pl.ds(f * ROWS + kap, ROWS, 27), :] = val


def q_to_flat(win, flat, tmp, o, f):
    tmp[0] = turned(win, o)
    for kb in range(4):
        xs = swap_groups([tmp[0, pl.ds(32 * kb + i, ROWS, 4), :] for i in range(4)], 32)
        for u in range(4):
            flat[pl.ds((f + 4 * u + kb) * ROWS, ROWS), :] = xs[u]


def kv_to_flat(win, flat, tmp, o, f):
    tmp[0] = turned(win, o)
    xs = swap_groups([tmp[0, pl.ds(i, ROWS, 16), :] for i in range(16)], ROWS)
    for u in range(16):
        flat[pl.ds((f + u) * ROWS, ROWS), :] = xs[u]


def copy_to_flat(win, flat, tmp, o, f):
    flat[pl.ds(f * ROWS, ROWS), :] = win[o]


def rows9_to_tiles(stage, flat, tmp, o, f):
    for ct in range(9):
        stage[o + ct] = flat[pl.ds(f * ROWS + ct, ROWS, 9), :].astype(BF16)


def gate_to_tiles(stage, flat, tmp, o, f):
    ids = lanes()
    rows = [flat[pl.ds(f * ROWS + kap, ROWS, 27), :] for kap in range(27)]
    for (i, half), pieces in gate_inverse().items():
        val = rows[pieces[0][2]]
        for lo, hi, kap in pieces[1:]:
            val = jnp.where((ids >= lo) & (ids < hi), rows[kap], val)
        tmp[half, pl.ds(i, ROWS, 16), :] = pltpu.roll(val, (LANES - SHIFT * i) % LANES, 1)
    stage[pl.ds(o, 16)] = tmp[0].T.reshape(16, ROWS, LANES).astype(BF16)
    stage[pl.ds(o + 16, 11)] = tmp[1].T[:SHIFT].reshape(11, ROWS, LANES).astype(BF16)


def q_to_tiles(stage, flat, tmp, o, f):
    for kb in range(4):
        xs = swap_groups([flat[pl.ds((f + 4 * u + kb) * ROWS, ROWS), :] for u in range(4)], 32)
        for i in range(4):
            tmp[0, pl.ds(32 * kb + i, ROWS, 4), :] = xs[i]
    stage[pl.ds(o, 16)] = tmp[0].T.reshape(16, ROWS, LANES).astype(BF16)


def kv_to_tiles(stage, flat, tmp, o, f):
    xs = swap_groups([flat[pl.ds((f + u) * ROWS, ROWS), :] for u in range(16)], ROWS)
    for i in range(16):
        tmp[0, pl.ds(i, ROWS, 16), :] = xs[i]
    stage[pl.ds(o, 16)] = tmp[0].T.reshape(16, ROWS, LANES).astype(BF16)


def copy_to_tiles(stage, flat, tmp, o, f):
    stage[o] = flat[pl.ds(f * ROWS, ROWS), :].astype(BF16)


TO_FLAT = (rows9_to_flat, gate_to_flat, q_to_flat, kv_to_flat, copy_to_flat)
TO_TILES = (rows9_to_tiles, gate_to_tiles, q_to_tiles, kv_to_tiles, copy_to_tiles)


def walk_units(me, wide, lo, hi, fns, run):
    def pick(table):
        return sum(jnp.where(me == d, n, 0) for d, n in table.items())
    rows9, gate, q, kv, one = fns
    ends = (SHARE * (me + 1) + (8 if wide else 0)) // 9 - (SHARE * me) // 9
    first = jnp.where(me < 10, ends, pick({10: 41, 11: 3, 15: 95}))
    n_gate = pick({11: 32, 12: 33 if wide else 32, 13: 34 if wide else 33, 14: 11})
    second = pick({10: 22 if wide else 21, 14: 67})
    pos = 0
    for count, size, fn, over in ((first, 9, rows9, 0), (pick({10: 14}), 16, q, pick({10: 8})), (pick({10: 7}), 16, kv, pick({10: 4})),
                                  (n_gate, 27, gate, 0), (second, 9, rows9, 0), (pick({15: 30}), 1, one, 0)):
        def done(x):
            return jnp.minimum(jnp.maximum(x - pos + (0 if wide else size - 1), 0) // size, count)

        loop(done(lo), done(hi), lambda u, pos=pos, size=size, fn=fn: run(fn, pos + u * size))
        pos = pos + count * size - over


def norm_rows(fn):
    for l in range(6):
        for ct in range(9):
            fn(0, l, ct * LANES, pl.ds(36 * l + ct, 4, 9))
        for ct in range(2):
            fn(1, l, ct * LANES, pl.ds(216 + 4 * l + ct, 2, 2))


def step_kernel(emb, q, k, v, out, gate, up, down, norms, qk, mom, var, mas, hyper,
                full, m_buf, v_buf, p_buf, lay,
                norms_v, qk_v, acc, buf, recv3, tmp, part, acc_m, recv2_m, recv3_m,
                norm_sem, lay_sem, state_sem, head_sems, own_sem, raw_send, raw_recv, s2_send, s2_recv, s3_send, s3_recv, n_send, n_recv,
                m_raw_send, m_raw_recv, m_own, m_send, m_recv, a_send, a_recv, pair_recv):
    me = lax.axis_index("dp")
    core = me % 2
    pair = me + 1 - 2 * core
    flat = buf.reshape(2 * WIDE * ROWS, LANES)

    state = ((mom, m_buf), (var, v_buf), (mas, p_buf))
    loads = [pltpu.make_async_copy(src, dst.at[pl.ds(HEAD * ROWS, SHARE * ROWS)], state_sem.at[n]) for n, (src, dst) in enumerate(state)]
    for copy in loads:
        copy.start()
    small = [pltpu.make_async_copy(src, dst, norm_sem.at[n]) for n, (src, dst) in enumerate(((norms, norms_v), (qk, qk_v)))]
    for copy in small:
        copy.start()
    barrier = pltpu.get_barrier_semaphore()
    loop(1, DEVICES, lambda n: pl.semaphore_signal(barrier, inc=1, device_id=(lax.rem(me + n, DEVICES),), device_id_type=MESH))
    pl.semaphore_wait(barrier, DEVICES - 1)
    heads = [put(src.at[pl.ds((SHARE - HEAD) * ROWS, HEAD * ROWS)], dst.at[pl.ds(0, HEAD * ROWS)], head_sems.at[0, n], head_sems.at[1, n],
                 lax.rem(me + 1, DEVICES)) for n, (src, dst) in enumerate(state)]

    def raw_at(kc, ch, src, j):
        return full.at[pl.ds(((kc * NC + ch) * 12 + src * 4 + j) * T, T)]

    def share_tiles(s, pos, n, fn):
        first = start_of(s) + pos

        @pl.when(s < 10)
        def _():
            fn(emb.at[pl.ds(first, n)])

        @pl.when(s >= 10)
        def _():
            fn(lay.at[pl.ds(first - TAIL, n)])

    def scatter(ch, with_emb, with_lay):
        def one(s, kc, src, j, target):
            @pl.when(jnp.where(s < 10, with_emb, with_lay) == 1)
            def _():
                share_tiles(s, (ch * 3 + kc) * T, T, lambda ref: put(ref, raw_at(kc, ch, src, j), raw_send, raw_recv.at[kc, ch], target))

        for kc in range(3):
            a, b, e = axes(kc)
            far = flip(me, a)

            def share_step(j):
                near = (j // 2) * DIM[b] + (j % 2) * DIM[e]
                for to in range(2):
                    one((1 - bit(me, a)) * DIM[a] + near + to, kc, core, j, far - core + to)
                one(bit(me, a) * DIM[a] + near + 1 - core, kc, 2, j, pair)

            loop(0, 4, share_step)

    rows2 = tmp.reshape(2 * LANES, LANES)

    def norm_row(which, l, lane, at):
        rows2[at, :] = (norms_v, qk_v)[which][l, :, lane:lane + LANES].astype(F32)

    loop(0, EARLY, lambda ch: scatter(ch, 1, 0))
    for copy in small:
        copy.wait()
    norm_rows(norm_row)
    for lo, whole, split in ((0, ((emb.at[pl.ds(TAIL, OFF_Q)], 0), (out, OFF_O)), ((q, OFF_Q, 4), (k, OFF_K, 1), (v, OFF_V, 1), (gate, OFF_G, 27))),
                             (HALF, ((down, OFF_D),), ((up, OFF_U, 27),))):
        n = HALF if lo == 0 else LAY - HALF
        stage = full.at[pl.ds(STAGE_AT, n)]
        for src, off in whole:
            pltpu.make_async_copy(src, full.at[pl.ds(STAGE_AT + off - lo, src.shape[0])], lay_sem.at[0]).start()

        def load(i):
            for src, off, size in split:
                pltpu.make_async_copy(src.at[i // 9, :, lax.rem(i, 9)], full.at[pl.ds(STAGE_AT + off - lo + i * size, size)], lay_sem.at[0]).start()

        loop(0, 54, load)
        if lo == 0:
            copies_wait(stage, lay_sem.at[0])
        else:
            copies_wait(full.at[pl.ds(STAGE_AT, n - 30)], lay_sem.at[0])
            full[pl.ds(STAGE_AT + n - 30, 30)] = rows2[pl.ds(0, 30 * ROWS), :].reshape((30,) + TILE).astype(BF16)
        save = pltpu.make_async_copy(stage, lay.at[pl.ds(lo, n)], lay_sem.at[1])
        save.start()
        save.wait()
    loop(0, NC, lambda ch: scatter(ch, jnp.where(ch < EARLY, 0, 1), 1))

    cut = jnp.where(core == 0, *CUT)

    def extra_at(kc):
        return WIN + kc * MINI

    def extra_sends(fn):
        for kc in range(3):
            for to, s in enumerate(CUT):
                far = bit(me, kc) != bit(s, kc)

                @pl.when(far | (core != to))
                def _():
                    fn(kc, to, s, far)

    def extra_send(kc, to, s, far):
        put(lay.at[pl.ds(start_of(s) - TAIL + extra_at(kc), MINI)],
            full.at[pl.ds(RAW_M + (kc * 3 + jnp.where(far, core, 2)) * MINI, MINI)], m_raw_send.at[kc, to], m_raw_recv.at[kc],
            jnp.where(far, flip(me, kc), me) - core + to)

    extra_sends(extra_send)

    def fetch(ch, kc):
        a, b, e = axes(kc)
        for j in range(4):
            s = bit(me, a) * DIM[a] + (j // 2) * DIM[b] + (j % 2) * DIM[e] + core
            share_tiles(s, (ch * 3 + kc) * T, T,
                        lambda ref: pltpu.make_async_copy(ref, full.at[pl.ds(OWN_AT + (kc * 4 + j) * T, T)], own_sem.at[kc]).start())

    for kc in range(3):
        fetch(0, kc)

    def first_sum(ch):
        for kc in range(3):
            a, b, e = axes(kc)
            copies_wait(full.at[pl.ds((kc * NC + ch) * 12 * T, 12 * T)], raw_recv.at[kc, ch])
            copies_wait(full.at[pl.ds(OWN_AT + kc * 4 * T, 4 * T)], own_sem.at[kc])

            def sum_step(n):
                j = (n // 2 + 1 - bit(me, b)) % 2 * 2 + n % 2

                def tile_step(t):
                    def one(at):
                        return full[pl.ds(at + t * STEP, STEP)].astype(F32)
                    raw = [one(((kc * NC + ch) * 12 + src * 4 + j) * T) for src in range(3)]
                    acc[kc, ch, pl.ds(j * T + t * STEP, STEP)] = (one(OWN_AT + (kc * 4 + j) * T) + raw[2]) + (raw[0] + raw[1])

                loop(0, T // STEP, tile_step)

            loop(0, 4, sum_step)
            put(acc.at[kc, ch, pl.ds(2 * (1 - bit(me, b)) * T, 2 * T)], buf.at[pl.ds((kc * NC + ch) * 2 * T, 2 * T)],
                s2_send, s2_recv.at[kc, ch], flip(me, b))

            @pl.when(ch + 1 < NC)
            def _():
                fetch(ch + 1, kc)

    loop(0, NC, first_sum)

    def near(*dims):
        same = bit(me, dims[0]) == bit(cut, dims[0])
        for dim in dims[1:]:
            same = same & (bit(me, dim) == bit(cut, dim))
        return same

    for kc in range(3):
        a, b, e = axes(kc)

        @pl.when(near(a))
        def _():
            own = full.at[pl.ds(OWN_M + kc * MINI, MINI)]
            copy = pltpu.make_async_copy(lay.at[pl.ds(start_of(cut) - TAIL + extra_at(kc), MINI)], own, m_own)
            copy.start()
            raw = [full.at[pl.ds(RAW_M + (kc * 3 + src) * MINI, MINI)] for src in range(3)]
            copies_wait(full.at[pl.ds(RAW_M + kc * 3 * MINI, 3 * MINI)], m_raw_recv.at[kc])
            copy.wait()
            acc_m[kc] = (own[...].astype(F32) + raw[2][...].astype(F32)) + (raw[0][...].astype(F32) + raw[1][...].astype(F32))

            @pl.when(bit(me, b) != bit(cut, b))
            def _():
                put(acc_m.at[kc], recv2_m.at[kc], m_send.at[kc], m_recv.at[0, kc], flip(me, b))

    def second_sum(ch):
        for kc in range(3):
            a, b, e = axes(kc)
            slot = (kc * NC + ch) * 2 * T
            copies_wait(buf.at[pl.ds(slot, 2 * T)], s2_recv.at[kc, ch])
            for je in ((1 - bit(me, e)), bit(me, e)):
                def tile_step(t):
                    at = pl.ds((2 * bit(me, b) + je) * T + t * STEP, STEP)
                    acc[kc, ch, at] = acc[kc, ch, at] + buf[pl.ds(slot + je * T + t * STEP, STEP)]

                loop(0, T // STEP, tile_step)
            put(acc.at[kc, ch, pl.ds((2 * bit(me, b) + 1 - bit(me, e)) * T, T)], recv3.at[pl.ds((ch * 3 + kc) * T, T)],
                s3_send, s3_recv.at[kc, ch], flip(me, e))

    loop(0, NC, second_sum)
    for kc in range(3):
        a, b, e = axes(kc)

        @pl.when(near(a, b))
        def _():
            copies_wait(recv2_m.at[kc], m_recv.at[0, kc])
            acc_m[kc] = acc_m[kc] + recv2_m[kc]

            @pl.when(bit(me, e) != bit(cut, e))
            def _():
                put(acc_m.at[kc], recv3_m.at[kc], m_send.at[kc], m_recv.at[1, kc], flip(me, e))

    base = HEAD - (SHARE * me - start_of(me))

    def to_flat(lo, hi):
        walk_units(me, True, lo, hi, TO_FLAT, lambda fn, o: fn(buf, flat, tmp, o, WIDE + base + o))

    def flat_rows(t):
        return pl.ds((WIDE + t) * ROWS, ROWS)

    def squares(lo, hi, total):
        def step(t, total):
            for n in range(15):
                x = flat[flat_rows(HEAD + t * 15 + n), :]
                total = total + x * x
            return total
        return lax.fori_loop(lo, hi, step, total)

    def ready(ch):
        return jnp.maximum((ch * 3 * T - 48) // 15, 0)

    def third_sum(ch, total):
        for kc in range(3):
            a, b, e = axes(kc)
            copies_wait(recv3.at[pl.ds((ch * 3 + kc) * T, T)], s3_recv.at[kc, ch])

            def tile_step(t):
                i = pl.ds((ch * 3 + kc) * T + t * STEP, STEP)
                buf[i] = (acc[kc, ch, pl.ds((2 * bit(me, b) + bit(me, e)) * T + t * STEP, STEP)] + recv3[i]) * 0.0625

            loop(0, T // STEP, tile_step)
        to_flat(ch * 3 * T, (ch + 1) * 3 * T)
        return squares(ready(ch), ready(ch + 1), total)

    total = lax.fori_loop(0, NC, third_sum, jnp.zeros(TILE, F32))

    @pl.when(me == cut)
    def _():
        for kc in range(3):
            copies_wait(recv3_m.at[kc], m_recv.at[1, kc])
            buf[pl.ds(extra_at(kc), MINI)] = (acc_m[kc] + recv3_m[kc]) * 0.0625

    to_flat(NC * 3 * T, 2 * WIDE)
    part[me] = squares(ready(NC), SHARE // 15, total)
    loop(1, DEVICES, lambda n: put(part.at[me], part.at[me], n_send, n_recv, lax.rem(me + n, DEVICES)))

    for copy in loads + heads:
        copy.wait()

    def fill(x):
        return jnp.full(TILE, x, F32)

    def power7(x):
        x2 = x * x
        return x2 * x2 * x2 * x

    rate, b1, b2, decay, limit = (fill(hyper[n]) for n in range(5))
    fix1 = 1.0 / (1.0 - power7(b1))
    fix2 = 1.0 / (1.0 - power7(b2))
    others = pl.ds(0, DEVICES - 1)
    copies_wait(part.at[others], n_recv)
    norm_sum = fill(jnp.sum(jnp.sum(part[...], axis=0)))
    clip = jnp.minimum(1.0, limit / (jnp.sqrt(norm_sum) + CLIP_EPS))

    def update(t):
        for n in range(6):
            tile = t * 6 + n
            i = pl.ds(tile * ROWS, ROWS)
            h = flat[flat_rows(tile), :] * clip
            pt = p_buf[i, :]
            mt = b1 * m_buf[i, :] + (1.0 - b1) * h
            vt = b2 * v_buf[i, :] + (1.0 - b2) * (h * h)
            has_decay = SHARE * me - HEAD + tile < TAIL + OFF_N
            u = (mt * fix1) / (jnp.sqrt(vt * fix2) + ADAM_EPS) + jnp.where(has_decay, decay, 0.0) * pt
            m_buf[i, :] = mt
            v_buf[i, :] = vt
            p_buf[i, :] = pt - rate * u

    def send(owner, c, kc, target, recv):
        block = full.at[pl.ds(owner * PUB + (c * 3 + kc) * PC, PC)]
        put(block, block, a_send, recv, target)

    mine = full.at[pl.ds(me * PUB, PUB)]

    def publish(c):
        loop(jnp.where(c == 0, 0, 9 + PC // 2 * c), jnp.minimum(9 + PC // 2 * (c + 1), EXT // 6), update)
        walk_units(me, False, c * 3 * PC, (c + 1) * 3 * PC, TO_TILES, lambda fn, o: fn(mine, p_buf, tmp, o, base + o))
        for hop in range(3):
            for kc in range(3):
                dim = axes(kc)[hop]
                send(me, c, kc, flip(me, dim), a_recv.at[c, kc, (0, 1, 3)[hop]])
        for kc in range(3):
            send(me, c, kc, pair, pair_recv)

    loop(0, NA, publish)

    def pass_on(level, c):
        for kc in range(3):
            a, b, e = axes(kc)
            for n in ((1,), (2, 3), (4, 5, 6, 7))[level]:
                owner = me
                for pos, dim in enumerate((a, b, e)):
                    if (n >> pos) & 1:
                        owner = flip(owner, dim)
                copies_wait(full.at[pl.ds(owner * PUB + (c * 3 + kc) * PC, PC)], a_recv.at[c, kc, n - 1])
                if level == 0:
                    send(owner, c, kc, flip(me, b), a_recv.at[c, kc, 2])
                if level < 2:
                    send(owner, c, kc, flip(me, e), a_recv.at[c, kc, n + 3])
                send(owner, c, kc, pair, pair_recv)

    for level in range(3):
        loop(0, NA, functools.partial(pass_on, level))

    copies_wait(full.at[pl.ds(0, DEVICES // 2 * PUB)], pair_recv)
    copies_wait(full.at[pl.ds(0, (DEVICES - 1) * PUB)], a_send)
    copies_wait(full.at[pl.ds(0, RAW_END)], raw_send)
    copies_wait(buf.at[pl.ds(0, 2 * WIN)], s2_send)
    copies_wait(recv3, s3_send)
    copies_wait(part.at[others], n_send)
    extra_sends(lambda kc, to, s, far: copies_wait(lay.at[pl.ds(0, MINI)], m_raw_send.at[kc, to]))
    for kc in range(3):
        a, b, e = axes(kc)

        @pl.when(near(a) & jnp.logical_not(near(a, b, e)))
        def _():
            copies_wait(acc_m.at[kc], m_send.at[kc])


def finish_kernel(gathered, m, v, p, emb, q, k, v_out, out, gate, up, down, norms, qk, mom_out, var_out, mas_out, norms_v, qk_v, rows2, sem, state_sem):
    starts = [9 * (SHARE * s // 9) - {13: 18, 14: 9}.get(s, 0) for s in range(16)] + [TAIL + LAY]
    state = [pltpu.make_async_copy(src.at[pl.ds(HEAD * ROWS, SHARE * ROWS)], dst, state_sem.at[n])
             for n, (src, dst) in enumerate(((m, mom_out), (v, var_out), (p, mas_out)))]
    for copy in state:
        copy.start()
    for dst, first, n, size in ((emb, 0, EMB, 1), (q, TAIL + OFF_Q, 54, 4), (k, TAIL + OFF_K, 54, 1), (v_out, TAIL + OFF_V, 54, 1),
                                (out, TAIL + OFF_O, 216, 1), (gate, TAIL + OFF_G, 54, 27), (up, TAIL + OFF_U, 54, 27),
                                (down, TAIL + OFF_D, 1458, 1)):
        for s in range(16):
            lo, hi = max(starts[s], first), min(starts[s + 1], first + n * size)
            if lo >= hi:
                continue
            src = s * PUB + lo - starts[s]
            if len(dst.shape) == 3:
                pltpu.make_async_copy(gathered.at[pl.ds(src, hi - lo)], dst.at[pl.ds(lo - first, hi - lo)], sem).start()
                continue
            unit = (lo - first) // size

            def step(i, carry, dst=dst, src=src, unit=unit, size=size):
                l, rb = (unit + i) // 9, lax.rem(unit + i, 9)
                pltpu.make_async_copy(gathered.at[pl.ds(src + i * size, size)], dst.at[l, :, rb], sem).start()
                return carry

            lax.fori_loop(0, (hi - lo) // size, step, 0)
    rows2[...] = gathered[pl.ds(15 * PUB + OFF_N - 4428, 30)].astype(F32).reshape(30 * ROWS, LANES)

    def norm_row(which, l, lane, at):
        (norms_v, qk_v)[which][l, :, lane:lane + LANES] = rows2[at, :].astype(BF16)

    norm_rows(norm_row)
    small = [pltpu.make_async_copy(src, dst, state_sem.at[3 + n]) for n, (src, dst) in enumerate(((norms_v, norms), (qk_v, qk)))]
    for copy in small:
        copy.start()
    copies_wait(gathered.at[pl.ds(0, TAIL + OFF_N)], sem)
    for copy in state + small:
        copy.wait()


ANY = pl.BlockSpec(memory_space=pl.ANY)
VM = pl.BlockSpec(memory_space=pltpu.VMEM)
DMA = pltpu.SemaphoreType.DMA


def tiled(x):
    rows, cols = x.shape[-2:]
    x = x.reshape(x.shape[:-2] + (rows // ROWS, ROWS, cols // LANES, LANES))
    return jnp.swapaxes(x, -3, -2)


def flat_tiles(x):
    return tiled(x).reshape((-1,) + TILE)


def solution(mesh):
    def local_update(*arrays):
        emb, q, k, v, out, gate, up, down, norms, qk = [a[0] for a in arrays[:GRAD_COUNT]]
        *state, hyper = arrays[GRAD_COUNT:]
        q_t, k_t, v_t, gate_t, up_t = [tiled(jnp.swapaxes(x, 1, 2)) for x in (q, k, v, gate, up)]
        small = [pltpu.VMEM(x.shape, BF16) for x in (norms, qk)]
        rows = [x.reshape(SHARE * ROWS, LANES) for x in state]
        args = [flat_tiles(emb), q_t, k_t, v_t, flat_tiles(out), gate_t, up_t, flat_tiles(down), norms, qk] + rows

        *kept, _ = pl.pallas_call(
            step_kernel,
            out_shape=(pltpu.VMEM((DEVICES * PUB,) + TILE, BF16),) + (pltpu.VMEM((EXT * ROWS, LANES), F32),) * 3
            + (jax.ShapeDtypeStruct((LAYP,) + TILE, BF16),),
            in_specs=[ANY] * 13 + [pl.BlockSpec(memory_space=pltpu.SMEM)],
            out_specs=(VM,) * 4 + (ANY,),
            scratch_shapes=small + [
                pltpu.VMEM((3, NC, 4 * T) + TILE, F32), pltpu.VMEM((2 * WIDE,) + TILE, F32), pltpu.VMEM((WIN,) + TILE, F32),
                pltpu.VMEM((2, LANES, LANES), F32), pltpu.VMEM((DEVICES,) + TILE, F32)]
            + [pltpu.VMEM((3, MINI) + TILE, F32)] * 3
            + [DMA((2,)), DMA((2,)), DMA((3,)), DMA((2, 3)), DMA((3,)), DMA, DMA((3, NC)), DMA, DMA((3, NC)), DMA, DMA((3, NC)), DMA, DMA,
               DMA((3, 2)), DMA((3,)), DMA, DMA((3,)), DMA((2, 3)), DMA, DMA((NA, 3, 7)), DMA],
            compiler_params=pltpu.CompilerParams(collective_id=0, has_side_effects=True, vmem_limit_bytes=GRANT),
            name="step",
        )(*args, hyper)

        emb2, q2, k2, v2, out2, gate2, up2, down2, norms2, qk2, *state2 = pl.pallas_call(
            finish_kernel,
            out_shape=tuple(jax.ShapeDtypeStruct(x.shape, x.dtype) for x in args),
            in_specs=[VM] * 4,
            out_specs=(ANY,) * 13,
            scratch_shapes=small + [pltpu.VMEM((30 * ROWS, LANES), F32), DMA, DMA((5,))],
            compiler_params=pltpu.CompilerParams(vmem_limit_bytes=GRANT),
            name="finish",
        )(*[pltpu.with_memory_space_constraint(x, pltpu.VMEM) for x in kept])

        def matrices(x, like):
            x = x.reshape(like.shape[:-2] + (-1, like.shape[-1] // LANES) + TILE)
            return jnp.swapaxes(x, -3, -2).reshape(like.shape)

        def columns(x, like):
            return jnp.swapaxes(matrices(x, jnp.swapaxes(like, 1, 2)), 1, 2)

        params = (matrices(emb2, emb), columns(q2, q), columns(k2, k), columns(v2, v), matrices(out2, out), columns(gate2, gate), columns(up2, up),
                  matrices(down2, down), norms2, qk2)
        return params + tuple(x.reshape(-1) for x in state2)

    in_specs = tuple([P("dp")] * GRAD_COUNT + [P("dp"), P("dp"), P("dp"), P()])
    out_specs = tuple([P()] * GRAD_COUNT + [P("dp"), P("dp"), P("dp")])
    return jax.shard_map(local_update, mesh=mesh, in_specs=in_specs, out_specs=out_specs, check_vma=False)
```

```python
import functools
import jax
import jax.numpy as jnp
from jax import lax
from jax.experimental import pallas as pl
from jax.experimental.pallas import tpu as pltpu
from jax.sharding import PartitionSpec as P

ADAM_EPS = 1e-8
CLIP_EPS = 1e-6
GRAD_COUNT = 10
MESH = pl.DeviceIdType.MESH
F32, BF16 = jnp.float32, jnp.bfloat16

ROWS, LANES = 8, 128
TILE = (ROWS, LANES)
DEVICES = 16
SHARE = 885
WIN = 891
WIDE = 918
CUT = (14, 13)
NC = 9
T = 33
EARLY = 5
STEP = 11
MINI = 9
EMB = 9216
TAIL = 8847
LAY = 5313
LAYP = LAY + MINI
HALF = 2367
HEAD = 21
PUB = 900
NA = 6
PC = 50
EXT = HEAD + SHARE
OFF_Q, OFF_K, OFF_V, OFF_O = 369, 585, 639, 693
OFF_G, OFF_U, OFF_D, OFF_N = 909, 2367, 3825, 5283
DIM = (2, 4, 8)
SHIFT = 88
GRANT = 26400000
RAW_END = 12 * WIN
RAW_M = RAW_END
OWN_M = RAW_M + 9 * MINI
STAGE_AT = OWN_M + 3 * MINI
OWN_AT = STAGE_AT


def start_of(s):
    return 9 * ((SHARE * s) // 9) - jnp.where(s == 13, 18, 0) - jnp.where(s == 14, 9, 0)


def axes(colour):
    return [(colour + n) % 3 for n in range(3)]


def bit(d, dim):
    return (d // DIM[dim]) % 2


def flip(d, dim):
    return d + DIM[dim] * (1 - 2 * bit(d, dim))


def copies_wait(ref, sem):
    pltpu.make_async_copy(ref, ref, sem).wait()


def put(src, dst, send_sem, recv_sem, target):
    copy = pltpu.make_async_remote_copy(
        src_ref=src, dst_ref=dst, send_sem=send_sem, recv_sem=recv_sem, device_id=(target,), device_id_type=MESH)
    copy.start()
    return copy


def loop(lo, hi, fn):
    def step(i, carry):
        fn(i)
        return carry
    lax.fori_loop(lo, hi, step, 0)


def lanes():
    return lax.broadcasted_iota(jnp.int32, TILE, 1)


def gate_segments():
    rows = []
    for kap in range(27):
        pieces, f = [], LANES * kap
        while f < LANES * (kap + 1):
            i, c = f // 216, f % 216
            pieces.append((f - LANES * kap, i, c // LANES))
            f = min(LANES * (kap + 1), 216 * i + (LANES if c < LANES else 216))
        rows.append(pieces)
    return rows


def gate_inverse():
    table = {}
    for kap, pieces in enumerate(gate_segments()):
        ends = [lo for lo, _, _ in pieces[1:]] + [LANES]
        for (lo, i, half), hi in zip(pieces, ends):
            table.setdefault((i, half), []).append((lo, hi, kap))
    return table


def swap_groups(xs, width):
    ids = lanes() // width
    xs, step = list(xs), 1
    while step < len(xs):
        high = (ids // step) % 2 == 1
        for n in range(len(xs)):
            if not n & step:
                lo, hi = xs[n], xs[n + step]
                xs[n] = jnp.where(high, pltpu.roll(hi, width * step, 1), lo)
                xs[n + step] = jnp.where(high, hi, pltpu.roll(lo, LANES - width * step, 1))
        step = 2 * step
    return xs


def turned(win, o):
    return win[pl.ds(o, 16)].reshape(LANES, LANES).T


def rows9_to_flat(win, flat, tmp, o, f):
    for ct in range(9):
        flat[pl.ds(f * ROWS + ct, ROWS, 9), :] = win[o + ct]


def gate_to_flat(win, flat, tmp, o, f):
    for half in range(2):
        tmp[half] = turned(win, o + 16 * half)
    ids = lanes()
    rolled = {}
    for i in range(16):
        for half in range(2):
            rolled[i, half] = pltpu.roll(tmp[half, pl.ds(i, ROWS, 16), :], (SHIFT * i) % LANES, 1)
    for kap, pieces in enumerate(gate_segments()):
        val = None
        for lo, i, half in pieces:
            val = rolled[i, half] if val is None else jnp.where(ids >= lo, rolled[i, half], val)
        flat[pl.ds(f * ROWS + kap, ROWS, 27), :] = val


def q_to_flat(win, flat, tmp, o, f):
    tmp[0] = turned(win, o)
    for kb in range(4):
        xs = swap_groups([tmp[0, pl.ds(32 * kb + i, ROWS, 4), :] for i in range(4)], 32)
        for u in range(4):
            flat[pl.ds((f + 4 * u + kb) * ROWS, ROWS), :] = xs[u]


def kv_to_flat(win, flat, tmp, o, f):
    tmp[0] = turned(win, o)
    xs = swap_groups([tmp[0, pl.ds(i, ROWS, 16), :] for i in range(16)], ROWS)
    for u in range(16):
        flat[pl.ds((f + u) * ROWS, ROWS), :] = xs[u]


def copy_to_flat(win, flat, tmp, o, f):
    flat[pl.ds(f * ROWS, ROWS), :] = win[o]


def rows9_to_tiles(stage, flat, tmp, o, f):
    for ct in range(9):
        stage[o + ct] = flat[pl.ds(f * ROWS + ct, ROWS, 9), :].astype(BF16)


def gate_to_tiles(stage, flat, tmp, o, f):
    ids = lanes()
    rows = [flat[pl.ds(f * ROWS + kap, ROWS, 27), :] for kap in range(27)]
    for (i, half), pieces in gate_inverse().items():
        val = rows[pieces[0][2]]
        for lo, hi, kap in pieces[1:]:
            val = jnp.where((ids >= lo) & (ids < hi), rows[kap], val)
        tmp[half, pl.ds(i, ROWS, 16), :] = pltpu.roll(val, (LANES - SHIFT * i) % LANES, 1)
    stage[pl.ds(o, 16)] = tmp[0].T.reshape(16, ROWS, LANES).astype(BF16)
    stage[pl.ds(o + 16, 11)] = tmp[1].T[:SHIFT].reshape(11, ROWS, LANES).astype(BF16)


def q_to_tiles(stage, flat, tmp, o, f):
    for kb in range(4):
        xs = swap_groups([flat[pl.ds((f + 4 * u + kb) * ROWS, ROWS), :] for u in range(4)], 32)
        for i in range(4):
            tmp[0, pl.ds(32 * kb + i, ROWS, 4), :] = xs[i]
    stage[pl.ds(o, 16)] = tmp[0].T.reshape(16, ROWS, LANES).astype(BF16)


def kv_to_tiles(stage, flat, tmp, o, f):
    xs = swap_groups([flat[pl.ds((f + u) * ROWS, ROWS), :] for u in range(16)], ROWS)
    for i in range(16):
        tmp[0, pl.ds(i, ROWS, 16), :] = xs[i]
    stage[pl.ds(o, 16)] = tmp[0].T.reshape(16, ROWS, LANES).astype(BF16)


def copy_to_tiles(stage, flat, tmp, o, f):
    stage[o] = flat[pl.ds(f * ROWS, ROWS), :].astype(BF16)


TO_FLAT = (rows9_to_flat, gate_to_flat, q_to_flat, kv_to_flat, copy_to_flat)
TO_TILES = (rows9_to_tiles, gate_to_tiles, q_to_tiles, kv_to_tiles, copy_to_tiles)


def walk_units(me, wide, lo, hi, fns, run):
    def pick(table):
        return sum(jnp.where(me == d, n, 0) for d, n in table.items())
    rows9, gate, q, kv, one = fns
    ends = (SHARE * (me + 1) + (8 if wide else 0)) // 9 - (SHARE * me) // 9
    first = jnp.where(me < 10, ends, pick({10: 41, 11: 3, 15: 95}))
    n_gate = pick({11: 32, 12: 33 if wide else 32, 13: 34 if wide else 33, 14: 11})
    second = pick({10: 22 if wide else 21, 14: 67})
    pos = 0
    for count, size, fn, over in ((first, 9, rows9, 0), (pick({10: 14}), 16, q, pick({10: 8})), (pick({10: 7}), 16, kv, pick({10: 4})),
                                  (n_gate, 27, gate, 0), (second, 9, rows9, 0), (pick({15: 30}), 1, one, 0)):
        def done(x):
            return jnp.minimum(jnp.maximum(x - pos + (0 if wide else size - 1), 0) // size, count)

        loop(done(lo), done(hi), lambda u, pos=pos, size=size, fn=fn: run(fn, pos + u * size))
        pos = pos + count * size - over


def norm_rows(fn):
    for l in range(6):
        for ct in range(9):
            fn(0, l, ct * LANES, pl.ds(36 * l + ct, 4, 9))
        for ct in range(2):
            fn(1, l, ct * LANES, pl.ds(216 + 4 * l + ct, 2, 2))


def step_kernel(emb, q, k, v, out, gate, up, down, norms, qk, mom, var, mas, hyper,
                full, m_buf, v_buf, p_buf, lay,
                norms_v, qk_v, acc, buf, recv3, tmp, part, acc_m, recv2_m, recv3_m,
                norm_sem, lay_sem, state_sem, head_sems, own_sem, raw_send, raw_recv, s2_send, s2_recv, s3_send, s3_recv, n_send, n_recv,
                m_raw_send, m_raw_recv, m_own, m_send, m_recv, a_send, a_recv, pair_recv):
    me = lax.axis_index("dp")
    core = me % 2
    pair = me + 1 - 2 * core
    flat = buf.reshape(2 * WIDE * ROWS, LANES)

    small = [pltpu.make_async_copy(src, dst, norm_sem.at[n]) for n, (src, dst) in enumerate(((norms, norms_v), (qk, qk_v)))]
    for copy in small:
        copy.start()
    barrier = pltpu.get_barrier_semaphore()
    peers = [pair] + [flip(me, dim) + to for dim in range(3) for to in (0, 1 - 2 * core)]
    for peer in peers:
        pl.semaphore_signal(barrier, inc=1, device_id=(peer,), device_id_type=MESH)
    pl.semaphore_wait(barrier, len(peers))

    def raw_at(kc, ch, src, j):
        return full.at[pl.ds(((kc * NC + ch) * 12 + src * 4 + j) * T, T)]

    def share_tiles(s, pos, n, fn):
        first = start_of(s) + pos

        @pl.when(s < 10)
        def _():
            fn(emb.at[pl.ds(first, n)])

        @pl.when(s >= 10)
        def _():
            fn(lay.at[pl.ds(first - TAIL, n)])

    def scatter(ch, with_emb, with_lay):
        def one(s, kc, src, j, target):
            @pl.when(jnp.where(s < 10, with_emb, with_lay) == 1)
            def _():
                share_tiles(s, (ch * 3 + kc) * T, T, lambda ref: put(ref, raw_at(kc, ch, src, j), raw_send, raw_recv.at[kc, ch], target))

        for kc in range(3):
            a, b, e = axes(kc)
            far = flip(me, a)

            def share_step(j):
                near = (j // 2) * DIM[b] + (j % 2) * DIM[e]
                for to in range(2):
                    one((1 - bit(me, a)) * DIM[a] + near + to, kc, core, j, far - core + to)
                one(bit(me, a) * DIM[a] + near + 1 - core, kc, 2, j, pair)

            loop(0, 4, share_step)

    rows2 = tmp.reshape(2 * LANES, LANES)

    def norm_row(which, l, lane, at):
        rows2[at, :] = (norms_v, qk_v)[which][l, :, lane:lane + LANES].astype(F32)

    loop(0, EARLY, lambda ch: scatter(ch, 1, 0))
    for copy in small:
        copy.wait()
    norm_rows(norm_row)
    for lo, whole, split in ((0, ((emb.at[pl.ds(TAIL, OFF_Q)], 0), (out, OFF_O)), ((q, OFF_Q, 4), (k, OFF_K, 1), (v, OFF_V, 1), (gate, OFF_G, 27))),
                             (HALF, ((down, OFF_D),), ((up, OFF_U, 27),))):
        n = HALF if lo == 0 else LAY - HALF
        stage = full.at[pl.ds(STAGE_AT, n)]
        for src, off in whole:
            pltpu.make_async_copy(src, full.at[pl.ds(STAGE_AT + off - lo, src.shape[0])], lay_sem.at[0]).start()

        def load(i):
            for src, off, size in split:
                pltpu.make_async_copy(src.at[i // 9, :, lax.rem(i, 9)], full.at[pl.ds(STAGE_AT + off - lo + i * size, size)], lay_sem.at[0]).start()

        loop(0, 54, load)
        if lo == 0:
            copies_wait(stage, lay_sem.at[0])
        else:
            copies_wait(full.at[pl.ds(STAGE_AT, n - 30)], lay_sem.at[0])
            full[pl.ds(STAGE_AT + n - 30, 30)] = rows2[pl.ds(0, 30 * ROWS), :].reshape((30,) + TILE).astype(BF16)
        save = pltpu.make_async_copy(stage, lay.at[pl.ds(lo, n)], lay_sem.at[1])
        save.start()
        save.wait()
    loop(0, NC, lambda ch: scatter(ch, jnp.where(ch < EARLY, 0, 1), 1))
    state = ((mom, m_buf), (var, v_buf), (mas, p_buf))
    loads = [pltpu.make_async_copy(src, dst.at[pl.ds(HEAD * ROWS, SHARE * ROWS)], state_sem.at[n]) for n, (src, dst) in enumerate(state)]
    for copy in loads:
        copy.start()

    cut = jnp.where(core == 0, *CUT)

    def extra_at(kc):
        return WIN + kc * MINI

    def extra_sends(fn):
        for kc in range(3):
            for to, s in enumerate(CUT):
                far = bit(me, kc) != bit(s, kc)

                @pl.when(far | (core != to))
                def _():
                    fn(kc, to, s, far)

    def extra_send(kc, to, s, far):
        put(lay.at[pl.ds(start_of(s) - TAIL + extra_at(kc), MINI)],
            full.at[pl.ds(RAW_M + (kc * 3 + jnp.where(far, core, 2)) * MINI, MINI)], m_raw_send.at[kc, to], m_raw_recv.at[kc],
            jnp.where(far, flip(me, kc), me) - core + to)

    extra_sends(extra_send)

    def fetch(ch, kc):
        a, b, e = axes(kc)
        for j in range(4):
            s = bit(me, a) * DIM[a] + (j // 2) * DIM[b] + (j % 2) * DIM[e] + core
            share_tiles(s, (ch * 3 + kc) * T, T,
                        lambda ref: pltpu.make_async_copy(ref, full.at[pl.ds(OWN_AT + (kc * 4 + j) * T, T)], own_sem.at[kc]).start())

    for kc in range(3):
        fetch(0, kc)

    def first_sum(ch):
        for kc in range(3):
            a, b, e = axes(kc)
            copies_wait(full.at[pl.ds((kc * NC + ch) * 12 * T, 12 * T)], raw_recv.at[kc, ch])
            copies_wait(full.at[pl.ds(OWN_AT + kc * 4 * T, 4 * T)], own_sem.at[kc])

            def sum_step(n):
                j = (n // 2 + 1 - bit(me, b)) % 2 * 2 + n % 2

                def tile_step(t):
                    def one(at):
                        return full[pl.ds(at + t * STEP, STEP)].astype(F32)
                    raw = [one(((kc * NC + ch) * 12 + src * 4 + j) * T) for src in range(3)]
                    acc[kc, ch, pl.ds(j * T + t * STEP, STEP)] = (one(OWN_AT + (kc * 4 + j) * T) + raw[2]) + (raw[0] + raw[1])

                loop(0, T // STEP, tile_step)

            loop(0, 4, sum_step)
            put(acc.at[kc, ch, pl.ds(2 * (1 - bit(me, b)) * T, 2 * T)], buf.at[pl.ds((kc * NC + ch) * 2 * T, 2 * T)],
                s2_send, s2_recv.at[kc, ch], flip(me, b))

            @pl.when(ch + 1 < NC)
            def _():
                fetch(ch + 1, kc)

    loop(0, NC, first_sum)

    def near(*dims):
        same = bit(me, dims[0]) == bit(cut, dims[0])
        for dim in dims[1:]:
            same = same & (bit(me, dim) == bit(cut, dim))
        return same

    for kc in range(3):
        a, b, e = axes(kc)

        @pl.when(near(a))
        def _():
            own = full.at[pl.ds(OWN_M + kc * MINI, MINI)]
            copy = pltpu.make_async_copy(lay.at[pl.ds(start_of(cut) - TAIL + extra_at(kc), MINI)], own, m_own)
            copy.start()
            raw = [full.at[pl.ds(RAW_M + (kc * 3 + src) * MINI, MINI)] for src in range(3)]
            copies_wait(full.at[pl.ds(RAW_M + kc * 3 * MINI, 3 * MINI)], m_raw_recv.at[kc])
            copy.wait()
            acc_m[kc] = (own[...].astype(F32) + raw[2][...].astype(F32)) + (raw[0][...].astype(F32) + raw[1][...].astype(F32))

            @pl.when(bit(me, b) != bit(cut, b))
            def _():
                put(acc_m.at[kc], recv2_m.at[kc], m_send.at[kc], m_recv.at[0, kc], flip(me, b))

    def second_sum(ch):
        for kc in range(3):
            a, b, e = axes(kc)
            slot = (kc * NC + ch) * 2 * T
            copies_wait(buf.at[pl.ds(slot, 2 * T)], s2_recv.at[kc, ch])
            for je in ((1 - bit(me, e)), bit(me, e)):
                def tile_step(t):
                    at = pl.ds((2 * bit(me, b) + je) * T + t * STEP, STEP)
                    acc[kc, ch, at] = acc[kc, ch, at] + buf[pl.ds(slot + je * T + t * STEP, STEP)]

                loop(0, T // STEP, tile_step)
            put(acc.at[kc, ch, pl.ds((2 * bit(me, b) + 1 - bit(me, e)) * T, T)], recv3.at[pl.ds((ch * 3 + kc) * T, T)],
                s3_send, s3_recv.at[kc, ch], flip(me, e))

    loop(0, NC, second_sum)
    for kc in range(3):
        a, b, e = axes(kc)

        @pl.when(near(a, b))
        def _():
            copies_wait(recv2_m.at[kc], m_recv.at[0, kc])
            acc_m[kc] = acc_m[kc] + recv2_m[kc]

            @pl.when(bit(me, e) != bit(cut, e))
            def _():
                put(acc_m.at[kc], recv3_m.at[kc], m_send.at[kc], m_recv.at[1, kc], flip(me, e))

    base = HEAD - (SHARE * me - start_of(me))

    def to_flat(lo, hi):
        walk_units(me, True, lo, hi, TO_FLAT, lambda fn, o: fn(buf, flat, tmp, o, WIDE + base + o))

    def flat_rows(t):
        return pl.ds((WIDE + t) * ROWS, ROWS)

    published = jnp.where(me == 15, SHARE, start_of(me + 1) - start_of(me))

    def squares(x, first):
        ids = first + lax.broadcasted_iota(jnp.int32, x.shape, 0)
        return jnp.sum(jnp.where(ids < published, x * x, 0.0), axis=0)

    def third_sum(ch, total):
        to_flat((ch - 1) * 3 * T, ch * 3 * T)
        for kc in range(3):
            a, b, e = axes(kc)
            copies_wait(recv3.at[pl.ds((ch * 3 + kc) * T, T)], s3_recv.at[kc, ch])

            def tile_step(t, total):
                i = pl.ds((ch * 3 + kc) * T + t * STEP, STEP)
                x = (acc[kc, ch, pl.ds((2 * bit(me, b) + bit(me, e)) * T + t * STEP, STEP)] + recv3[i]) * 0.0625
                buf[i] = x
                return total + squares(x, (ch * 3 + kc) * T + t * STEP)

            total = lax.fori_loop(0, T // STEP, tile_step, total)
        return total

    total = lax.fori_loop(0, NC, third_sum, jnp.zeros(TILE, F32))
    part[me] = jnp.sum(total, axis=0, keepdims=True)

    @pl.when(me == cut)
    def _():
        extra = jnp.zeros(TILE, F32)
        for kc in range(3):
            copies_wait(recv3_m.at[kc], m_recv.at[1, kc])
            x = (acc_m[kc] + recv3_m[kc]) * 0.0625
            buf[pl.ds(extra_at(kc), MINI)] = x
            extra = extra + squares(x, extra_at(kc))
        part[me] = part[me] + jnp.sum(extra, axis=0, keepdims=True)

    loop(1, DEVICES, lambda n: put(part.at[me], part.at[me], n_send, n_recv, lax.rem(me + n, DEVICES)))

    def heads(d, fn):
        for many in (True, False):
            n = HEAD if many else 6

            @pl.when((d != 15) & (((d == 12) | (d == 13)) == many))
            def _():
                for m, (src, dst) in enumerate(state):
                    fn(m, src.at[pl.ds((SHARE - n) * ROWS, n * ROWS)], dst.at[pl.ds((HEAD - n) * ROWS, n * ROWS)])

    heads(me, lambda m, src, dst: put(src, dst, head_sems.at[0, m], head_sems.at[1, m], lax.rem(me + 1, DEVICES)))
    to_flat((NC - 1) * 3 * T, 2 * WIDE)

    for copy in loads:
        copy.wait()

    def fill(x):
        return jnp.full(TILE, x, F32)

    def power7(x):
        x2 = x * x
        return x2 * x2 * x2 * x

    rate, b1, b2, decay, limit = (fill(hyper[n]) for n in range(5))
    fix1 = 1.0 / (1.0 - power7(b1))
    fix2 = 1.0 / (1.0 - power7(b2))
    others = pl.ds(0, DEVICES - 1)
    copies_wait(part.at[others], n_recv)
    norm_sum = fill(jnp.sum(part[...]))
    clip = jnp.minimum(1.0, limit / (jnp.sqrt(norm_sum) + CLIP_EPS))

    heads(lax.rem(me + 15, DEVICES), lambda m, src, dst: copies_wait(dst, head_sems.at[1, m]))

    def update(t):
        for n in range(6):
            tile = t * 6 + n
            i = pl.ds(tile * ROWS, ROWS)
            h = flat[flat_rows(tile), :] * clip
            pt = p_buf[i, :]
            mt = b1 * m_buf[i, :] + (1.0 - b1) * h
            vt = b2 * v_buf[i, :] + (1.0 - b2) * (h * h)
            has_decay = SHARE * me - HEAD + tile < TAIL + OFF_N
            u = (mt * fix1) / (jnp.sqrt(vt * fix2) + ADAM_EPS) + jnp.where(has_decay, decay, 0.0) * pt
            m_buf[i, :] = mt
            v_buf[i, :] = vt
            p_buf[i, :] = pt - rate * u

    def send(owner, c, kc, target, recv):
        block = full.at[pl.ds(owner * PUB + (c * 3 + kc) * PC, PC)]
        put(block, block, a_send, recv, target)

    mine = full.at[pl.ds(me * PUB, PUB)]

    def publish(c):
        loop(jnp.where(c == 0, 0, 9 + PC // 2 * c), jnp.minimum(9 + PC // 2 * (c + 1), EXT // 6), update)
        walk_units(me, False, c * 3 * PC, (c + 1) * 3 * PC, TO_TILES, lambda fn, o: fn(mine, p_buf, tmp, o, base + o))
        for hop in range(3):
            for kc in range(3):
                dim = axes(kc)[hop]
                send(me, c, kc, flip(me, dim), a_recv.at[c, kc, (0, 1, 3)[hop]])
        for kc in range(3):
            send(me, c, kc, pair, pair_recv)

    loop(0, NA, publish)

    def pass_on(level, c):
        for kc in range(3):
            a, b, e = axes(kc)
            for n in ((1,), (2, 3), (4, 5, 6, 7))[level]:
                owner = me
                for pos, dim in enumerate((a, b, e)):
                    if (n >> pos) & 1:
                        owner = flip(owner, dim)
                copies_wait(full.at[pl.ds(owner * PUB + (c * 3 + kc) * PC, PC)], a_recv.at[c, kc, n - 1])
                if level == 0:
                    send(owner, c, kc, flip(me, b), a_recv.at[c, kc, 2])
                if level < 2:
                    send(owner, c, kc, flip(me, e), a_recv.at[c, kc, n + 3])
                send(owner, c, kc, pair, pair_recv)

    for level in range(3):
        loop(0, NA, functools.partial(pass_on, level))

    copies_wait(full.at[pl.ds(0, DEVICES // 2 * PUB)], pair_recv)
    copies_wait(full.at[pl.ds(0, (DEVICES - 1) * PUB)], a_send)
    copies_wait(full.at[pl.ds(0, RAW_END)], raw_send)
    copies_wait(buf.at[pl.ds(0, 2 * WIN)], s2_send)
    copies_wait(recv3, s3_send)
    copies_wait(part.at[others], n_send)
    heads(me, lambda m, src, dst: copies_wait(dst, head_sems.at[0, m]))
    extra_sends(lambda kc, to, s, far: copies_wait(lay.at[pl.ds(0, MINI)], m_raw_send.at[kc, to]))
    for kc in range(3):
        a, b, e = axes(kc)

        @pl.when(near(a) & jnp.logical_not(near(a, b, e)))
        def _():
            copies_wait(acc_m.at[kc], m_send.at[kc])


def finish_kernel(gathered, m, v, p, emb, q, k, v_out, out, gate, up, down, norms, qk, mom_out, var_out, mas_out, norms_v, qk_v, rows2, sem, state_sem):
    starts = [9 * (SHARE * s // 9) - {13: 18, 14: 9}.get(s, 0) for s in range(16)] + [TAIL + LAY]
    state = [pltpu.make_async_copy(src.at[pl.ds(HEAD * ROWS, SHARE * ROWS)], dst, state_sem.at[n])
             for n, (src, dst) in enumerate(((m, mom_out), (v, var_out), (p, mas_out)))]
    for copy in state:
        copy.start()
    for dst, first, n, size in ((emb, 0, EMB, 1), (q, TAIL + OFF_Q, 54, 4), (k, TAIL + OFF_K, 54, 1), (v_out, TAIL + OFF_V, 54, 1),
                                (out, TAIL + OFF_O, 216, 1), (gate, TAIL + OFF_G, 54, 27), (up, TAIL + OFF_U, 54, 27),
                                (down, TAIL + OFF_D, 1458, 1)):
        for s in range(16):
            lo, hi = max(starts[s], first), min(starts[s + 1], first + n * size)
            if lo >= hi:
                continue
            src = s * PUB + lo - starts[s]
            if len(dst.shape) == 3:
                pltpu.make_async_copy(gathered.at[pl.ds(src, hi - lo)], dst.at[pl.ds(lo - first, hi - lo)], sem).start()
                continue
            unit = (lo - first) // size

            def step(i, carry, dst=dst, src=src, unit=unit, size=size):
                l, rb = (unit + i) // 9, lax.rem(unit + i, 9)
                pltpu.make_async_copy(gathered.at[pl.ds(src + i * size, size)], dst.at[l, :, rb], sem).start()
                return carry

            lax.fori_loop(0, (hi - lo) // size, step, 0)
    rows2[...] = gathered[pl.ds(15 * PUB + OFF_N - 4428, 30)].astype(F32).reshape(30 * ROWS, LANES)

    def norm_row(which, l, lane, at):
        (norms_v, qk_v)[which][l, :, lane:lane + LANES] = rows2[at, :].astype(BF16)

    norm_rows(norm_row)
    small = [pltpu.make_async_copy(src, dst, state_sem.at[3 + n]) for n, (src, dst) in enumerate(((norms_v, norms), (qk_v, qk)))]
    for copy in small:
        copy.start()
    copies_wait(gathered.at[pl.ds(0, TAIL + OFF_N)], sem)
    for copy in state + small:
        copy.wait()


ANY = pl.BlockSpec(memory_space=pl.ANY)
VM = pl.BlockSpec(memory_space=pltpu.VMEM)
DMA = pltpu.SemaphoreType.DMA


def tiled(x):
    rows, cols = x.shape[-2:]
    x = x.reshape(x.shape[:-2] + (rows // ROWS, ROWS, cols // LANES, LANES))
    return jnp.swapaxes(x, -3, -2)


def flat_tiles(x):
    return tiled(x).reshape((-1,) + TILE)


def solution(mesh):
    def local_update(*arrays):
        emb, q, k, v, out, gate, up, down, norms, qk = [a[0] for a in arrays[:GRAD_COUNT]]
        *state, hyper = arrays[GRAD_COUNT:]
        q_t, k_t, v_t, gate_t, up_t = [tiled(jnp.swapaxes(x, 1, 2)) for x in (q, k, v, gate, up)]
        small = [pltpu.VMEM(x.shape, BF16) for x in (norms, qk)]
        rows = [x.reshape(SHARE * ROWS, LANES) for x in state]
        args = [flat_tiles(emb), q_t, k_t, v_t, flat_tiles(out), gate_t, up_t, flat_tiles(down), norms, qk] + rows

        *kept, _ = pl.pallas_call(
            step_kernel,
            out_shape=(pltpu.VMEM((DEVICES * PUB,) + TILE, BF16),) + (pltpu.VMEM((EXT * ROWS, LANES), F32),) * 3
            + (jax.ShapeDtypeStruct((LAYP,) + TILE, BF16),),
            in_specs=[ANY] * 13 + [pl.BlockSpec(memory_space=pltpu.SMEM)],
            out_specs=(VM,) * 4 + (ANY,),
            scratch_shapes=small + [
                pltpu.VMEM((3, NC, 4 * T) + TILE, F32), pltpu.VMEM((2 * WIDE,) + TILE, F32), pltpu.VMEM((WIN,) + TILE, F32),
                pltpu.VMEM((2, LANES, LANES), F32), pltpu.VMEM((DEVICES, 1, LANES), F32)]
            + [pltpu.VMEM((3, MINI) + TILE, F32)] * 3
            + [DMA((2,)), DMA((2,)), DMA((3,)), DMA((2, 3)), DMA((3,)), DMA, DMA((3, NC)), DMA, DMA((3, NC)), DMA, DMA((3, NC)), DMA, DMA,
               DMA((3, 2)), DMA((3,)), DMA, DMA((3,)), DMA((2, 3)), DMA, DMA((NA, 3, 7)), DMA],
            compiler_params=pltpu.CompilerParams(collective_id=0, has_side_effects=True, vmem_limit_bytes=GRANT),
            name="step",
        )(*args, hyper)

        emb2, q2, k2, v2, out2, gate2, up2, down2, norms2, qk2, *state2 = pl.pallas_call(
            finish_kernel,
            out_shape=tuple(jax.ShapeDtypeStruct(x.shape, x.dtype) for x in args),
            in_specs=[VM] * 4,
            out_specs=(ANY,) * 13,
            scratch_shapes=small + [pltpu.VMEM((30 * ROWS, LANES), F32), DMA, DMA((5,))],
            compiler_params=pltpu.CompilerParams(vmem_limit_bytes=GRANT),
            name="finish",
        )(*[pltpu.with_memory_space_constraint(x, pltpu.VMEM) for x in kept])

        def matrices(x, like):
            x = x.reshape(like.shape[:-2] + (-1, like.shape[-1] // LANES) + TILE)
            return jnp.swapaxes(x, -3, -2).reshape(like.shape)

        def columns(x, like):
            return jnp.swapaxes(matrices(x, jnp.swapaxes(like, 1, 2)), 1, 2)

        params = (matrices(emb2, emb), columns(q2, q), columns(k2, k), columns(v2, v), matrices(out2, out), columns(gate2, gate), columns(up2, up),
                  matrices(down2, down), norms2, qk2)
        return params + tuple(x.reshape(-1) for x in state2)

    in_specs = tuple([P("dp")] * GRAD_COUNT + [P("dp"), P("dp"), P("dp"), P()])
    out_specs = tuple([P()] * GRAD_COUNT + [P("dp"), P("dp"), P("dp")])
    return jax.shard_map(local_update, mesh=mesh, in_specs=in_specs, out_specs=out_specs, check_vma=False)
```

```python
import functools
import jax
import jax.numpy as jnp
from jax import lax
from jax.experimental import pallas as pl
from jax.experimental.pallas import tpu as pltpu
from jax.sharding import PartitionSpec as P

ADAM_EPS = 1e-8
CLIP_EPS = 1e-6
GRAD_COUNT = 10
MESH = pl.DeviceIdType.MESH
F32, BF16 = jnp.float32, jnp.bfloat16

ROWS, LANES = 8, 128
TILE = (ROWS, LANES)
DEVICES = 16
SHARE = 885
WIN = 891
WIDE = 918
CUT = (14, 13)
NC = 9
T = 33
EARLY = 5
STEP = 11
MINI = 9
EMB = 9216
TAIL = 8847
LAY = 5313
LAYP = LAY + MINI
HALF = 2367
HEAD = 21
PUB = 900
NA = 10
PC = 30
EXT = HEAD + SHARE
OFF_Q, OFF_K, OFF_V, OFF_O = 369, 585, 639, 693
OFF_G, OFF_U, OFF_D, OFF_N = 909, 2367, 3825, 5283
DIM = (2, 4, 8)
SHIFT = 88
GRANT = 26400000
RAW_END = 12 * WIN
RAW_M = RAW_END
OWN_M = RAW_M + 9 * MINI
STAGE_AT = OWN_M + 3 * MINI
OWN_AT = STAGE_AT
BLOCK, COLS, BLOCKS, SCALES = 27, 216, 54, 30


def start_of(s):
    return 9 * ((SHARE * s) // 9) - jnp.where(s == 13, 18, 0) - jnp.where(s == 14, 9, 0)


def axes(colour):
    return [(colour + n) % 3 for n in range(3)]


def bit(d, dim):
    return (d // DIM[dim]) % 2


def flip(d, dim):
    return d + DIM[dim] * (1 - 2 * bit(d, dim))


def copies_wait(ref, sem):
    pltpu.make_async_copy(ref, ref, sem).wait()


def put(src, dst, send_sem, recv_sem, target):
    copy = pltpu.make_async_remote_copy(
        src_ref=src, dst_ref=dst, send_sem=send_sem, recv_sem=recv_sem, device_id=(target,), device_id_type=MESH)
    copy.start()
    return copy


def loop(lo, hi, fn):
    def step(i, carry):
        fn(i)
        return carry
    lax.fori_loop(lo, hi, step, 0)


def lanes():
    return lax.broadcasted_iota(jnp.int32, TILE, 1)


def gate_segments():
    rows = []
    for kap in range(BLOCK):
        pieces, f = [], LANES * kap
        while f < LANES * (kap + 1):
            i, c = f // COLS, f % COLS
            pieces.append((f - LANES * kap, i, c // LANES))
            f = min(LANES * (kap + 1), COLS * i + (LANES if c < LANES else COLS))
        rows.append(pieces)
    return rows


def gate_inverse():
    table = {}
    for kap, pieces in enumerate(gate_segments()):
        ends = [lo for lo, _, _ in pieces[1:]] + [LANES]
        for (lo, i, half), hi in zip(pieces, ends):
            table.setdefault((i, half), []).append((lo, hi, kap))
    return table


def swap_groups(xs, width):
    ids = lanes() // width
    xs, step = list(xs), 1
    while step < len(xs):
        high = (ids // step) % 2 == 1
        for n in range(len(xs)):
            if not n & step:
                lo, hi = xs[n], xs[n + step]
                xs[n] = jnp.where(high, pltpu.roll(hi, width * step, 1), lo)
                xs[n + step] = jnp.where(high, hi, pltpu.roll(lo, LANES - width * step, 1))
        step = 2 * step
    return xs


def turned(win, o):
    return win[pl.ds(o, 16)].reshape(LANES, LANES).T


def rows9_to_flat(win, flat, tmp, o, f):
    for ct in range(9):
        flat[pl.ds(f * ROWS + ct, ROWS, 9), :] = win[o + ct]


def gate_to_flat(win, flat, tmp, o, f):
    for half in range(2):
        tmp[half] = turned(win, o + 16 * half)
    ids = lanes()
    rolled = {}
    for i in range(16):
        for half in range(2):
            rolled[i, half] = pltpu.roll(tmp[half, pl.ds(i, ROWS, 16), :], (SHIFT * i) % LANES, 1)
    for kap, pieces in enumerate(gate_segments()):
        val = None
        for lo, i, half in pieces:
            val = rolled[i, half] if val is None else jnp.where(ids >= lo, rolled[i, half], val)
        flat[pl.ds(f * ROWS + kap, ROWS, BLOCK), :] = val


def q_to_flat(win, flat, tmp, o, f):
    tmp[0] = turned(win, o)
    for kb in range(4):
        xs = swap_groups([tmp[0, pl.ds(32 * kb + i, ROWS, 4), :] for i in range(4)], 32)
        for u in range(4):
            flat[pl.ds((f + 4 * u + kb) * ROWS, ROWS), :] = xs[u]


def kv_to_flat(win, flat, tmp, o, f):
    tmp[0] = turned(win, o)
    xs = swap_groups([tmp[0, pl.ds(i, ROWS, 16), :] for i in range(16)], ROWS)
    for u in range(16):
        flat[pl.ds((f + u) * ROWS, ROWS), :] = xs[u]


def copy_to_flat(win, flat, tmp, o, f):
    flat[pl.ds(f * ROWS, ROWS), :] = win[o]


def rows9_to_tiles(stage, flat, tmp, o, f):
    for ct in range(9):
        stage[o + ct] = flat[pl.ds(f * ROWS + ct, ROWS, 9), :].astype(BF16)


def gate_to_tiles(stage, flat, tmp, o, f):
    ids = lanes()
    rows = [flat[pl.ds(f * ROWS + kap, ROWS, BLOCK), :] for kap in range(BLOCK)]
    for (i, half), pieces in gate_inverse().items():
        val = rows[pieces[0][2]]
        for lo, hi, kap in pieces[1:]:
            val = jnp.where((ids >= lo) & (ids < hi), rows[kap], val)
        tmp[half, pl.ds(i, ROWS, 16), :] = pltpu.roll(val, (LANES - SHIFT * i) % LANES, 1)
    stage[pl.ds(o, 16)] = tmp[0].T.reshape(16, ROWS, LANES).astype(BF16)
    stage[pl.ds(o + 16, 11)] = tmp[1].T[:SHIFT].reshape(11, ROWS, LANES).astype(BF16)


def q_to_tiles(stage, flat, tmp, o, f):
    for kb in range(4):
        xs = swap_groups([flat[pl.ds((f + 4 * u + kb) * ROWS, ROWS), :] for u in range(4)], 32)
        for i in range(4):
            tmp[0, pl.ds(32 * kb + i, ROWS, 4), :] = xs[i]
    stage[pl.ds(o, 16)] = tmp[0].T.reshape(16, ROWS, LANES).astype(BF16)


def kv_to_tiles(stage, flat, tmp, o, f):
    xs = swap_groups([flat[pl.ds((f + u) * ROWS, ROWS), :] for u in range(16)], ROWS)
    for i in range(16):
        tmp[0, pl.ds(i, ROWS, 16), :] = xs[i]
    stage[pl.ds(o, 16)] = tmp[0].T.reshape(16, ROWS, LANES).astype(BF16)


def copy_to_tiles(stage, flat, tmp, o, f):
    stage[o] = flat[pl.ds(f * ROWS, ROWS), :].astype(BF16)


TO_FLAT = (rows9_to_flat, gate_to_flat, q_to_flat, kv_to_flat, copy_to_flat)
TO_TILES = (rows9_to_tiles, gate_to_tiles, q_to_tiles, kv_to_tiles, copy_to_tiles)


def walk_units(me, wide, lo, hi, fns, run):
    def pick(table):
        return sum(jnp.where(me == d, n, 0) for d, n in table.items())
    rows9, gate, q, kv, one = fns
    ends = (SHARE * (me + 1) + (8 if wide else 0)) // 9 - (SHARE * me) // 9
    first = jnp.where(me < 10, ends, pick({10: 41, 11: 3, 15: 95}))
    n_gate = pick({11: 32, 12: 33 if wide else 32, 13: 34 if wide else 33, 14: 11})
    second = pick({10: 22 if wide else 21, 14: 67})
    pos = 0
    for count, size, fn, over in ((first, 9, rows9, 0), (pick({10: 14}), 16, q, pick({10: 8})), (pick({10: 7}), 16, kv, pick({10: 4})),
                                  (n_gate, BLOCK, gate, 0), (second, 9, rows9, 0), (pick({15: SCALES}), 1, one, 0)):
        def done(x):
            return jnp.minimum(jnp.maximum(x - pos + (0 if wide else size - 1), 0) // size, count)

        loop(done(lo), done(hi), lambda u, pos=pos, size=size, fn=fn: run(fn, pos + u * size))
        pos = pos + count * size - over


def norm_rows(fn):
    for l in range(6):
        for ct in range(9):
            fn(0, l, ct * LANES, pl.ds(36 * l + ct, 4, 9))
        for ct in range(2):
            fn(1, l, ct * LANES, pl.ds(COLS + 4 * l + ct, 2, 2))


def step_kernel(emb, q, k, v, out, gate, up, down, norms, qk, mom, var, mas, hyper_in,
                full, m_buf, v_buf, p_buf, lay,
                hyper, norms_v, qk_v, acc, buf, recv3, tmp, part, acc_m, recv2_m, recv3_m,
                norm_sem, lay_sem, state_sem, head_sems, own_sem, recv_sems, raw_send, s2_send, s3_send, n_send, n_recv,
                m_raw_send, m_raw_recv, m_own, m_send, m_recv, a_send, pair_recv, hyper_sem):
    me = lax.axis_index("dp")
    core = me % 2
    pair = me + 1 - 2 * core
    flat = buf.reshape(2 * WIDE * ROWS, LANES)

    small = [pltpu.make_async_copy(src, dst, norm_sem.at[n]) for n, (src, dst) in enumerate(((norms, norms_v), (qk, qk_v)))]
    small.append(pltpu.make_async_copy(hyper_in, hyper, hyper_sem))
    for copy in small:
        copy.start()
    barrier = pltpu.get_barrier_semaphore()
    peers = [pair] + [flip(me, dim) + to for dim in range(3) for to in (0, 1 - 2 * core)]
    for peer in peers:
        pl.semaphore_signal(barrier, inc=1, device_id=(peer,), device_id_type=MESH)
    pl.semaphore_wait(barrier, len(peers))

    def hop_sem(hop, ch):
        return recv_sems.at[hop * NC + ch]

    def piece_sem(c, piece):
        return recv_sems.at[c * 7 + piece]

    def raw_at(kc, ch, src, j):
        return full.at[pl.ds(((kc * NC + ch) * 12 + src * 4 + j) * T, T)]

    def share_tiles(s, pos, n, fn):
        first = start_of(s) + pos

        @pl.when(s < 10)
        def _():
            fn(emb.at[pl.ds(first, n)])

        @pl.when(s >= 10)
        def _():
            fn(lay.at[pl.ds(first - TAIL, n)])

    def scatter(ch, with_emb, with_lay):
        def one(s, kc, src, j, target):
            @pl.when(jnp.where(s < 10, with_emb, with_lay) == 1)
            def _():
                share_tiles(s, (ch * 3 + kc) * T, T, lambda ref: put(ref, raw_at(kc, ch, src, j), raw_send, hop_sem(0, ch), target))

        for kc in range(3):
            a, b, e = axes(kc)
            far = flip(me, a)

            def share_step(j):
                near = (j // 2) * DIM[b] + (j % 2) * DIM[e]
                for to in range(2):
                    one((1 - bit(me, a)) * DIM[a] + near + to, kc, core, j, far - core + to)
                one(bit(me, a) * DIM[a] + near + 1 - core, kc, 2, j, pair)

            loop(0, 4, share_step)

    rows2 = tmp.reshape(2 * LANES, LANES)

    def norm_row(which, l, lane, at):
        rows2[at, :] = (norms_v, qk_v)[which][l, :, lane:lane + LANES].astype(F32)

    loop(0, EARLY, lambda ch: scatter(ch, 1, 0))
    for copy in small:
        copy.wait()
    norm_rows(norm_row)
    for lo, whole, split in ((0, ((emb.at[pl.ds(TAIL, OFF_Q)], 0), (out, OFF_O)), ((q, OFF_Q, 4), (k, OFF_K, 1), (v, OFF_V, 1), (gate, OFF_G, BLOCK))),
                             (HALF, ((down, OFF_D),), ((up, OFF_U, BLOCK),))):
        n = HALF if lo == 0 else LAY - HALF
        stage = full.at[pl.ds(STAGE_AT, n)]
        for src, off in whole:
            pltpu.make_async_copy(src, full.at[pl.ds(STAGE_AT + off - lo, src.shape[0])], lay_sem.at[0]).start()

        def load(i):
            for src, off, size in split:
                pltpu.make_async_copy(src.at[i // 9, :, lax.rem(i, 9)], full.at[pl.ds(STAGE_AT + off - lo + i * size, size)], lay_sem.at[0]).start()

        loop(0, BLOCKS, load)
        if lo == 0:
            copies_wait(stage, lay_sem.at[0])
        else:
            copies_wait(full.at[pl.ds(STAGE_AT, n - SCALES)], lay_sem.at[0])
            full[pl.ds(STAGE_AT + n - SCALES, SCALES)] = rows2[pl.ds(0, SCALES * ROWS), :].reshape((SCALES,) + TILE).astype(BF16)
        save = pltpu.make_async_copy(stage, lay.at[pl.ds(lo, n)], lay_sem.at[1])
        save.start()
        save.wait()
    loop(0, NC, lambda ch: scatter(ch, jnp.where(ch < EARLY, 0, 1), 1))
    state = ((mom, m_buf), (var, v_buf), (mas, p_buf))
    loads = [pltpu.make_async_copy(src, dst.at[pl.ds(HEAD * ROWS, SHARE * ROWS)], state_sem.at[n]) for n, (src, dst) in enumerate(state)]
    for copy in loads:
        copy.start()

    cut = jnp.where(core == 0, *CUT)

    def extra_at(kc):
        return WIN + kc * MINI

    def extra_sends(fn):
        for kc in range(3):
            for to, s in enumerate(CUT):
                far = bit(me, kc) != bit(s, kc)

                @pl.when(far | (core != to))
                def _():
                    fn(kc, to, s, far)

    def extra_send(kc, to, s, far):
        put(lay.at[pl.ds(start_of(s) - TAIL + extra_at(kc), MINI)],
            full.at[pl.ds(RAW_M + (kc * 3 + jnp.where(far, core, 2)) * MINI, MINI)], m_raw_send.at[kc, to], m_raw_recv.at[kc],
            jnp.where(far, flip(me, kc), me) - core + to)

    extra_sends(extra_send)

    def fetch(ch, kc):
        a, b, e = axes(kc)
        for j in range(4):
            s = bit(me, a) * DIM[a] + (j // 2) * DIM[b] + (j % 2) * DIM[e] + core
            share_tiles(s, (ch * 3 + kc) * T, T,
                        lambda ref: pltpu.make_async_copy(ref, full.at[pl.ds(OWN_AT + (kc * 4 + j) * T, T)], own_sem.at[kc]).start())

    for kc in range(3):
        fetch(0, kc)

    def first_sum(ch):
        copies_wait(full.at[pl.ds(0, 36 * T)], hop_sem(0, ch))
        for kc in range(3):
            a, b, e = axes(kc)
            copies_wait(full.at[pl.ds(OWN_AT + kc * 4 * T, 4 * T)], own_sem.at[kc])

            def sum_step(n):
                j = (n // 2 + 1 - bit(me, b)) % 2 * 2 + n % 2

                def tile_step(t):
                    def one(at):
                        return full[pl.ds(at + t * STEP, STEP)].astype(F32)
                    raw = [one(((kc * NC + ch) * 12 + src * 4 + j) * T) for src in range(3)]
                    acc[kc, ch, pl.ds(j * T + t * STEP, STEP)] = (one(OWN_AT + (kc * 4 + j) * T) + raw[2]) + (raw[0] + raw[1])

                loop(0, T // STEP, tile_step)

            loop(0, 4, sum_step)
            put(acc.at[kc, ch, pl.ds(2 * (1 - bit(me, b)) * T, 2 * T)], buf.at[pl.ds((kc * NC + ch) * 2 * T, 2 * T)],
                s2_send, hop_sem(1, ch), flip(me, b))

            @pl.when(ch + 1 < NC)
            def _():
                fetch(ch + 1, kc)

    loop(0, NC, first_sum)

    def near(*dims):
        same = bit(me, dims[0]) == bit(cut, dims[0])
        for dim in dims[1:]:
            same = same & (bit(me, dim) == bit(cut, dim))
        return same

    for kc in range(3):
        a, b, e = axes(kc)

        @pl.when(near(a))
        def _():
            own = full.at[pl.ds(OWN_M + kc * MINI, MINI)]
            copy = pltpu.make_async_copy(lay.at[pl.ds(start_of(cut) - TAIL + extra_at(kc), MINI)], own, m_own)
            copy.start()
            raw = [full.at[pl.ds(RAW_M + (kc * 3 + src) * MINI, MINI)] for src in range(3)]
            copies_wait(full.at[pl.ds(RAW_M + kc * 3 * MINI, 3 * MINI)], m_raw_recv.at[kc])
            copy.wait()
            acc_m[kc] = (own[...].astype(F32) + raw[2][...].astype(F32)) + (raw[0][...].astype(F32) + raw[1][...].astype(F32))

            @pl.when(bit(me, b) != bit(cut, b))
            def _():
                put(acc_m.at[kc], recv2_m.at[kc], m_send.at[kc], m_recv.at[0, kc], flip(me, b))

    def second_sum(ch):
        copies_wait(buf.at[pl.ds(0, 6 * T)], hop_sem(1, ch))
        for kc in range(3):
            a, b, e = axes(kc)
            slot = (kc * NC + ch) * 2 * T
            for je in ((1 - bit(me, e)), bit(me, e)):
                def tile_step(t):
                    at = pl.ds((2 * bit(me, b) + je) * T + t * STEP, STEP)
                    acc[kc, ch, at] = acc[kc, ch, at] + buf[pl.ds(slot + je * T + t * STEP, STEP)]

                loop(0, T // STEP, tile_step)
            put(acc.at[kc, ch, pl.ds((2 * bit(me, b) + 1 - bit(me, e)) * T, T)], recv3.at[pl.ds((ch * 3 + kc) * T, T)],
                s3_send, hop_sem(2, ch), flip(me, e))

    loop(0, NC, second_sum)
    for kc in range(3):
        a, b, e = axes(kc)

        @pl.when(near(a, b))
        def _():
            copies_wait(recv2_m.at[kc], m_recv.at[0, kc])
            acc_m[kc] = acc_m[kc] + recv2_m[kc]

            @pl.when(bit(me, e) != bit(cut, e))
            def _():
                put(acc_m.at[kc], recv3_m.at[kc], m_send.at[kc], m_recv.at[1, kc], flip(me, e))

    base = HEAD - (SHARE * me - start_of(me))

    def to_flat(lo, hi):
        walk_units(me, True, lo, hi, TO_FLAT, lambda fn, o: fn(buf, flat, tmp, o, WIDE + base + o))

    def flat_rows(t):
        return pl.ds((WIDE + t) * ROWS, ROWS)

    published = jnp.where(me == 15, SHARE, start_of(me + 1) - start_of(me))

    def squares(x, first):
        ids = first + lax.broadcasted_iota(jnp.int32, x.shape, 0)
        return jnp.sum(jnp.where(ids < published, x * x, 0.0), axis=0)

    def third_sum(ch, total):
        to_flat((ch - 1) * 3 * T, ch * 3 * T)
        copies_wait(recv3.at[pl.ds(ch * 3 * T, 3 * T)], hop_sem(2, ch))
        for kc in range(3):
            a, b, e = axes(kc)

            def tile_step(t, total):
                i = pl.ds((ch * 3 + kc) * T + t * STEP, STEP)
                x = (acc[kc, ch, pl.ds((2 * bit(me, b) + bit(me, e)) * T + t * STEP, STEP)] + recv3[i]) * 0.0625
                buf[i] = x
                return total + squares(x, (ch * 3 + kc) * T + t * STEP)

            total = lax.fori_loop(0, T // STEP, tile_step, total)
        return total

    total = lax.fori_loop(0, NC, third_sum, jnp.zeros(TILE, F32))
    part[me] = jnp.sum(total, axis=0, keepdims=True)

    @pl.when(me == cut)
    def _():
        extra = jnp.zeros(TILE, F32)
        for kc in range(3):
            copies_wait(recv3_m.at[kc], m_recv.at[1, kc])
            x = (acc_m[kc] + recv3_m[kc]) * 0.0625
            buf[pl.ds(extra_at(kc), MINI)] = x
            extra = extra + squares(x, extra_at(kc))
        part[me] = part[me] + jnp.sum(extra, axis=0, keepdims=True)

    loop(1, DEVICES, lambda n: put(part.at[me], part.at[me], n_send, n_recv, lax.rem(me + n, DEVICES)))

    def heads(d, fn):
        for many in (True, False):
            n = HEAD if many else 6

            @pl.when((d != 15) & (((d == 12) | (d == 13)) == many))
            def _():
                for m, (src, dst) in enumerate(state):
                    fn(m, src.at[pl.ds((SHARE - n) * ROWS, n * ROWS)], dst.at[pl.ds((HEAD - n) * ROWS, n * ROWS)])

    heads(me, lambda m, src, dst: put(src, dst, head_sems.at[0, m], head_sems.at[1, m], lax.rem(me + 1, DEVICES)))
    to_flat((NC - 1) * 3 * T, 2 * WIDE)

    for copy in loads:
        copy.wait()

    def fill(x):
        return jnp.full(TILE, x, F32)

    def power7(x):
        x2 = x * x
        return x2 * x2 * x2 * x

    rate, b1, b2, decay, limit = (fill(hyper[n]) for n in range(5))
    fix1 = 1.0 / (1.0 - power7(b1))
    fix2 = 1.0 / (1.0 - power7(b2))
    others = pl.ds(0, DEVICES - 1)
    copies_wait(part.at[others], n_recv)
    norm_sum = fill(jnp.sum(part[...]))
    clip = jnp.minimum(1.0, limit / (jnp.sqrt(norm_sum) + CLIP_EPS))

    heads(lax.rem(me + 15, DEVICES), lambda m, src, dst: copies_wait(dst, head_sems.at[1, m]))

    def update(t):
        for n in range(6):
            tile = t * 6 + n
            i = pl.ds(tile * ROWS, ROWS)
            h = flat[flat_rows(tile), :] * clip
            pt = p_buf[i, :]
            mt = b1 * m_buf[i, :] + (1.0 - b1) * h
            vt = b2 * v_buf[i, :] + (1.0 - b2) * (h * h)
            has_decay = SHARE * me - HEAD + tile < TAIL + OFF_N
            u = (mt * fix1) / (jnp.sqrt(vt * fix2) + ADAM_EPS) + jnp.where(has_decay, decay, 0.0) * pt
            m_buf[i, :] = mt
            v_buf[i, :] = vt
            p_buf[i, :] = pt - rate * u

    def send(owner, c, kc, target, recv):
        block = full.at[pl.ds(owner * PUB + (c * 3 + kc) * PC, PC)]
        put(block, block, a_send, recv, target)

    mine = full.at[pl.ds(me * PUB, PUB)]

    def made(c):
        return (c * 3 * PC + BLOCKS) // 6

    def publish(c):
        loop(jnp.where(c == 0, 0, made(c)), jnp.minimum(made(c + 1), EXT // 6), update)
        walk_units(me, False, c * 3 * PC, (c + 1) * 3 * PC, TO_TILES, lambda fn, o: fn(mine, p_buf, tmp, o, base + o))
        for hop in range(3):
            for kc in range(3):
                dim = axes(kc)[hop]
                send(me, c, kc, flip(me, dim), piece_sem(c, (0, 1, 3)[hop]))
        for kc in range(3):
            send(me, c, kc, pair, pair_recv)

    loop(0, NA, publish)

    def pass_on(level, c):
        for n in ((1,), (2, 3), (4, 5, 6, 7))[level]:
            copies_wait(full.at[pl.ds(0, 3 * PC)], piece_sem(c, n - 1))
            for kc in range(3):
                a, b, e = axes(kc)
                owner = me
                for pos, dim in enumerate((a, b, e)):
                    if (n >> pos) & 1:
                        owner = flip(owner, dim)
                if level == 0:
                    send(owner, c, kc, flip(me, b), piece_sem(c, 2))
                if level < 2:
                    send(owner, c, kc, flip(me, e), piece_sem(c, n + 3))
                send(owner, c, kc, pair, pair_recv)

    for level in range(3):
        loop(0, NA, functools.partial(pass_on, level))

    copies_wait(full.at[pl.ds(0, DEVICES // 2 * PUB)], pair_recv)
    copies_wait(full.at[pl.ds(0, (DEVICES - 1) * PUB)], a_send)
    copies_wait(full.at[pl.ds(0, RAW_END)], raw_send)
    copies_wait(buf.at[pl.ds(0, 2 * WIN)], s2_send)
    copies_wait(recv3, s3_send)
    copies_wait(part.at[others], n_send)
    heads(me, lambda m, src, dst: copies_wait(dst, head_sems.at[0, m]))
    extra_sends(lambda kc, to, s, far: copies_wait(lay.at[pl.ds(0, MINI)], m_raw_send.at[kc, to]))
    for kc in range(3):
        a, b, e = axes(kc)

        @pl.when(near(a) & jnp.logical_not(near(a, b, e)))
        def _():
            copies_wait(acc_m.at[kc], m_send.at[kc])


def finish_kernel(gathered, m, v, p, emb, q, k, v_out, out, gate, up, down, norms, qk, mom_out, var_out, mas_out, norms_v, qk_v, rows2, sem, state_sem):
    starts = [9 * (SHARE * s // 9) - {13: 18, 14: 9}.get(s, 0) for s in range(16)] + [TAIL + LAY]
    state = [pltpu.make_async_copy(src.at[pl.ds(HEAD * ROWS, SHARE * ROWS)], dst, state_sem.at[n])
             for n, (src, dst) in enumerate(((m, mom_out), (v, var_out), (p, mas_out)))]
    for copy in state:
        copy.start()
    for dst, first, n, size in ((emb, 0, EMB, 1), (q, TAIL + OFF_Q, BLOCKS, 4), (k, TAIL + OFF_K, BLOCKS, 1), (v_out, TAIL + OFF_V, BLOCKS, 1),
                                (out, TAIL + OFF_O, COLS, 1), (gate, TAIL + OFF_G, BLOCKS, BLOCK), (up, TAIL + OFF_U, BLOCKS, BLOCK),
                                (down, TAIL + OFF_D, 1458, 1)):
        for s in range(16):
            lo, hi = max(starts[s], first), min(starts[s + 1], first + n * size)
            if lo >= hi:
                continue
            src = s * PUB + lo - starts[s]
            if len(dst.shape) == 3:
                pltpu.make_async_copy(gathered.at[pl.ds(src, hi - lo)], dst.at[pl.ds(lo - first, hi - lo)], sem).start()
                continue
            unit = (lo - first) // size

            def step(i, carry, dst=dst, src=src, unit=unit, size=size):
                l, rb = (unit + i) // 9, lax.rem(unit + i, 9)
                pltpu.make_async_copy(gathered.at[pl.ds(src + i * size, size)], dst.at[l, :, rb], sem).start()
                return carry

            lax.fori_loop(0, (hi - lo) // size, step, 0)
    rows2[...] = gathered[pl.ds(15 * PUB + OFF_N - 4428, SCALES)].astype(F32).reshape(SCALES * ROWS, LANES)

    def norm_row(which, l, lane, at):
        (norms_v, qk_v)[which][l, :, lane:lane + LANES] = rows2[at, :].astype(BF16)

    norm_rows(norm_row)
    small = [pltpu.make_async_copy(src, dst, state_sem.at[3 + n]) for n, (src, dst) in enumerate(((norms_v, norms), (qk_v, qk)))]
    for copy in small:
        copy.start()
    copies_wait(gathered.at[pl.ds(0, TAIL + OFF_N)], sem)
    for copy in state + small:
        copy.wait()


ANY = pl.BlockSpec(memory_space=pl.ANY)
VM = pl.BlockSpec(memory_space=pltpu.VMEM)
DMA = pltpu.SemaphoreType.DMA


def tiled(x):
    rows, cols = x.shape[-2:]
    x = x.reshape(x.shape[:-2] + (rows // ROWS, ROWS, cols // LANES, LANES))
    return jnp.swapaxes(x, -3, -2)


def flat_tiles(x):
    return tiled(x).reshape((-1,) + TILE)


def solution(mesh):
    def local_update(*arrays):
        emb, q, k, v, out, gate, up, down, norms, qk = [a[0] for a in arrays[:GRAD_COUNT]]
        *state, hyper = arrays[GRAD_COUNT:]
        q_t, k_t, v_t, gate_t, up_t = [tiled(jnp.swapaxes(x, 1, 2)) for x in (q, k, v, gate, up)]
        small = [pltpu.VMEM(x.shape, BF16) for x in (norms, qk)]
        rows = [x.reshape(SHARE * ROWS, LANES) for x in state]
        args = [flat_tiles(emb), q_t, k_t, v_t, flat_tiles(out), gate_t, up_t, flat_tiles(down), norms, qk] + rows

        *kept, _ = pl.pallas_call(
            step_kernel,
            out_shape=(pltpu.VMEM((DEVICES * PUB,) + TILE, BF16),) + (pltpu.VMEM((EXT * ROWS, LANES), F32),) * 3
            + (jax.ShapeDtypeStruct((LAYP,) + TILE, BF16),),
            in_specs=[ANY] * 14,
            out_specs=(VM,) * 4 + (ANY,),
            scratch_shapes=[pltpu.SMEM(hyper.shape, F32)] + small + [
                pltpu.VMEM((3, NC, 4 * T) + TILE, F32), pltpu.VMEM((2 * WIDE,) + TILE, F32), pltpu.VMEM((WIN,) + TILE, F32),
                pltpu.VMEM((2, LANES, LANES), F32), pltpu.VMEM((DEVICES, 1, LANES), F32)]
            + [pltpu.VMEM((3, MINI) + TILE, F32)] * 3
            + [DMA((2,)), DMA((2,)), DMA((3,)), DMA((2, 3)), DMA((3,)), DMA((max(3 * NC, 7 * NA),)), DMA, DMA, DMA, DMA, DMA,
               DMA((3, 2)), DMA((3,)), DMA, DMA((3,)), DMA((2, 3)), DMA, DMA, DMA],
            compiler_params=pltpu.CompilerParams(collective_id=0, has_side_effects=True, vmem_limit_bytes=GRANT),
            name="step",
        )(*args, hyper)

        emb2, q2, k2, v2, out2, gate2, up2, down2, norms2, qk2, *state2 = pl.pallas_call(
            finish_kernel,
            out_shape=tuple(jax.ShapeDtypeStruct(x.shape, x.dtype) for x in args),
            in_specs=[VM] * 4,
            out_specs=(ANY,) * 13,
            scratch_shapes=small + [pltpu.VMEM((SCALES * ROWS, LANES), F32), DMA, DMA((5,))],
            compiler_params=pltpu.CompilerParams(vmem_limit_bytes=GRANT),
            name="finish",
        )(*[pltpu.with_memory_space_constraint(x, pltpu.VMEM) for x in kept])

        def matrices(x, like):
            x = x.reshape(like.shape[:-2] + (-1, like.shape[-1] // LANES) + TILE)
            return jnp.swapaxes(x, -3, -2).reshape(like.shape)

        def columns(x, like):
            return jnp.swapaxes(matrices(x, jnp.swapaxes(like, 1, 2)), 1, 2)

        params = (matrices(emb2, emb), columns(q2, q), columns(k2, k), columns(v2, v), matrices(out2, out), columns(gate2, gate), columns(up2, up),
                  matrices(down2, down), norms2, qk2)
        return params + tuple(x.reshape(-1) for x in state2)

    in_specs = tuple([P("dp")] * GRAD_COUNT + [P("dp"), P("dp"), P("dp"), P()])
    out_specs = tuple([P()] * GRAD_COUNT + [P("dp"), P("dp"), P("dp")])
    return jax.shard_map(local_update, mesh=mesh, in_specs=in_specs, out_specs=out_specs, check_vma=False)
```

```python
import functools
import jax
import jax.numpy as jnp
from jax import lax
from jax.experimental import pallas as pl
from jax.experimental.pallas import tpu as pltpu
from jax.sharding import PartitionSpec as P

ADAM_EPS = 1e-8
CLIP_EPS = 1e-6
GRAD_COUNT = 10
MESH = pl.DeviceIdType.MESH
F32, BF16 = jnp.float32, jnp.bfloat16

ROWS, LANES = 8, 128
TILE = (ROWS, LANES)
DEVICES = 16
SHARE = 885
WIN = 891
WIDE = 918
CUT = (14, 13)
NC = 9
T = 33
EARLY = 5
STEP = 11
MINI = 9
EMB = 9216
TAIL = 8847
LAY = 5313
LAYP = LAY + MINI
HALF = 2367
HEAD = 6
LAST = 12
FLAT = WIDE + 15
PUB = 891
NA = 9
PC = 33
EXT = HEAD + SHARE + LAST
OFF_Q, OFF_K, OFF_V, OFF_O = 369, 585, 639, 693
OFF_G, OFF_U, OFF_D, OFF_N = 909, 2367, 3825, 5283
DIM = (2, 4, 8)
SHIFT = 88
GRANT = 26400000
RAW_END = 12 * WIN
RAW_M = RAW_END
OWN_M = RAW_M + 9 * MINI
STAGE_AT = OWN_M + 3 * MINI
OWN_AT = STAGE_AT
BLOCK, COLS, BLOCKS, SCALES = 27, 216, 54, 30


def start_of(s):
    return 9 * ((SHARE * s) // 9) - jnp.where(s == 13, 18, 0) - jnp.where(s == 14, 9, 0)


def skip_of(s):
    return jnp.where((s == 13) | (s == 14), BLOCK, 0)


def axes(colour):
    return [(colour + n) % 3 for n in range(3)]


def bit(d, dim):
    return (d // DIM[dim]) % 2


def flip(d, dim):
    return d + DIM[dim] * (1 - 2 * bit(d, dim))


def copies_wait(ref, sem):
    pltpu.make_async_copy(ref, ref, sem).wait()


def put(src, dst, send_sem, recv_sem, target):
    copy = pltpu.make_async_remote_copy(
        src_ref=src, dst_ref=dst, send_sem=send_sem, recv_sem=recv_sem, device_id=(target,), device_id_type=MESH)
    copy.start()
    return copy


def loop(lo, hi, fn):
    def step(i, carry):
        fn(i)
        return carry
    lax.fori_loop(lo, hi, step, 0)


def lanes():
    return lax.broadcasted_iota(jnp.int32, TILE, 1)


def gate_segments():
    rows = []
    for kap in range(BLOCK):
        pieces, f = [], LANES * kap
        while f < LANES * (kap + 1):
            i, c = f // COLS, f % COLS
            pieces.append((f - LANES * kap, i, c // LANES))
            f = min(LANES * (kap + 1), COLS * i + (LANES if c < LANES else COLS))
        rows.append(pieces)
    return rows


def gate_inverse():
    table = {}
    for kap, pieces in enumerate(gate_segments()):
        ends = [lo for lo, _, _ in pieces[1:]] + [LANES]
        for (lo, i, half), hi in zip(pieces, ends):
            table.setdefault((i, half), []).append((lo, hi, kap))
    return table


def swap_groups(xs, width):
    ids = lanes() // width
    xs, step = list(xs), 1
    while step < len(xs):
        high = (ids // step) % 2 == 1
        for n in range(len(xs)):
            if not n & step:
                lo, hi = xs[n], xs[n + step]
                xs[n] = jnp.where(high, pltpu.roll(hi, width * step, 1), lo)
                xs[n + step] = jnp.where(high, hi, pltpu.roll(lo, LANES - width * step, 1))
        step = 2 * step
    return xs


def turned(win, o):
    return win[pl.ds(o, 16)].reshape(LANES, LANES).T


def rows9_to_flat(win, flat, tmp, o, f):
    for ct in range(9):
        flat[pl.ds(f * ROWS + ct, ROWS, 9), :] = win[o + ct]


def gate_to_flat(win, flat, tmp, o, f):
    for half in range(2):
        tmp[half] = turned(win, o + 16 * half)
    ids = lanes()
    rolled = {}
    for i in range(16):
        for half in range(2):
            rolled[i, half] = pltpu.roll(tmp[half, pl.ds(i, ROWS, 16), :], (SHIFT * i) % LANES, 1)
    for kap, pieces in enumerate(gate_segments()):
        val = None
        for lo, i, half in pieces:
            val = rolled[i, half] if val is None else jnp.where(ids >= lo, rolled[i, half], val)
        flat[pl.ds(f * ROWS + kap, ROWS, BLOCK), :] = val


def q_to_flat(win, flat, tmp, o, f):
    tmp[0] = turned(win, o)
    for kb in range(4):
        xs = swap_groups([tmp[0, pl.ds(32 * kb + i, ROWS, 4), :] for i in range(4)], 32)
        for u in range(4):
            flat[pl.ds((f + 4 * u + kb) * ROWS, ROWS), :] = xs[u]


def kv_to_flat(win, flat, tmp, o, f):
    tmp[0] = turned(win, o)
    xs = swap_groups([tmp[0, pl.ds(i, ROWS, 16), :] for i in range(16)], ROWS)
    for u in range(16):
        flat[pl.ds((f + u) * ROWS, ROWS), :] = xs[u]


def copy_to_flat(win, flat, tmp, o, f):
    flat[pl.ds(f * ROWS, ROWS), :] = win[o]


def rows9_to_tiles(stage, flat, tmp, o, f):
    for ct in range(9):
        stage[o + ct] = flat[pl.ds(f * ROWS + ct, ROWS, 9), :].astype(BF16)


def gate_to_tiles(stage, flat, tmp, o, f):
    ids = lanes()
    rows = [flat[pl.ds(f * ROWS + kap, ROWS, BLOCK), :] for kap in range(BLOCK)]
    for (i, half), pieces in gate_inverse().items():
        val = rows[pieces[0][2]]
        for lo, hi, kap in pieces[1:]:
            val = jnp.where((ids >= lo) & (ids < hi), rows[kap], val)
        tmp[half, pl.ds(i, ROWS, 16), :] = pltpu.roll(val, (LANES - SHIFT * i) % LANES, 1)
    stage[pl.ds(o, 16)] = tmp[0].T.reshape(16, ROWS, LANES).astype(BF16)
    stage[pl.ds(o + 16, 11)] = tmp[1].T[:SHIFT].reshape(11, ROWS, LANES).astype(BF16)


def q_to_tiles(stage, flat, tmp, o, f):
    for kb in range(4):
        xs = swap_groups([flat[pl.ds((f + 4 * u + kb) * ROWS, ROWS), :] for u in range(4)], 32)
        for i in range(4):
            tmp[0, pl.ds(32 * kb + i, ROWS, 4), :] = xs[i]
    stage[pl.ds(o, 16)] = tmp[0].T.reshape(16, ROWS, LANES).astype(BF16)


def kv_to_tiles(stage, flat, tmp, o, f):
    xs = swap_groups([flat[pl.ds((f + u) * ROWS, ROWS), :] for u in range(16)], ROWS)
    for i in range(16):
        tmp[0, pl.ds(i, ROWS, 16), :] = xs[i]
    stage[pl.ds(o, 16)] = tmp[0].T.reshape(16, ROWS, LANES).astype(BF16)


def copy_to_tiles(stage, flat, tmp, o, f):
    stage[o] = flat[pl.ds(f * ROWS, ROWS), :].astype(BF16)


TO_FLAT = (rows9_to_flat, gate_to_flat, q_to_flat, kv_to_flat, copy_to_flat)
TO_TILES = (rows9_to_tiles, gate_to_tiles, q_to_tiles, kv_to_tiles, copy_to_tiles)


def walk_units(me, wide, lo, hi, fns, run):
    def pick(table):
        return sum(jnp.where(me == d, n, 0) for d, n in table.items())
    rows9, gate, q, kv, one = fns
    ends = (SHARE * (me + 1) + (8 if wide else 0)) // 9 - (SHARE * me) // 9
    first = jnp.where(me < 10, ends, pick({10: 41, 11: 3, 15: 95}))
    n_gate = pick({11: 32, 12: 33, 13: 34, 14: 11})
    second = pick({10: 22 if wide else 21, 14: 67})
    pos = 0
    for count, size, fn, over in ((first, 9, rows9, 0), (pick({10: 14}), 16, q, pick({10: 8})), (pick({10: 7}), 16, kv, pick({10: 4})),
                                  (n_gate, BLOCK, gate, 0), (second, 9, rows9, 0), (pick({15: SCALES}), 1, one, 0)):
        def done(x):
            return jnp.minimum(jnp.maximum(x - pos + (0 if wide else size - 1), 0) // size, count)

        loop(done(lo), done(hi), lambda u, pos=pos, size=size, fn=fn: run(fn, pos + u * size))
        pos = pos + count * size - over


def norm_rows(fn):
    for l in range(6):
        for ct in range(9):
            fn(0, l, ct * LANES, pl.ds(36 * l + ct, 4, 9))
        for ct in range(2):
            fn(1, l, ct * LANES, pl.ds(COLS + 4 * l + ct, 2, 2))


def step_kernel(emb, q, k, v, out, gate, up, down, norms, qk, mom, var, mas, hyper_in,
                full, m_buf, v_buf, p_buf, lay,
                hyper, norms_v, qk_v, acc, buf, recv3, tmp, part, acc_m, recv2_m, recv3_m,
                norm_sem, lay_sem, state_sem, head_sems, own_sem, recv_sems, raw_send, s2_send, s3_send, n_send, n_recv,
                m_raw_send, m_raw_recv, m_own, m_send, m_recv, a_send, pair_recv, hyper_sem):
    me = lax.axis_index("dp")
    core = me % 2
    pair = me + 1 - 2 * core
    flat = buf.reshape(2 * WIDE * ROWS, LANES)

    small = [pltpu.make_async_copy(src, dst, norm_sem.at[n]) for n, (src, dst) in enumerate(((norms, norms_v), (qk, qk_v)))]
    small.append(pltpu.make_async_copy(hyper_in, hyper, hyper_sem))
    for copy in small:
        copy.start()
    barrier = pltpu.get_barrier_semaphore()
    peers = [pair] + [flip(me, dim) + to for dim in range(3) for to in (0, 1 - 2 * core)]
    for peer in peers:
        pl.semaphore_signal(barrier, inc=1, device_id=(peer,), device_id_type=MESH)
    pl.semaphore_wait(barrier, len(peers))

    def hop_sem(hop, ch):
        return recv_sems.at[hop * NC + ch]

    def piece_sem(c, piece):
        return recv_sems.at[c * 7 + piece]

    def raw_at(kc, ch, src, j):
        return full.at[pl.ds(((kc * NC + ch) * 12 + src * 4 + j) * T, T)]

    def share_tiles(s, pos, n, fn):
        first = start_of(s) + pos

        @pl.when(s < 10)
        def _():
            fn(emb.at[pl.ds(first, n)])

        @pl.when(s >= 10)
        def _():
            fn(lay.at[pl.ds(first - TAIL, n)])

    def scatter(ch, with_emb, with_lay):
        def one(s, kc, src, j, target):
            @pl.when(jnp.where(s < 10, with_emb, with_lay) == 1)
            def _():
                share_tiles(s, (ch * 3 + kc) * T, T, lambda ref: put(ref, raw_at(kc, ch, src, j), raw_send, hop_sem(0, ch), target))

        for kc in range(3):
            a, b, e = axes(kc)
            far = flip(me, a)

            def share_step(j):
                near = (j // 2) * DIM[b] + (j % 2) * DIM[e]
                for to in range(2):
                    one((1 - bit(me, a)) * DIM[a] + near + to, kc, core, j, far - core + to)
                one(bit(me, a) * DIM[a] + near + 1 - core, kc, 2, j, pair)

            loop(0, 4, share_step)

    rows2 = tmp.reshape(2 * LANES, LANES)

    def norm_row(which, l, lane, at):
        rows2[at, :] = (norms_v, qk_v)[which][l, :, lane:lane + LANES].astype(F32)

    loop(0, EARLY, lambda ch: scatter(ch, 1, 0))
    for copy in small:
        copy.wait()
    norm_rows(norm_row)
    for lo, whole, split in ((0, ((emb.at[pl.ds(TAIL, OFF_Q)], 0), (out, OFF_O)), ((q, OFF_Q, 4), (k, OFF_K, 1), (v, OFF_V, 1), (gate, OFF_G, BLOCK))),
                             (HALF, ((down, OFF_D),), ((up, OFF_U, BLOCK),))):
        n = HALF if lo == 0 else LAY - HALF
        stage = full.at[pl.ds(STAGE_AT, n)]
        for src, off in whole:
            pltpu.make_async_copy(src, full.at[pl.ds(STAGE_AT + off - lo, src.shape[0])], lay_sem.at[0]).start()

        def load(i):
            for src, off, size in split:
                pltpu.make_async_copy(src.at[i // 9, :, lax.rem(i, 9)], full.at[pl.ds(STAGE_AT + off - lo + i * size, size)], lay_sem.at[0]).start()

        loop(0, BLOCKS, load)
        if lo == 0:
            copies_wait(stage, lay_sem.at[0])
        else:
            copies_wait(full.at[pl.ds(STAGE_AT, n - SCALES)], lay_sem.at[0])
            full[pl.ds(STAGE_AT + n - SCALES, SCALES)] = rows2[pl.ds(0, SCALES * ROWS), :].reshape((SCALES,) + TILE).astype(BF16)
        save = pltpu.make_async_copy(stage, lay.at[pl.ds(lo, n)], lay_sem.at[1])
        save.start()
        save.wait()
    loop(0, NC, lambda ch: scatter(ch, jnp.where(ch < EARLY, 0, 1), 1))
    state = ((mom, m_buf), (var, v_buf), (mas, p_buf))
    loads = [pltpu.make_async_copy(src, dst.at[pl.ds(HEAD * ROWS, SHARE * ROWS)], state_sem.at[n]) for n, (src, dst) in enumerate(state)]
    for copy in loads:
        copy.start()

    cut = jnp.where(core == 0, *CUT)

    def extra_at(kc):
        return WIN + kc * MINI

    def extra_sends(fn):
        for kc in range(3):
            for to, s in enumerate(CUT):
                far = bit(me, kc) != bit(s, kc)

                @pl.when(far | (core != to))
                def _():
                    fn(kc, to, s, far)

    def extra_send(kc, to, s, far):
        put(lay.at[pl.ds(start_of(s) - TAIL + extra_at(kc), MINI)],
            full.at[pl.ds(RAW_M + (kc * 3 + jnp.where(far, core, 2)) * MINI, MINI)], m_raw_send.at[kc, to], m_raw_recv.at[kc],
            jnp.where(far, flip(me, kc), me) - core + to)

    extra_sends(extra_send)

    def fetch(ch, kc):
        a, b, e = axes(kc)
        for j in range(4):
            s = bit(me, a) * DIM[a] + (j // 2) * DIM[b] + (j % 2) * DIM[e] + core
            share_tiles(s, (ch * 3 + kc) * T, T,
                        lambda ref: pltpu.make_async_copy(ref, full.at[pl.ds(OWN_AT + (kc * 4 + j) * T, T)], own_sem.at[kc]).start())

    for kc in range(3):
        fetch(0, kc)

    def first_sum(ch):
        copies_wait(full.at[pl.ds(0, 36 * T)], hop_sem(0, ch))
        for kc in range(3):
            a, b, e = axes(kc)
            copies_wait(full.at[pl.ds(OWN_AT + kc * 4 * T, 4 * T)], own_sem.at[kc])

            def sum_step(n):
                j = (n // 2 + 1 - bit(me, b)) % 2 * 2 + n % 2

                def tile_step(t):
                    def one(at):
                        return full[pl.ds(at + t * STEP, STEP)].astype(F32)
                    raw = [one(((kc * NC + ch) * 12 + src * 4 + j) * T) for src in range(3)]
                    acc[kc, ch, pl.ds(j * T + t * STEP, STEP)] = (one(OWN_AT + (kc * 4 + j) * T) + raw[2]) + (raw[0] + raw[1])

                loop(0, T // STEP, tile_step)

            loop(0, 4, sum_step)
            put(acc.at[kc, ch, pl.ds(2 * (1 - bit(me, b)) * T, 2 * T)], buf.at[pl.ds((kc * NC + ch) * 2 * T, 2 * T)],
                s2_send, hop_sem(1, ch), flip(me, b))

            @pl.when(ch + 1 < NC)
            def _():
                fetch(ch + 1, kc)

    loop(0, NC, first_sum)

    def near(*dims):
        same = bit(me, dims[0]) == bit(cut, dims[0])
        for dim in dims[1:]:
            same = same & (bit(me, dim) == bit(cut, dim))
        return same

    for kc in range(3):
        a, b, e = axes(kc)

        @pl.when(near(a))
        def _():
            own = full.at[pl.ds(OWN_M + kc * MINI, MINI)]
            copy = pltpu.make_async_copy(lay.at[pl.ds(start_of(cut) - TAIL + extra_at(kc), MINI)], own, m_own)
            copy.start()
            raw = [full.at[pl.ds(RAW_M + (kc * 3 + src) * MINI, MINI)] for src in range(3)]
            copies_wait(full.at[pl.ds(RAW_M + kc * 3 * MINI, 3 * MINI)], m_raw_recv.at[kc])
            copy.wait()
            acc_m[kc] = (own[...].astype(F32) + raw[2][...].astype(F32)) + (raw[0][...].astype(F32) + raw[1][...].astype(F32))

            @pl.when(bit(me, b) != bit(cut, b))
            def _():
                put(acc_m.at[kc], recv2_m.at[kc], m_send.at[kc], m_recv.at[0, kc], flip(me, b))

    def second_sum(ch):
        copies_wait(buf.at[pl.ds(0, 6 * T)], hop_sem(1, ch))
        for kc in range(3):
            a, b, e = axes(kc)
            slot = (kc * NC + ch) * 2 * T
            for je in ((1 - bit(me, e)), bit(me, e)):
                def tile_step(t):
                    at = pl.ds((2 * bit(me, b) + je) * T + t * STEP, STEP)
                    acc[kc, ch, at] = acc[kc, ch, at] + buf[pl.ds(slot + je * T + t * STEP, STEP)]

                loop(0, T // STEP, tile_step)
            put(acc.at[kc, ch, pl.ds((2 * bit(me, b) + 1 - bit(me, e)) * T, T)], recv3.at[pl.ds((ch * 3 + kc) * T, T)],
                s3_send, hop_sem(2, ch), flip(me, e))

    loop(0, NC, second_sum)
    for kc in range(3):
        a, b, e = axes(kc)

        @pl.when(near(a, b))
        def _():
            copies_wait(recv2_m.at[kc], m_recv.at[0, kc])
            acc_m[kc] = acc_m[kc] + recv2_m[kc]

            @pl.when(bit(me, e) != bit(cut, e))
            def _():
                put(acc_m.at[kc], recv3_m.at[kc], m_send.at[kc], m_recv.at[1, kc], flip(me, e))

    base = HEAD - (SHARE * me - start_of(me))

    def to_flat(lo, hi):
        walk_units(me, True, lo, hi, TO_FLAT, lambda fn, o: fn(buf, flat, tmp, o, FLAT + base + o))

    def flat_rows(t):
        return pl.ds((FLAT + t) * ROWS, ROWS)

    skip = skip_of(me)
    last = jnp.where(me == 15, SHARE, start_of(me + 1) + skip_of(me + 1) - start_of(me))

    def squares(x, first):
        ids = first + lax.broadcasted_iota(jnp.int32, x.shape, 0)
        return jnp.sum(jnp.where((ids >= skip) & (ids < last), x * x, 0.0), axis=0)

    def third_sum(ch, total):
        to_flat((ch - 1) * 3 * T, ch * 3 * T)
        copies_wait(recv3.at[pl.ds(ch * 3 * T, 3 * T)], hop_sem(2, ch))
        for kc in range(3):
            a, b, e = axes(kc)

            def tile_step(t, total):
                i = pl.ds((ch * 3 + kc) * T + t * STEP, STEP)
                x = (acc[kc, ch, pl.ds((2 * bit(me, b) + bit(me, e)) * T + t * STEP, STEP)] + recv3[i]) * 0.0625
                buf[i] = x
                return total + squares(x, (ch * 3 + kc) * T + t * STEP)

            total = lax.fori_loop(0, T // STEP, tile_step, total)
        return total

    total = lax.fori_loop(0, NC, third_sum, jnp.zeros(TILE, F32))
    part[me] = jnp.sum(total, axis=0, keepdims=True)

    @pl.when(me == cut)
    def _():
        extra = jnp.zeros(TILE, F32)
        for kc in range(3):
            copies_wait(recv3_m.at[kc], m_recv.at[1, kc])
            x = (acc_m[kc] + recv3_m[kc]) * 0.0625
            buf[pl.ds(extra_at(kc), MINI)] = x
            extra = extra + squares(x, extra_at(kc))
        part[me] = part[me] + jnp.sum(extra, axis=0, keepdims=True)

    loop(1, DEVICES, lambda n: put(part.at[me], part.at[me], n_send, n_recv, lax.rem(me + n, DEVICES)))

    def ends(cases, fn):
        for who, *case in cases:
            @pl.when(who)
            def _():
                fn(*case)

    sent = ((me < 12, 0, HEAD), (me == 13, 1, HEAD), (me == 14, 1, LAST))
    got = (((me > 0) & (me < 13), 0, HEAD), (me == 12, 1, HEAD), (me == 13, 1, LAST))

    def end_put(kind, n):
        at, to, target = ((SHARE - n, 0, me + 1), (0, HEAD + SHARE, me - 1))[kind]
        for src, dst in state:
            put(src.at[pl.ds(at * ROWS, n * ROWS)], dst.at[pl.ds(to * ROWS, n * ROWS)], head_sems.at[0, kind], head_sems.at[1, kind], target)

    def end_wait(side, kind, n):
        copies_wait(m_buf.at[pl.ds(0, 3 * n * ROWS)], head_sems.at[side, kind])

    ends(sent, end_put)
    to_flat((NC - 1) * 3 * T, 2 * WIDE)

    for copy in loads:
        copy.wait()

    def fill(x):
        return jnp.full(TILE, x, F32)

    def power7(x):
        x2 = x * x
        return x2 * x2 * x2 * x

    rate, b1, b2, decay, limit = (fill(hyper[n]) for n in range(5))
    fix1 = 1.0 / (1.0 - power7(b1))
    fix2 = 1.0 / (1.0 - power7(b2))
    others = pl.ds(0, DEVICES - 1)
    copies_wait(part.at[others], n_recv)
    norm_sum = fill(jnp.sum(part[...]))
    clip = jnp.minimum(1.0, limit / (jnp.sqrt(norm_sum) + CLIP_EPS))

    ends(got, functools.partial(end_wait, 1))

    def update(t):
        for n in range(7):
            tile = t * 7 + n
            i = pl.ds(tile * ROWS, ROWS)
            h = flat[flat_rows(tile), :] * clip
            pt = p_buf[i, :]
            mt = b1 * m_buf[i, :] + (1.0 - b1) * h
            vt = b2 * v_buf[i, :] + (1.0 - b2) * (h * h)
            has_decay = SHARE * me - HEAD + tile < TAIL + OFF_N
            u = (mt * fix1) / (jnp.sqrt(vt * fix2) + ADAM_EPS) + jnp.where(has_decay, decay, 0.0) * pt
            m_buf[i, :] = mt
            v_buf[i, :] = vt
            p_buf[i, :] = pt - rate * u

    def send(owner, c, kc, target, recv):
        block = full.at[pl.ds(owner * PUB + (c * 3 + kc) * PC, PC)]
        put(block, block, a_send, recv, target)

    mine = full.at[pl.ds(me * PUB, PUB)]

    def made(c):
        return (c * 3 * PC + 51) // 7

    def publish(c):
        loop(jnp.where(c == 0, 0, made(c)), jnp.minimum(made(c + 1), EXT // 7), update)
        walk_units(me, False, skip + c * 3 * PC, skip + (c + 1) * 3 * PC, TO_TILES, lambda fn, o: fn(mine, p_buf, tmp, o - skip, base + o))
        for hop in range(3):
            for kc in range(3):
                dim = axes(kc)[hop]
                send(me, c, kc, flip(me, dim), piece_sem(c, (0, 1, 3)[hop]))
        for kc in range(3):
            send(me, c, kc, pair, pair_recv)

    loop(0, NA, publish)

    def pass_on(level, c):
        for n in ((1,), (2, 3), (4, 5, 6, 7))[level]:
            copies_wait(full.at[pl.ds(0, 3 * PC)], piece_sem(c, n - 1))
            for kc in range(3):
                a, b, e = axes(kc)
                owner = me
                for pos, dim in enumerate((a, b, e)):
                    if (n >> pos) & 1:
                        owner = flip(owner, dim)
                if level == 0:
                    send(owner, c, kc, flip(me, b), piece_sem(c, 2))
                if level < 2:
                    send(owner, c, kc, flip(me, e), piece_sem(c, n + 3))
                send(owner, c, kc, pair, pair_recv)

    for level in range(3):
        loop(0, NA, functools.partial(pass_on, level))

    copies_wait(full.at[pl.ds(0, DEVICES // 2 * PUB)], pair_recv)
    copies_wait(full.at[pl.ds(0, (DEVICES - 1) * PUB)], a_send)
    copies_wait(full.at[pl.ds(0, RAW_END)], raw_send)
    copies_wait(buf.at[pl.ds(0, 2 * WIN)], s2_send)
    copies_wait(recv3, s3_send)
    copies_wait(part.at[others], n_send)
    ends(sent, functools.partial(end_wait, 0))
    extra_sends(lambda kc, to, s, far: copies_wait(lay.at[pl.ds(0, MINI)], m_raw_send.at[kc, to]))
    for kc in range(3):
        a, b, e = axes(kc)

        @pl.when(near(a) & jnp.logical_not(near(a, b, e)))
        def _():
            copies_wait(acc_m.at[kc], m_send.at[kc])


def finish_kernel(gathered, m, v, p, emb, q, k, v_out, out, gate, up, down, norms, qk, mom_out, var_out, mas_out, norms_v, qk_v, rows2, sem, state_sem):
    starts = [9 * (SHARE * s // 9) + {13: 9, 14: 18}.get(s, 0) for s in range(16)] + [TAIL + LAY]
    state = [pltpu.make_async_copy(src.at[pl.ds(HEAD * ROWS, SHARE * ROWS)], dst, state_sem.at[n])
             for n, (src, dst) in enumerate(((m, mom_out), (v, var_out), (p, mas_out)))]
    for copy in state:
        copy.start()
    for dst, first, n, size in ((emb, 0, EMB, 1), (q, TAIL + OFF_Q, BLOCKS, 4), (k, TAIL + OFF_K, BLOCKS, 1), (v_out, TAIL + OFF_V, BLOCKS, 1),
                                (out, TAIL + OFF_O, COLS, 1), (gate, TAIL + OFF_G, BLOCKS, BLOCK), (up, TAIL + OFF_U, BLOCKS, BLOCK),
                                (down, TAIL + OFF_D, 1458, 1)):
        for s in range(16):
            lo, hi = max(starts[s], first), min(starts[s + 1], first + n * size)
            if lo >= hi:
                continue
            src = s * PUB + lo - starts[s]
            if len(dst.shape) == 3:
                pltpu.make_async_copy(gathered.at[pl.ds(src, hi - lo)], dst.at[pl.ds(lo - first, hi - lo)], sem).start()
                continue
            unit = (lo - first) // size

            def step(i, carry, dst=dst, src=src, unit=unit, size=size):
                l, rb = (unit + i) // 9, lax.rem(unit + i, 9)
                pltpu.make_async_copy(gathered.at[pl.ds(src + i * size, size)], dst.at[l, :, rb], sem).start()
                return carry

            lax.fori_loop(0, (hi - lo) // size, step, 0)
    rows2[...] = gathered[pl.ds(15 * PUB + OFF_N - 4428, SCALES)].astype(F32).reshape(SCALES * ROWS, LANES)

    def norm_row(which, l, lane, at):
        (norms_v, qk_v)[which][l, :, lane:lane + LANES] = rows2[at, :].astype(BF16)

    norm_rows(norm_row)
    small = [pltpu.make_async_copy(src, dst, state_sem.at[3 + n]) for n, (src, dst) in enumerate(((norms_v, norms), (qk_v, qk)))]
    for copy in small:
        copy.start()
    copies_wait(gathered.at[pl.ds(0, TAIL + OFF_N)], sem)
    for copy in state + small:
        copy.wait()


ANY = pl.BlockSpec(memory_space=pl.ANY)
VM = pl.BlockSpec(memory_space=pltpu.VMEM)
DMA = pltpu.SemaphoreType.DMA


def tiled(x):
    rows, cols = x.shape[-2:]
    x = x.reshape(x.shape[:-2] + (rows // ROWS, ROWS, cols // LANES, LANES))
    return jnp.swapaxes(x, -3, -2)


def flat_tiles(x):
    return tiled(x).reshape((-1,) + TILE)


def solution(mesh):
    def local_update(*arrays):
        emb, q, k, v, out, gate, up, down, norms, qk = [a[0] for a in arrays[:GRAD_COUNT]]
        *state, hyper = arrays[GRAD_COUNT:]
        q_t, k_t, v_t, gate_t, up_t = [tiled(jnp.swapaxes(x, 1, 2)) for x in (q, k, v, gate, up)]
        small = [pltpu.VMEM(x.shape, BF16) for x in (norms, qk)]
        rows = [x.reshape(SHARE * ROWS, LANES) for x in state]
        args = [flat_tiles(emb), q_t, k_t, v_t, flat_tiles(out), gate_t, up_t, flat_tiles(down), norms, qk] + rows

        *kept, _ = pl.pallas_call(
            step_kernel,
            out_shape=(pltpu.VMEM((DEVICES * PUB,) + TILE, BF16),) + (pltpu.VMEM((EXT * ROWS, LANES), F32),) * 3
            + (jax.ShapeDtypeStruct((LAYP,) + TILE, BF16),),
            in_specs=[ANY] * 14,
            out_specs=(VM,) * 4 + (ANY,),
            scratch_shapes=[pltpu.SMEM(hyper.shape, F32)] + small + [
                pltpu.VMEM((3, NC, 4 * T) + TILE, F32), pltpu.VMEM((2 * WIDE,) + TILE, F32), pltpu.VMEM((WIN,) + TILE, F32),
                pltpu.VMEM((2, LANES, LANES), F32), pltpu.VMEM((DEVICES, 1, LANES), F32)]
            + [pltpu.VMEM((3, MINI) + TILE, F32)] * 3
            + [DMA((2,)), DMA((2,)), DMA((3,)), DMA((2, 2)), DMA((3,)), DMA((max(3 * NC, 7 * NA),)), DMA, DMA, DMA, DMA, DMA,
               DMA((3, 2)), DMA((3,)), DMA, DMA((3,)), DMA((2, 3)), DMA, DMA, DMA],
            compiler_params=pltpu.CompilerParams(collective_id=0, has_side_effects=True, vmem_limit_bytes=GRANT),
            name="step",
        )(*args, hyper)

        emb2, q2, k2, v2, out2, gate2, up2, down2, norms2, qk2, *state2 = pl.pallas_call(
            finish_kernel,
            out_shape=tuple(jax.ShapeDtypeStruct(x.shape, x.dtype) for x in args),
            in_specs=[VM] * 4,
            out_specs=(ANY,) * 13,
            scratch_shapes=small + [pltpu.VMEM((SCALES * ROWS, LANES), F32), DMA, DMA((5,))],
            compiler_params=pltpu.CompilerParams(vmem_limit_bytes=GRANT),
            name="finish",
        )(*[pltpu.with_memory_space_constraint(x, pltpu.VMEM) for x in kept])

        def matrices(x, like):
            x = x.reshape(like.shape[:-2] + (-1, like.shape[-1] // LANES) + TILE)
            return jnp.swapaxes(x, -3, -2).reshape(like.shape)

        def columns(x, like):
            return jnp.swapaxes(matrices(x, jnp.swapaxes(like, 1, 2)), 1, 2)

        params = (matrices(emb2, emb), columns(q2, q), columns(k2, k), columns(v2, v), matrices(out2, out), columns(gate2, gate), columns(up2, up),
                  matrices(down2, down), norms2, qk2)
        return params + tuple(x.reshape(-1) for x in state2)

    in_specs = tuple([P("dp")] * GRAD_COUNT + [P("dp"), P("dp"), P("dp"), P()])
    out_specs = tuple([P()] * GRAD_COUNT + [P("dp"), P("dp"), P("dp")])
    return jax.shard_map(local_update, mesh=mesh, in_specs=in_specs, out_specs=out_specs, check_vma=False)
```

```python
import functools
import jax
import jax.numpy as jnp
from jax import lax
from jax.experimental import pallas as pl
from jax.experimental.pallas import tpu as pltpu
from jax.sharding import PartitionSpec as P

ADAM_EPS = 1e-8
CLIP_EPS = 1e-6
GRAD_COUNT = 10
MESH = pl.DeviceIdType.MESH
F32, BF16 = jnp.float32, jnp.bfloat16

ROWS, LANES = 8, 128
TILE = (ROWS, LANES)
DEVICES = 16
SHARE = 885
WIN = 891
WIDE = 918
CUT = (14, 13)
NC = 9
T = 33
EARLY = 5
STEP = 11
MINI = 9
EMB = 9216
TAIL = 8847
LAY = 5313
LAYP = LAY + MINI
HALF = 2367
HEAD = 6
LAST = 12
FLAT = WIDE + 15
PUB = 891
NA = 9
PC = 33
EXT = HEAD + SHARE + LAST
OFF_Q, OFF_K, OFF_V, OFF_O = 369, 585, 639, 693
OFF_G, OFF_U, OFF_D, OFF_N = 909, 2367, 3825, 5283
DIM = (2, 4, 8)
SHIFT = 88
GRANT = 26400000
RAW_END = 12 * WIN
RAW_M = RAW_END
OWN_M = RAW_M + 9 * MINI
STAGE_AT = OWN_M + 3 * MINI
OWN_AT = STAGE_AT
BLOCK, COLS, BLOCKS, SCALES = 27, 216, 54, 30


def start_of(s):
    return 9 * ((SHARE * s) // 9) - jnp.where(s == 13, 18, 0) - jnp.where(s == 14, 9, 0)


def skip_of(s):
    return jnp.where((s == 13) | (s == 14), BLOCK, 0)


def axes(colour):
    return [(colour + n) % 3 for n in range(3)]


def bit(d, dim):
    return (d // DIM[dim]) % 2


def flip(d, dim):
    return d + DIM[dim] * (1 - 2 * bit(d, dim))


def copies_wait(ref, sem):
    pltpu.make_async_copy(ref, ref, sem).wait()


def put(src, dst, send_sem, recv_sem, target):
    copy = pltpu.make_async_remote_copy(
        src_ref=src, dst_ref=dst, send_sem=send_sem, recv_sem=recv_sem, device_id=(target,), device_id_type=MESH)
    copy.start()
    return copy


def loop(lo, hi, fn):
    def step(i, carry):
        fn(i)
        return carry
    lax.fori_loop(lo, hi, step, 0)


def lanes():
    return lax.broadcasted_iota(jnp.int32, TILE, 1)


def gate_segments():
    rows = []
    for kap in range(BLOCK):
        pieces, f = [], LANES * kap
        while f < LANES * (kap + 1):
            i, c = f // COLS, f % COLS
            pieces.append((f - LANES * kap, i, c // LANES))
            f = min(LANES * (kap + 1), COLS * i + (LANES if c < LANES else COLS))
        rows.append(pieces)
    return rows


def gate_inverse():
    table = {}
    for kap, pieces in enumerate(gate_segments()):
        ends = [lo for lo, _, _ in pieces[1:]] + [LANES]
        for (lo, i, half), hi in zip(pieces, ends):
            table.setdefault((i, half), []).append((lo, hi, kap))
    return table


def swap_groups(xs, width):
    ids = lanes() // width
    xs, step = list(xs), 1
    while step < len(xs):
        high = (ids // step) % 2 == 1
        for n in range(len(xs)):
            if not n & step:
                lo, hi = xs[n], xs[n + step]
                xs[n] = jnp.where(high, pltpu.roll(hi, width * step, 1), lo)
                xs[n + step] = jnp.where(high, hi, pltpu.roll(lo, LANES - width * step, 1))
        step = 2 * step
    return xs


def turned(win, o):
    return win[pl.ds(o, 16)].reshape(LANES, LANES).T


def rows9_to_flat(win, flat, tmp, o, f):
    for ct in range(9):
        flat[pl.ds(f * ROWS + ct, ROWS, 9), :] = win[o + ct]


def gate_to_flat(win, flat, tmp, o, f):
    for half in range(2):
        tmp[half] = turned(win, o + 16 * half)
    ids = lanes()
    rolled = {}
    for i in range(16):
        for half in range(2):
            rolled[i, half] = pltpu.roll(tmp[half, pl.ds(i, ROWS, 16), :], (SHIFT * i) % LANES, 1)
    for kap, pieces in enumerate(gate_segments()):
        val = None
        for lo, i, half in pieces:
            val = rolled[i, half] if val is None else jnp.where(ids >= lo, rolled[i, half], val)
        flat[pl.ds(f * ROWS + kap, ROWS, BLOCK), :] = val


def q_to_flat(win, flat, tmp, o, f):
    tmp[0] = turned(win, o)
    for kb in range(4):
        xs = swap_groups([tmp[0, pl.ds(32 * kb + i, ROWS, 4), :] for i in range(4)], 32)
        for u in range(4):
            flat[pl.ds((f + 4 * u + kb) * ROWS, ROWS), :] = xs[u]


def kv_to_flat(win, flat, tmp, o, f):
    tmp[0] = turned(win, o)
    xs = swap_groups([tmp[0, pl.ds(i, ROWS, 16), :] for i in range(16)], ROWS)
    for u in range(16):
        flat[pl.ds((f + u) * ROWS, ROWS), :] = xs[u]


def copy_to_flat(win, flat, tmp, o, f):
    flat[pl.ds(f * ROWS, ROWS), :] = win[o]


def rows9_to_tiles(stage, flat, tmp, o, f):
    for ct in range(9):
        stage[o + ct] = flat[pl.ds(f * ROWS + ct, ROWS, 9), :].astype(BF16)


def gate_to_tiles(stage, flat, tmp, o, f):
    ids = lanes()
    rows = [flat[pl.ds(f * ROWS + kap, ROWS, BLOCK), :] for kap in range(BLOCK)]
    for (i, half), pieces in gate_inverse().items():
        val = rows[pieces[0][2]]
        for lo, hi, kap in pieces[1:]:
            val = jnp.where((ids >= lo) & (ids < hi), rows[kap], val)
        tmp[half, pl.ds(i, ROWS, 16), :] = pltpu.roll(val, (LANES - SHIFT * i) % LANES, 1)
    stage[pl.ds(o, 16)] = tmp[0].T.reshape(16, ROWS, LANES).astype(BF16)
    stage[pl.ds(o + 16, 11)] = tmp[1].T[:SHIFT].reshape(11, ROWS, LANES).astype(BF16)


def q_to_tiles(stage, flat, tmp, o, f):
    for kb in range(4):
        xs = swap_groups([flat[pl.ds((f + 4 * u + kb) * ROWS, ROWS), :] for u in range(4)], 32)
        for i in range(4):
            tmp[0, pl.ds(32 * kb + i, ROWS, 4), :] = xs[i]
    stage[pl.ds(o, 16)] = tmp[0].T.reshape(16, ROWS, LANES).astype(BF16)


def kv_to_tiles(stage, flat, tmp, o, f):
    xs = swap_groups([flat[pl.ds((f + u) * ROWS, ROWS), :] for u in range(16)], ROWS)
    for i in range(16):
        tmp[0, pl.ds(i, ROWS, 16), :] = xs[i]
    stage[pl.ds(o, 16)] = tmp[0].T.reshape(16, ROWS, LANES).astype(BF16)


def copy_to_tiles(stage, flat, tmp, o, f):
    stage[o] = flat[pl.ds(f * ROWS, ROWS), :].astype(BF16)


TO_FLAT = (rows9_to_flat, gate_to_flat, q_to_flat, kv_to_flat, copy_to_flat)
TO_TILES = (rows9_to_tiles, gate_to_tiles, q_to_tiles, kv_to_tiles, copy_to_tiles)


def walk_units(me, wide, lo, hi, fns, run):
    def pick(table):
        return sum(jnp.where(me == d, n, 0) for d, n in table.items())
    rows9, gate, q, kv, one = fns
    ends = (SHARE * (me + 1) + (8 if wide else 0)) // 9 - (SHARE * me) // 9
    first = jnp.where(me < 10, ends, pick({10: 41, 11: 3, 15: 95}))
    n_gate = pick({11: 32, 12: 33, 13: 34, 14: 11})
    second = pick({10: 22 if wide else 21, 14: 67})
    pos = 0
    for count, size, fn, over in ((first, 9, rows9, 0), (pick({10: 14}), 16, q, pick({10: 8})), (pick({10: 7}), 16, kv, pick({10: 4})),
                                  (n_gate, BLOCK, gate, 0), (second, 9, rows9, 0), (pick({15: SCALES}), 1, one, 0)):
        def done(x):
            return jnp.minimum(jnp.maximum(x - pos + (0 if wide else size - 1), 0) // size, count)

        loop(done(lo), done(hi), lambda u, pos=pos, size=size, fn=fn: run(fn, pos + u * size))
        pos = pos + count * size - over


def norm_rows(fn):
    for l in range(6):
        for ct in range(9):
            fn(0, l, ct * LANES, pl.ds(36 * l + ct, 4, 9))
        for ct in range(2):
            fn(1, l, ct * LANES, pl.ds(COLS + 4 * l + ct, 2, 2))


def step_kernel(emb, q, k, v, out, gate, up, down, norms, qk, mom, var, mas, hyper_in,
                full, m_buf, v_buf, p_buf, lay,
                hyper, norms_v, qk_v, acc, buf, recv3, tmp, part, acc_m, recv2_m, recv3_m,
                norm_sem, lay_sem, state_sem, head_sems, own_sem, recv_sems, raw_send, s2_send, s3_send, n_send, n_recv,
                m_raw_send, m_raw_recv, m_own, m_send, m_recv, a_send, pair_recv, hyper_sem):
    me = lax.axis_index("dp")
    core = me % 2
    pair = me + 1 - 2 * core
    flat = buf.reshape(2 * WIDE * ROWS, LANES)

    small = [pltpu.make_async_copy(src, dst, norm_sem.at[n]) for n, (src, dst) in enumerate(((norms, norms_v), (qk, qk_v)))]
    small.append(pltpu.make_async_copy(hyper_in, hyper, hyper_sem))
    for copy in small:
        copy.start()
    barrier = pltpu.get_barrier_semaphore()
    peers = [pair] + [flip(me, dim) + to for dim in range(3) for to in (0, 1 - 2 * core)]
    for peer in peers:
        pl.semaphore_signal(barrier, inc=1, device_id=(peer,), device_id_type=MESH)
    pl.semaphore_wait(barrier, len(peers))

    def hop_sem(hop, ch):
        return recv_sems.at[hop * NC + ch]

    def piece_sem(c, piece):
        return recv_sems.at[c * 7 + piece]

    def raw_at(kc, ch, src, j):
        return full.at[pl.ds(((kc * NC + ch) * 12 + src * 4 + j) * T, T)]

    def share_tiles(s, pos, n, fn):
        first = start_of(s) + pos

        @pl.when(s < 10)
        def _():
            fn(emb.at[pl.ds(first, n)])

        @pl.when(s >= 10)
        def _():
            fn(lay.at[pl.ds(first - TAIL, n)])

    def scatter(ch, with_emb, with_lay):
        def one(s, kc, src, j, target):
            @pl.when(jnp.where(s < 10, with_emb, with_lay) == 1)
            def _():
                share_tiles(s, (ch * 3 + kc) * T, T, lambda ref: put(ref, raw_at(kc, ch, src, j), raw_send, hop_sem(0, ch), target))

        for kc in range(3):
            a, b, e = axes(kc)
            far = flip(me, a)

            def share_step(j):
                near = (j // 2) * DIM[b] + (j % 2) * DIM[e]
                for to in range(2):
                    one((1 - bit(me, a)) * DIM[a] + near + to, kc, core, j, far - core + to)
                one(bit(me, a) * DIM[a] + near + 1 - core, kc, 2, j, pair)

            loop(0, 4, share_step)

    rows2 = tmp.reshape(2 * LANES, LANES)

    def norm_row(which, l, lane, at):
        rows2[at, :] = (norms_v, qk_v)[which][l, :, lane:lane + LANES].astype(F32)

    loop(0, EARLY, lambda ch: scatter(ch, 1, 0))
    for copy in small:
        copy.wait()
    norm_rows(norm_row)
    for lo, whole, split in ((0, ((emb.at[pl.ds(TAIL, OFF_Q)], 0), (out, OFF_O)), ((q, OFF_Q, 4), (k, OFF_K, 1), (v, OFF_V, 1), (gate, OFF_G, BLOCK))),
                             (HALF, ((down, OFF_D),), ((up, OFF_U, BLOCK),))):
        n = HALF if lo == 0 else LAY - HALF
        stage = full.at[pl.ds(STAGE_AT, n)]
        for src, off in whole:
            pltpu.make_async_copy(src, full.at[pl.ds(STAGE_AT + off - lo, src.shape[0])], lay_sem.at[0]).start()

        def load(i):
            for src, off, size in split:
                pltpu.make_async_copy(src.at[i // 9, :, lax.rem(i, 9)], full.at[pl.ds(STAGE_AT + off - lo + i * size, size)], lay_sem.at[0]).start()

        loop(0, BLOCKS, load)
        if lo == 0:
            copies_wait(stage, lay_sem.at[0])
        else:
            copies_wait(full.at[pl.ds(STAGE_AT, n - SCALES)], lay_sem.at[0])
            full[pl.ds(STAGE_AT + n - SCALES, SCALES)] = rows2[pl.ds(0, SCALES * ROWS), :].reshape((SCALES,) + TILE).astype(BF16)
        save = pltpu.make_async_copy(stage, lay.at[pl.ds(lo, n)], lay_sem.at[1])
        save.start()
        save.wait()
    loop(0, NC, lambda ch: scatter(ch, jnp.where(ch < EARLY, 0, 1), 1))
    state = ((mom, m_buf), (var, v_buf), (mas, p_buf))
    loads = [pltpu.make_async_copy(src, dst.at[pl.ds(HEAD * ROWS, SHARE * ROWS)], state_sem.at[n]) for n, (src, dst) in enumerate(state)]
    for copy in loads:
        copy.start()

    cut = jnp.where(core == 0, *CUT)

    def extra_at(kc):
        return WIN + kc * MINI

    def extra_sends(fn):
        for kc in range(3):
            for to, s in list(enumerate(CUT))[min(kc, 1):]:
                far = bit(me, kc) != bit(s, kc)

                @pl.when(far | (core != to))
                def _():
                    fn(kc, to, s, far)

    def extra_send(kc, to, s, far):
        put(lay.at[pl.ds(start_of(s) - TAIL + extra_at(kc), MINI)],
            full.at[pl.ds(RAW_M + (kc * 3 + jnp.where(far, core, 2)) * MINI, MINI)], m_raw_send.at[kc, to], m_raw_recv.at[kc],
            jnp.where(far, flip(me, kc), me) - core + to)

    extra_sends(extra_send)

    def fetch(ch, kc):
        a, b, e = axes(kc)
        for j in range(4):
            s = bit(me, a) * DIM[a] + (j // 2) * DIM[b] + (j % 2) * DIM[e] + core
            share_tiles(s, (ch * 3 + kc) * T, T,
                        lambda ref: pltpu.make_async_copy(ref, full.at[pl.ds(OWN_AT + (kc * 4 + j) * T, T)], own_sem.at[kc]).start())

    for kc in range(3):
        fetch(0, kc)

    def first_sum(ch):
        copies_wait(full.at[pl.ds(0, 36 * T)], hop_sem(0, ch))
        for kc in range(3):
            a, b, e = axes(kc)
            copies_wait(full.at[pl.ds(OWN_AT + kc * 4 * T, 4 * T)], own_sem.at[kc])

            def sum_step(n):
                j = (n // 2 + 1 - bit(me, b)) % 2 * 2 + n % 2

                def tile_step(t):
                    def one(at):
                        return full[pl.ds(at + t * STEP, STEP)].astype(F32)
                    raw = [one(((kc * NC + ch) * 12 + src * 4 + j) * T) for src in range(3)]
                    acc[kc, ch, pl.ds(j * T + t * STEP, STEP)] = (one(OWN_AT + (kc * 4 + j) * T) + raw[2]) + (raw[0] + raw[1])

                loop(0, T // STEP, tile_step)

            loop(0, 4, sum_step)
            put(acc.at[kc, ch, pl.ds(2 * (1 - bit(me, b)) * T, 2 * T)], buf.at[pl.ds((kc * NC + ch) * 2 * T, 2 * T)],
                s2_send, hop_sem(1, ch), flip(me, b))

            @pl.when(ch + 1 < NC)
            def _():
                fetch(ch + 1, kc)

    loop(0, NC, first_sum)

    def near(*dims):
        same = (bit(me, dims[0]) == bit(cut, dims[0])) & (core >= min(dims[0], 1))
        for dim in dims[1:]:
            same = same & (bit(me, dim) == bit(cut, dim))
        return same

    for kc in range(3):
        a, b, e = axes(kc)

        @pl.when(near(a))
        def _():
            own = full.at[pl.ds(OWN_M + kc * MINI, MINI)]
            copy = pltpu.make_async_copy(lay.at[pl.ds(start_of(cut) - TAIL + extra_at(kc), MINI)], own, m_own)
            copy.start()
            raw = [full.at[pl.ds(RAW_M + (kc * 3 + src) * MINI, MINI)] for src in range(3)]
            copies_wait(full.at[pl.ds(RAW_M + kc * 3 * MINI, 3 * MINI)], m_raw_recv.at[kc])
            copy.wait()
            acc_m[kc] = (own[...].astype(F32) + raw[2][...].astype(F32)) + (raw[0][...].astype(F32) + raw[1][...].astype(F32))

            @pl.when(bit(me, b) != bit(cut, b))
            def _():
                put(acc_m.at[kc], recv2_m.at[kc], m_send.at[kc], m_recv.at[0, kc], flip(me, b))

    def second_sum(ch):
        copies_wait(buf.at[pl.ds(0, 6 * T)], hop_sem(1, ch))
        for kc in range(3):
            a, b, e = axes(kc)
            slot = (kc * NC + ch) * 2 * T
            for je in ((1 - bit(me, e)), bit(me, e)):
                def tile_step(t):
                    at = pl.ds((2 * bit(me, b) + je) * T + t * STEP, STEP)
                    acc[kc, ch, at] = acc[kc, ch, at] + buf[pl.ds(slot + je * T + t * STEP, STEP)]

                loop(0, T // STEP, tile_step)
            put(acc.at[kc, ch, pl.ds((2 * bit(me, b) + 1 - bit(me, e)) * T, T)], recv3.at[pl.ds((ch * 3 + kc) * T, T)],
                s3_send, hop_sem(2, ch), flip(me, e))

    loop(0, NC, second_sum)
    for kc in range(3):
        a, b, e = axes(kc)

        @pl.when(near(a, b))
        def _():
            copies_wait(recv2_m.at[kc], m_recv.at[0, kc])
            acc_m[kc] = acc_m[kc] + recv2_m[kc]

            @pl.when(bit(me, e) != bit(cut, e))
            def _():
                put(acc_m.at[kc], recv3_m.at[kc], m_send.at[kc], m_recv.at[1, kc], flip(me, e))

    base = HEAD - (SHARE * me - start_of(me))

    def to_flat(lo, hi):
        walk_units(me, True, lo, hi, TO_FLAT, lambda fn, o: fn(buf, flat, tmp, o, FLAT + base + o))

    def flat_rows(t):
        return pl.ds((FLAT + t) * ROWS, ROWS)

    skip = skip_of(me)
    last = jnp.where(me == 15, SHARE, start_of(me + 1) + skip_of(me + 1) - start_of(me))

    def squares(x, first):
        ids = first + lax.broadcasted_iota(jnp.int32, x.shape, 0)
        return jnp.sum(jnp.where((ids >= skip) & (ids < last), x * x, 0.0), axis=0)

    def third_sum(ch, total):
        to_flat((ch - 1) * 3 * T, ch * 3 * T)
        copies_wait(recv3.at[pl.ds(ch * 3 * T, 3 * T)], hop_sem(2, ch))
        for kc in range(3):
            a, b, e = axes(kc)

            def tile_step(t, total):
                i = pl.ds((ch * 3 + kc) * T + t * STEP, STEP)
                x = (acc[kc, ch, pl.ds((2 * bit(me, b) + bit(me, e)) * T + t * STEP, STEP)] + recv3[i]) * 0.0625
                buf[i] = x
                return total + squares(x, (ch * 3 + kc) * T + t * STEP)

            total = lax.fori_loop(0, T // STEP, tile_step, total)
        return total

    total = lax.fori_loop(0, NC, third_sum, jnp.zeros(TILE, F32))
    part[me] = jnp.sum(total, axis=0, keepdims=True)

    for kc in range(3):
        @pl.when((me == cut) & (core >= min(kc, 1)))
        def _():
            copies_wait(recv3_m.at[kc], m_recv.at[1, kc])
            x = (acc_m[kc] + recv3_m[kc]) * 0.0625
            buf[pl.ds(extra_at(kc), MINI)] = x
            part[me] = part[me] + jnp.sum(squares(x, extra_at(kc)), axis=0, keepdims=True)

    loop(1, DEVICES, lambda n: put(part.at[me], part.at[me], n_send, n_recv, lax.rem(me + n, DEVICES)))

    def ends(cases, fn):
        for who, *case in cases:
            @pl.when(who)
            def _():
                fn(*case)

    sent = ((me < 12, 0, HEAD), (me == 13, 1, HEAD), (me == 14, 1, LAST))
    got = (((me > 0) & (me < 13), 0, HEAD), (me == 12, 1, HEAD), (me == 13, 1, LAST))

    def end_put(kind, n):
        at, to, target = ((SHARE - n, 0, me + 1), (0, HEAD + SHARE, me - 1))[kind]
        for src, dst in state:
            put(src.at[pl.ds(at * ROWS, n * ROWS)], dst.at[pl.ds(to * ROWS, n * ROWS)], head_sems.at[0, kind], head_sems.at[1, kind], target)

    def end_wait(side, kind, n):
        copies_wait(m_buf.at[pl.ds(0, 3 * n * ROWS)], head_sems.at[side, kind])

    ends(sent, end_put)
    to_flat((NC - 1) * 3 * T, 2 * WIDE)

    for copy in loads:
        copy.wait()

    def fill(x):
        return jnp.full(TILE, x, F32)

    def power7(x):
        x2 = x * x
        return x2 * x2 * x2 * x

    rate, b1, b2, decay, limit = (fill(hyper[n]) for n in range(5))
    fix1 = 1.0 / (1.0 - power7(b1))
    fix2 = 1.0 / (1.0 - power7(b2))
    others = pl.ds(0, DEVICES - 1)
    copies_wait(part.at[others], n_recv)
    norm_sum = fill(jnp.sum(part[...]))
    clip = jnp.minimum(1.0, limit / (jnp.sqrt(norm_sum) + CLIP_EPS))

    ends(got, functools.partial(end_wait, 1))

    def update(t):
        for n in range(7):
            tile = t * 7 + n
            i = pl.ds(tile * ROWS, ROWS)
            h = flat[flat_rows(tile), :] * clip
            pt = p_buf[i, :]
            mt = b1 * m_buf[i, :] + (1.0 - b1) * h
            vt = b2 * v_buf[i, :] + (1.0 - b2) * (h * h)
            has_decay = SHARE * me - HEAD + tile < TAIL + OFF_N
            u = (mt * fix1) / (jnp.sqrt(vt * fix2) + ADAM_EPS) + jnp.where(has_decay, decay, 0.0) * pt
            m_buf[i, :] = mt
            v_buf[i, :] = vt
            p_buf[i, :] = pt - rate * u

    def send(owner, c, kc, target, recv):
        block = full.at[pl.ds(owner * PUB + (c * 3 + kc) * PC, PC)]
        put(block, block, a_send, recv, target)

    mine = full.at[pl.ds(me * PUB, PUB)]

    def made(c):
        return (c * 3 * PC + 51) // 7

    def publish(c):
        loop(jnp.where(c == 0, 0, made(c)), jnp.minimum(made(c + 1), EXT // 7), update)
        walk_units(me, False, skip + c * 3 * PC, skip + (c + 1) * 3 * PC, TO_TILES, lambda fn, o: fn(mine, p_buf, tmp, o - skip, base + o))
        for hop in range(3):
            for kc in range(3):
                dim = axes(kc)[hop]
                send(me, c, kc, flip(me, dim), piece_sem(c, (0, 1, 3)[hop]))
        for kc in range(3):
            send(me, c, kc, pair, pair_recv)

    loop(0, NA, publish)

    def pass_on(level, c):
        for n in ((1,), (2, 3), (4, 5, 6, 7))[level]:
            copies_wait(full.at[pl.ds(0, 3 * PC)], piece_sem(c, n - 1))
            for kc in range(3):
                a, b, e = axes(kc)
                owner = me
                for pos, dim in enumerate((a, b, e)):
                    if (n >> pos) & 1:
                        owner = flip(owner, dim)
                if level == 0:
                    send(owner, c, kc, flip(me, b), piece_sem(c, 2))
                if level < 2:
                    send(owner, c, kc, flip(me, e), piece_sem(c, n + 3))
                send(owner, c, kc, pair, pair_recv)

    for level in range(3):
        loop(0, NA, functools.partial(pass_on, level))

    copies_wait(full.at[pl.ds(0, DEVICES // 2 * PUB)], pair_recv)
    copies_wait(full.at[pl.ds(0, (DEVICES - 1) * PUB)], a_send)
    copies_wait(full.at[pl.ds(0, RAW_END)], raw_send)
    copies_wait(buf.at[pl.ds(0, 2 * WIN)], s2_send)
    copies_wait(recv3, s3_send)
    copies_wait(part.at[others], n_send)
    ends(sent, functools.partial(end_wait, 0))
    extra_sends(lambda kc, to, s, far: copies_wait(lay.at[pl.ds(0, MINI)], m_raw_send.at[kc, to]))
    for kc in range(3):
        a, b, e = axes(kc)

        @pl.when(near(a) & jnp.logical_not(near(a, b, e)))
        def _():
            copies_wait(acc_m.at[kc], m_send.at[kc])


def finish_kernel(gathered, m, v, p, emb, q, k, v_out, out, gate, up, down, norms, qk, mom_out, var_out, mas_out, norms_v, qk_v, rows2, sem, state_sem):
    starts = [9 * (SHARE * s // 9) + {13: 9, 14: 18}.get(s, 0) for s in range(16)] + [TAIL + LAY]
    state = [pltpu.make_async_copy(src.at[pl.ds(HEAD * ROWS, SHARE * ROWS)], dst, state_sem.at[n])
             for n, (src, dst) in enumerate(((m, mom_out), (v, var_out), (p, mas_out)))]
    for copy in state:
        copy.start()
    for dst, first, n, size in ((emb, 0, EMB, 1), (q, TAIL + OFF_Q, BLOCKS, 4), (k, TAIL + OFF_K, BLOCKS, 1), (v_out, TAIL + OFF_V, BLOCKS, 1),
                                (out, TAIL + OFF_O, COLS, 1), (gate, TAIL + OFF_G, BLOCKS, BLOCK), (up, TAIL + OFF_U, BLOCKS, BLOCK),
                                (down, TAIL + OFF_D, 1458, 1)):
        for s in range(16):
            lo, hi = max(starts[s], first), min(starts[s + 1], first + n * size)
            if lo >= hi:
                continue
            src = s * PUB + lo - starts[s]
            if len(dst.shape) == 3:
                pltpu.make_async_copy(gathered.at[pl.ds(src, hi - lo)], dst.at[pl.ds(lo - first, hi - lo)], sem).start()
                continue
            unit = (lo - first) // size

            def step(i, carry, dst=dst, src=src, unit=unit, size=size):
                l, rb = (unit + i) // 9, lax.rem(unit + i, 9)
                pltpu.make_async_copy(gathered.at[pl.ds(src + i * size, size)], dst.at[l, :, rb], sem).start()
                return carry

            lax.fori_loop(0, (hi - lo) // size, step, 0)
    rows2[...] = gathered[pl.ds(15 * PUB + OFF_N - 4428, SCALES)].astype(F32).reshape(SCALES * ROWS, LANES)

    def norm_row(which, l, lane, at):
        (norms_v, qk_v)[which][l, :, lane:lane + LANES] = rows2[at, :].astype(BF16)

    norm_rows(norm_row)
    small = [pltpu.make_async_copy(src, dst, state_sem.at[3 + n]) for n, (src, dst) in enumerate(((norms_v, norms), (qk_v, qk)))]
    for copy in small:
        copy.start()
    copies_wait(gathered.at[pl.ds(0, TAIL + OFF_N)], sem)
    for copy in state + small:
        copy.wait()


ANY = pl.BlockSpec(memory_space=pl.ANY)
VM = pl.BlockSpec(memory_space=pltpu.VMEM)
DMA = pltpu.SemaphoreType.DMA


def tiled(x):
    rows, cols = x.shape[-2:]
    x = x.reshape(x.shape[:-2] + (rows // ROWS, ROWS, cols // LANES, LANES))
    return jnp.swapaxes(x, -3, -2)


def flat_tiles(x):
    return tiled(x).reshape((-1,) + TILE)


def solution(mesh):
    def local_update(*arrays):
        emb, q, k, v, out, gate, up, down, norms, qk = [a[0] for a in arrays[:GRAD_COUNT]]
        *state, hyper = arrays[GRAD_COUNT:]
        q_t, k_t, v_t, gate_t, up_t = [tiled(jnp.swapaxes(x, 1, 2)) for x in (q, k, v, gate, up)]
        small = [pltpu.VMEM(x.shape, BF16) for x in (norms, qk)]
        rows = [x.reshape(SHARE * ROWS, LANES) for x in state]
        args = [flat_tiles(emb), q_t, k_t, v_t, flat_tiles(out), gate_t, up_t, flat_tiles(down), norms, qk] + rows

        *kept, _ = pl.pallas_call(
            step_kernel,
            out_shape=(pltpu.VMEM((DEVICES * PUB,) + TILE, BF16),) + (pltpu.VMEM((EXT * ROWS, LANES), F32),) * 3
            + (jax.ShapeDtypeStruct((LAYP,) + TILE, BF16),),
            in_specs=[ANY] * 14,
            out_specs=(VM,) * 4 + (ANY,),
            scratch_shapes=[pltpu.SMEM(hyper.shape, F32)] + small + [
                pltpu.VMEM((3, NC, 4 * T) + TILE, F32), pltpu.VMEM((2 * WIDE,) + TILE, F32), pltpu.VMEM((WIN,) + TILE, F32),
                pltpu.VMEM((2, LANES, LANES), F32), pltpu.VMEM((DEVICES, 1, LANES), F32)]
            + [pltpu.VMEM((3, MINI) + TILE, F32)] * 3
            + [DMA((2,)), DMA((2,)), DMA((3,)), DMA((2, 2)), DMA((3,)), DMA((max(3 * NC, 7 * NA),)), DMA, DMA, DMA, DMA, DMA,
               DMA((3, 2)), DMA((3,)), DMA, DMA((3,)), DMA((2, 3)), DMA, DMA, DMA],
            compiler_params=pltpu.CompilerParams(collective_id=0, has_side_effects=True, vmem_limit_bytes=GRANT),
            name="step",
        )(*args, hyper)

        emb2, q2, k2, v2, out2, gate2, up2, down2, norms2, qk2, *state2 = pl.pallas_call(
            finish_kernel,
            out_shape=tuple(jax.ShapeDtypeStruct(x.shape, x.dtype) for x in args),
            in_specs=[VM] * 4,
            out_specs=(ANY,) * 13,
            scratch_shapes=small + [pltpu.VMEM((SCALES * ROWS, LANES), F32), DMA, DMA((5,))],
            compiler_params=pltpu.CompilerParams(vmem_limit_bytes=GRANT),
            name="finish",
        )(*[pltpu.with_memory_space_constraint(x, pltpu.VMEM) for x in kept])

        def matrices(x, like):
            x = x.reshape(like.shape[:-2] + (-1, like.shape[-1] // LANES) + TILE)
            return jnp.swapaxes(x, -3, -2).reshape(like.shape)

        def columns(x, like):
            return jnp.swapaxes(matrices(x, jnp.swapaxes(like, 1, 2)), 1, 2)

        params = (matrices(emb2, emb), columns(q2, q), columns(k2, k), columns(v2, v), matrices(out2, out), columns(gate2, gate), columns(up2, up),
                  matrices(down2, down), norms2, qk2)
        return params + tuple(x.reshape(-1) for x in state2)

    in_specs = tuple([P("dp")] * GRAD_COUNT + [P("dp"), P("dp"), P("dp"), P()])
    out_specs = tuple([P()] * GRAD_COUNT + [P("dp"), P("dp"), P("dp")])
    return jax.shard_map(local_update, mesh=mesh, in_specs=in_specs, out_specs=out_specs, check_vma=False)
```
